256 devices in a mesh: cells: 128 (over y_lo, x, z, core), ens: 2 (over y_hi).
Axes of the slice: x: 4, y: 4 (y_hi: 2, y_lo: 2; y = y_hi * 2 + y_lo), z: 8, core: 2. Of those that a mesh axis runs over, the one named last changes fastest.
Arguments:
- later_adjoint: float32 [4, 4, 256, 8, 128], P('ens', None, 'cells'), may hold values from -6 to 6
- coupling: bfloat16 [4, 6, 4, 4, 256, 8, 128], P('ens', None, None, None, 'cells'), may hold values from -0.59765625 to 0.59765625
- diag_inverse: bfloat16 [4, 4, 4, 256, 8, 128], P('ens', None, None, 'cells'), may hold values from -0.7 to 1.6, as said below
- sensitivity: bfloat16 [4, 4, 256, 8, 128, 128], P('ens', None, 'cells'), may hold values from -0.0625 to 0.0625
- well_cells: int32 [256], replicated, may hold values from 0 to 262143
- well_misfit: float32 [4, 4, 256], P('ens'), may hold values from -6 to 6
- block_map: int32 [256, 8, 128], P('cells'), may hold values from 0 to 511, as said below
Outputs:
- adjoint: float32 [4, 4, 256, 8, 128], P('ens', None, 'cells')
- gradient: float32 [512, 128], P('cells')
The draws below stay inside these ranges and needn't reach their ends.
Inputs may be any that keep to these rules, and one draw needn't show every extreme that they name: `block_map`: of the cells of each slab of 2 planes along the first dimension (x from i * 2 to i * 2 + 1), exactly 16 map to blocks whose number divided by 4 (rounded down) equals any given j. `diag_inverse`: each block is the inverse of a diagonal block; its diagonal entries lie in 0.4 to 1.6. `well_cells`: wells may share a cell.
All inputs are finite; a program needn't handle non-finite values.
Results may differ from the reference program's by a relative error of at most 0.0003.
Values sent between devices are 32-bit elements; how exact they have to be, the bound alone decides.
No kernel may reach another device: no remote copies, remote signals or barrier semaphores. Data moves between devices by JAX's collectives and lax.ppermute only.
A program may use at most 64 MiB of HBM per device.

```python
import jax
import jax.numpy as jnp
from jax import lax

UNK = 4
PBLK = 128
CX = 2
NY = 8
NZ = 128
ITERS = 4
WELLS = 256
BLK_DEV = 4
MEMBERS = 4
NX = 256
NBLK = 512
N_CELLS = 128


def draw_diag_inverse(key, part):
    shape = (MEMBERS, UNK, UNK, NX, NY, NZ)
    identity = jnp.eye(UNK, dtype=jnp.float32)[None, :, :, None, None, None]
    key_diag = jax.random.fold_in(key, 21)
    key_off = jax.random.fold_in(key, 22)
    diagonal = jax.random.uniform(key_diag, shape, jnp.float32, 0.6, 1.4)
    offdiag = jnp.clip(0.2 * jax.random.normal(key_off, shape, jnp.float32), -0.7, 0.7)
    return (identity * diagonal + (1.0 - identity) * offdiag).astype(jnp.bfloat16)


def draw_block_map(key, part):
    slab_cells = CX * NY * NZ
    per_owner = slab_cells // N_CELLS
    owners = jnp.repeat(jnp.arange(N_CELLS, dtype=jnp.int32), per_owner)
    keys = jax.random.split(jax.random.fold_in(key, 31), N_CELLS)
    shuffled = jax.vmap(lambda single: jax.random.permutation(single, owners))(keys)
    within = jax.random.randint(jax.random.fold_in(key, 32), (N_CELLS, slab_cells), 0, BLK_DEV, dtype=jnp.int32)
    return (shuffled * BLK_DEV + within).reshape(NX, NY, NZ)


def plant(entries, stream_key, low, high):
    longest = entries.shape.index(max(entries.shape))
    spots = []
    for shift in (0, 1):
        where = [jax.random.randint(jax.random.fold_in(stream_key, axis), (), 0, length) for axis, length in enumerate(entries.shape)]
        where[longest] = (where[longest] + shift) % entries.shape[longest]
        spots.append(tuple(where))
    return entries.at[spots[0]].set(low).at[spots[1]].set(high)


def level_of(rng, shape, cuts, smallest, largest):
    def one(position, blocks):
        heights = jax.random.uniform(jax.random.fold_in(jax.random.fold_in(rng, 6), position), (blocks,), jnp.float32, smallest / len(cuts), largest / len(cuts))
        return jnp.repeat(jnp.exp(heights), shape[position] // blocks).reshape((-1,) + (1,) * (len(shape) - position - 1))

    loudness = one(*cuts[0])
    for cut in cuts[1:]:
        loudness = loudness * one(*cut)
    return loudness


def scatter_about(own_key, shape, width, most, cuts=(), kind=jnp.bfloat16):
    factor_of = level_of(own_key, shape, cuts, -0.22, 0.18) if cuts else 1.0
    result = jax.random.normal(own_key, shape, jnp.float32) * width * factor_of
    return jnp.minimum(jnp.maximum(result, -most), most).astype(kind)


def setup_inputs(seed: int = 0) -> dict:
    splits = jax.random.split(jax.random.key(seed), 8)
    later_adjoint = scatter_about(splits[0], (MEMBERS, UNK, NX, NY, NZ), 1.0, 6.0, ((0, 2), (2, 128)), jnp.float32)
    coupling = scatter_about(splits[1], (MEMBERS, 6, UNK, UNK, NX, NY, NZ), 0.1, 0.59765625, ((0, 2), (4, 128)))
    diag_inverse = draw_diag_inverse(jax.random.fold_in(splits[7], 71), 0)
    sensitivity = scatter_about(splits[3], (MEMBERS, UNK, NX, NY, NZ, PBLK), (UNK * MEMBERS * CX * NY * NZ // BLK_DEV) ** -0.5, 0.0625, ((0, 2), (2, 128)))
    well_cells = plant(jax.random.randint(splits[4], (WELLS,), 0, NX * NY * NZ), jax.random.fold_in(splits[4], 1), 0, (NX * NY * NZ) - 1).astype(jnp.int32)
    well_misfit = scatter_about(splits[5], (MEMBERS, UNK, WELLS), 1.0, 6.0, ((0, 2),), jnp.float32)
    block_map = draw_block_map(jax.random.fold_in(splits[7], 71), 0)
    return {"later_adjoint": later_adjoint, "coupling": coupling, "diag_inverse": diag_inverse, "sensitivity": sensitivity, "well_cells": well_cells, "well_misfit": well_misfit, "block_map": block_map}


def move_along(field, axis, forward):
    length = field.shape[axis]
    shape = list(field.shape)
    shape[axis] = 1
    zeros = jnp.zeros(shape, jnp.float32)
    if forward:
        return jnp.concatenate([zeros, lax.slice_in_dim(field, 0, length - 1, axis=axis)], axis=axis)
    return jnp.concatenate([lax.slice_in_dim(field, 1, length, axis=axis), zeros], axis=axis)


def coupling_sum(adjoint, coupling):
    terms = jnp.sum(coupling.astype(jnp.float32) * adjoint[:, None, :, None], axis=2)
    total = jnp.zeros(adjoint.shape, jnp.float32)
    directions = [(2, True), (2, False), (3, True), (3, False), (4, True), (4, False)]
    for number, (axis, forward) in enumerate(directions):
        total = total + move_along(terms[:, number], axis, forward)
    return total


def apply_inverse(diag_inverse, source):
    return jnp.sum(diag_inverse.astype(jnp.float32) * source[:, :, None], axis=1)


def reference(later_adjoint, coupling, diag_inverse, sensitivity, well_cells, well_misfit, block_map):
    members = later_adjoint.shape[0]
    count = NX * NY * NZ
    flat = later_adjoint.reshape(members, UNK, count)
    flat = flat.at[:, :, well_cells].add(well_misfit)
    source = flat.reshape(later_adjoint.shape)
    adjoint = apply_inverse(diag_inverse, source)
    for sweep in range(ITERS):
        adjoint = apply_inverse(diag_inverse, source - coupling_sum(adjoint, coupling))
    adjoint_flat = adjoint.reshape(members, UNK, count)
    sens_flat = sensitivity.reshape(members, UNK, count, PBLK)
    cell_grad = jnp.zeros((count, PBLK), jnp.float32)
    for member in range(members):
        for unknown in range(UNK):
            cell_grad = cell_grad + adjoint_flat[member, unknown][:, None] * sens_flat[member, unknown].astype(jnp.float32)
    gradient = jax.ops.segment_sum(cell_grad, block_map.reshape(-1), num_segments=NBLK)
    return adjoint, gradient
```

```python
import jax
import jax.numpy as jnp
from jax import lax
from jax.experimental import pallas as pl
from jax.experimental.pallas import tpu as pltpu
from jax.sharding import PartitionSpec as P

BLK_DEV = 4
F32 = jnp.float32
BF16 = jnp.bfloat16


def shift_lanes(x, by):
    size = x.shape[2]
    lane = lax.broadcasted_iota(jnp.int32, x.shape, 2)
    keep = lane >= 1 if by == 1 else lane < size - 1
    return jnp.where(keep, pltpu.roll(x, by % size, 2), 0.0)


def shift_rows(x, by):
    size = x.shape[1]
    row = lax.broadcasted_iota(jnp.int32, x.shape, 1)
    keep = row >= 1 if by == 1 else row < size - 1
    return jnp.where(keep, pltpu.roll(x, by % size, 1), 0.0)


def products(cpl, m, k, a):
    unk = len(a)
    out = []
    for v in range(unk):
        total = cpl[m, k, 0, v].astype(F32) * a[0]
        for u in range(1, unk):
            total = total + cpl[m, k, u, v].astype(F32) * a[u]
        out.append(total)
    return out


def local_coupling(cpl, m, a):
    unk = len(a)
    terms = [products(cpl, m, k, a) for k in range(6)]
    inner, up, down = [], [], []
    for v in range(unk):
        t = [terms[k][v] for k in range(6)]
        planes = t[0].shape[0]
        zero = jnp.zeros_like(t[0][:1])
        total = jnp.concatenate([zero, t[0][: planes - 1]], axis=0)
        total = total + jnp.concatenate([t[1][1:], zero], axis=0)
        total = total + shift_rows(t[2], 1) + shift_rows(t[3], -1)
        total = total + shift_lanes(t[4], 1) + shift_lanes(t[5], -1)
        inner.append(total)
        up.append(t[0][planes - 1])
        down.append(t[1][0])
    return inner, up, down


def apply_inverse(inv, m, r):
    unk = len(r)
    out = []
    for v in range(unk):
        total = inv[m, 0, v].astype(F32) * r[0]
        for w in range(1, unk):
            total = total + inv[m, w, v].astype(F32) * r[w]
        out.append(total)
    return out


def plane_products(cpl, m, k, plane, a):
    unk = len(a)
    out = []
    for v in range(unk):
        total = cpl[m, k, 0, v, plane].astype(F32) * a[0]
        for u in range(1, unk):
            total = total + cpl[m, k, u, v, plane].astype(F32) * a[u]
        out.append(total)
    return out


def two_sweep_payload(cpl, inv, m, src, a):
    planes = a[0].shape[0]
    inner, up0, down0 = local_coupling(cpl, m, a)
    nxt = apply_inverse(inv, m, [s - b for s, b in zip(src, inner)])
    up1 = plane_products(cpl, m, 0, planes - 1, [x[planes - 1] for x in nxt])
    down1 = plane_products(cpl, m, 1, 0, [x[0] for x in nxt])
    return nxt, up0 + up1, down0 + down1


def transfer_blocks(cpl, inv, m, k, plane, unk):
    out = []
    for w in range(unk):
        for v in range(unk):
            total = inv[m, w, 0, plane].astype(F32) * cpl[m, k, 0, v, plane].astype(F32)
            for u in range(1, unk):
                total = total + inv[m, w, u, plane].astype(F32) * cpl[m, k, u, v, plane].astype(F32)
            out.append(total)
    return out


def split3(x):
    hi = x.astype(BF16)
    rest = x - hi.astype(F32)
    mid = rest.astype(BF16)
    lo = (rest - mid.astype(F32)).astype(BF16)
    return hi, mid, lo


def injected(wells, misfit, first, shape):
    members, unk, planes, rows, lanes = shape
    count = planes * rows * lanes
    nwell = wells.shape[1]
    place = wells[...] - first
    inside = (place >= 0) & (place < count)
    line = jnp.where(inside, place // lanes, -1)
    lane = jnp.where(inside, place % lanes, -1)
    lines = lax.broadcasted_iota(jnp.int32, (planes * rows, nwell), 0) == line
    onlane = (lax.broadcasted_iota(jnp.int32, (lanes, nwell), 0) == lane).astype(F32).astype(BF16)
    left = []
    for m in range(members):
        for u in range(unk):
            left.append(jnp.where(lines, misfit[m, u : u + 1, :], 0.0))
    stacked = jnp.concatenate(split3(jnp.concatenate(left, axis=0)), axis=0)
    full = lax.dot_general(stacked, onlane, (((1,), (1,)), ((), ())), preferred_element_type=F32)
    n = members * unk * planes * rows
    total = full[:n] + full[n : 2 * n] + full[2 * n :]
    return total.reshape(shape)


def start_kernel(pos, wells, misfit, later, cpl, inv, src_out, nxt_out, intra_out, cross_out):
    shape = later.shape
    members, unk, planes = shape[:3]
    even = pos[0] % 2 == 0
    count = planes * shape[3] * shape[4]
    src_out[...] = later[...] + injected(wells, misfit, pos[0] * count, shape)
    for m in range(members):
        src = [src_out[m, u] for u in range(unk)]
        a = apply_inverse(inv, m, src)
        nxt, up, down = two_sweep_payload(cpl, inv, m, src, a)
        up = up + transfer_blocks(cpl, inv, m, 0, planes - 1, unk)
        down = down + transfer_blocks(cpl, inv, m, 1, 0, unk)
        for u in range(unk):
            nxt_out[m, u] = nxt[u]
        for j in range(len(up)):
            intra_out[m, j] = jnp.where(even, up[j], down[j])
            cross_out[m, j] = jnp.where(even, down[j], up[j])


def incoming(pos, last, m, unk, blocks, sent_intra, sent_cross, got_intra, got_cross):
    even = pos[0] % 2 == 0
    has_cross = (pos[0] != 0) & (pos[0] != last)
    out = []
    sides = []
    for sent, got, block in ((sent_intra, got_intra, blocks[0]), (sent_cross, got_cross, blocks[1])):
        first = [got[m, v] for v in range(unk)]
        second = []
        for v in range(unk):
            total = got[m, unk + v]
            for w in range(unk):
                total = total - block[m, 2 * unk + w * unk + v] * sent[m, w]
            second.append(total)
        sides.append((first, second))
    for n in range(2):
        low, high = [], []
        for v in range(unk):
            near = sides[0][n][v]
            far = jnp.where(has_cross, sides[1][n][v], 0.0)
            low.append(jnp.where(even, far, near))
            high.append(jnp.where(even, near, far))
        out.append([jnp.stack([lo, hi], axis=0) for lo, hi in zip(low, high)])
    return out


def finish_two(cpl, inv, m, src, nxt, arrived):
    a1 = [x - d for x, d in zip(nxt, apply_inverse(inv, m, arrived[0]))]
    inner, _, _ = local_coupling(cpl, m, a1)
    return apply_inverse(inv, m, [s - b - p for s, b, p in zip(src, inner, arrived[1])])


def make_middle(last):
    def middle_kernel(pos, src, nxt, sent_intra, sent_cross, got_intra, got_cross, cpl, inv, nxt_out, intra_out, cross_out):
        members, unk = src.shape[:2]
        even = pos[0] % 2 == 0
        for m in range(members):
            arrived = incoming(
                pos, last, m, unk, (got_intra, got_cross), sent_intra, sent_cross, got_intra, got_cross
            )
            s = [src[m, u] for u in range(unk)]
            a = finish_two(cpl, inv, m, s, [nxt[m, u] for u in range(unk)], arrived)
            ahead, up, down = two_sweep_payload(cpl, inv, m, s, a)
            for u in range(unk):
                nxt_out[m, u] = ahead[u]
            for j in range(len(up)):
                intra_out[m, j] = jnp.where(even, up[j], down[j])
                cross_out[m, j] = jnp.where(even, down[j], up[j])

    return middle_kernel


def make_end(last, nblk):
    def end_kernel(
        pos, src, nxt, block_intra, block_cross, sent_intra, sent_cross, got_intra, got_cross, cpl, inv, bmap, sens,
        adj_out, mine_out, other_out, sens_buf, onehot, grads, sems,
    ):
        members, unk, planes, rows, lanes = src.shape
        params = sens.shape[-1]
        groups = planes * rows
        copies = []
        for x in range(planes):
            for half in range(2):
                n = rows // 2
                part = (slice(None), slice(None), x, slice(half * n, half * n + n))
                copies.append(pltpu.make_async_copy(sens.at[part], sens_buf.at[part], sems.at[x * 2 + half]))
        for c in copies:
            c.start()
        core = pos[0] % 2
        slot = lax.broadcasted_iota(jnp.int32, (nblk, lanes), 0)
        half_rows = nblk // 2
        parity = jnp.where(slot < half_rows, core, 1 - core)
        within = jnp.where(slot < half_rows, slot, slot - half_rows)
        block = (within // BLK_DEV * 2 + parity) * BLK_DEV + within % BLK_DEV
        for g in range(groups):
            row = bmap[g // rows, g % rows : g % rows + 1, :]
            onehot[:, g * lanes : (g + 1) * lanes] = (block == row).astype(F32).astype(BF16)
        for m in range(members):
            arrived = incoming(
                pos, last, m, unk, (block_intra, block_cross), sent_intra, sent_cross, got_intra, got_cross
            )
            a = finish_two(
                cpl, inv, m, [src[m, u] for u in range(unk)], [nxt[m, u] for u in range(unk)], arrived
            )
            for u in range(unk):
                adj_out[m, u] = a[u]
        turned = adj_out[...].reshape(members * unk * groups, lanes).T
        per = groups // len(copies)
        for i, c in enumerate(copies):
            c.wait()
            for g in range(i * per, i * per + per):
                x, y = g // rows, g % rows
                total = None
                for m in range(members):
                    for u in range(unk):
                        col = (m * unk + u) * groups + g
                        term = turned[:, col : col + 1] * sens_buf[m, u, x, y].astype(F32)
                        total = term if total is None else total + term
                hi = total.astype(BF16)
                lo = (total - hi.astype(F32)).astype(BF16)
                grads[g * lanes : (g + 1) * lanes, :params] = hi
                grads[g * lanes : (g + 1) * lanes, params:] = lo
        both = jnp.dot(onehot[...], grads[...], preferred_element_type=F32)
        out = both[:, :params] + both[:, params:]
        mine_out[...] = out[:half_rows]
        other_out[...] = out[half_rows:]

    return end_kernel


VM = pl.BlockSpec(memory_space=pltpu.VMEM)
SM = pl.BlockSpec(memory_space=pltpu.SMEM)
HB = pl.BlockSpec(memory_space=pl.ANY)


def shaped(*shape):
    return jax.ShapeDtypeStruct(shape, F32)


def body(later_adjoint, coupling, diag_inverse, sensitivity, well_cells, well_misfit, block_map):
    members, unk, planes, rows, lanes = later_adjoint.shape
    count = planes * rows * lanes
    params = sensitivity.shape[-1]
    ranks = lax.axis_size("cells")
    nblk = ranks * BLK_DEV
    pos = lax.axis_index("cells").astype(jnp.int32).reshape(1)
    intra_pairs = [(i, i ^ 1) for i in range(ranks)]
    cross_pairs = [(i, i + 1 if i % 2 else i - 1) for i in range(1, ranks - 1)] + [(0, 0), (ranks - 1, ranks - 1)]

    def exchange(intra, cross):
        return lax.ppermute(intra, "cells", intra_pairs), lax.ppermute(cross, "cells", cross_pairs)

    field = shaped(members, unk, planes, rows, lanes)
    first_size = 2 * unk + unk * unk
    with jax.named_scope("start"):
        src, nxt, intra, cross = pl.pallas_call(
            start_kernel,
            out_shape=(field, field, shaped(members, first_size, rows, lanes), shaped(members, first_size, rows, lanes)),
            in_specs=[SM, VM, VM, VM, VM, VM],
            out_specs=(VM, VM, VM, VM),
        )(pos, well_cells.reshape(1, -1), well_misfit, later_adjoint, coupling, diag_inverse)
    got_intra, got_cross = exchange(intra, cross)
    with jax.named_scope("middle"):
        nxt2, intra2, cross2 = pl.pallas_call(
            make_middle(ranks - 1),
            out_shape=(field, shaped(members, 2 * unk, rows, lanes), shaped(members, 2 * unk, rows, lanes)),
            in_specs=[SM] + [VM] * 8,
            out_specs=(VM, VM, VM),
        )(pos, src, nxt, intra, cross, got_intra, got_cross, coupling, diag_inverse)
    got_intra2, got_cross2 = exchange(intra2, cross2)
    with jax.named_scope("end"):
        adjoint, mine, other = pl.pallas_call(
            make_end(ranks - 1, nblk),
            out_shape=(field, shaped(nblk // 2, params), shaped(nblk // 2, params)),
            in_specs=[SM] + [VM] * 11 + [HB],
            out_specs=(VM, VM, VM),
            scratch_shapes=[
                pltpu.VMEM(sensitivity.shape, BF16),
                pltpu.VMEM((nblk, count), BF16),
                pltpu.VMEM((count, 2 * params), BF16),
                pltpu.SemaphoreType.DMA((2 * planes,)),
            ],
        )(
            pos, src, nxt2, got_intra, got_cross, intra2, cross2, got_intra2, got_cross2,
            coupling, diag_inverse, block_map, sensitivity,
        )
    chips = ranks // 2
    half = mine + lax.ppermute(other, "cells", intra_pairs)
    same_core = [[core + 2 * chip for chip in range(chips)] for core in range(2)]
    parts = lax.all_to_all(
        half.reshape(chips, BLK_DEV, params), "cells", 0, 0, tiled=True, axis_index_groups=same_core
    )
    owned = jnp.sum(parts, axis=0)
    gradient = owned + lax.ppermute(owned, "ens", [(0, 1), (1, 0)])
    return (adjoint, gradient)


def solution(mesh):
    placed = (
        P("ens", None, "cells", None, None),
        P("ens", None, None, None, "cells", None, None),
        P("ens", None, None, "cells", None, None),
        P("ens", None, "cells", None, None, None),
        P(),
        P("ens", None, None),
        P("cells", None, None),
    )
    return jax.shard_map(
        body,
        mesh=mesh,
        in_specs=placed,
        out_specs=(P("ens", None, "cells", None, None), P("cells", None)),
        check_vma=False,
    )
```

```python
import jax
import jax.numpy as jnp
from jax import lax
from jax.experimental import pallas as pl
from jax.experimental.pallas import tpu as pltpu
from jax.sharding import PartitionSpec as P

BLK_DEV = 4
F32 = jnp.float32
BF16 = jnp.bfloat16


def shift_lanes(x, by):
    size = x.shape[2]
    lane = lax.broadcasted_iota(jnp.int32, x.shape, 2)
    keep = lane >= 1 if by == 1 else lane < size - 1
    return jnp.where(keep, pltpu.roll(x, by % size, 2), 0.0)


def shift_rows(x, by):
    size = x.shape[1]
    row = lax.broadcasted_iota(jnp.int32, x.shape, 1)
    keep = row >= 1 if by == 1 else row < size - 1
    return jnp.where(keep, pltpu.roll(x, by % size, 1), 0.0)


def products(cpl, m, k, a):
    unk = len(a)
    out = []
    for v in range(unk):
        total = cpl[m, k, 0, v].astype(F32) * a[0]
        for u in range(1, unk):
            total = total + cpl[m, k, u, v].astype(F32) * a[u]
        out.append(total)
    return out


def local_coupling(cpl, m, a):
    unk = len(a)
    terms = [products(cpl, m, k, a) for k in range(6)]
    inner, up, down = [], [], []
    for v in range(unk):
        t = [terms[k][v] for k in range(6)]
        planes = t[0].shape[0]
        zero = jnp.zeros_like(t[0][:1])
        total = jnp.concatenate([zero, t[0][: planes - 1]], axis=0)
        total = total + jnp.concatenate([t[1][1:], zero], axis=0)
        total = total + shift_rows(t[2], 1) + shift_rows(t[3], -1)
        total = total + shift_lanes(t[4], 1) + shift_lanes(t[5], -1)
        inner.append(total)
        up.append(t[0][planes - 1])
        down.append(t[1][0])
    return inner, up, down


def apply_inverse(inv, m, r):
    unk = len(r)
    out = []
    for v in range(unk):
        total = inv[m, 0, v].astype(F32) * r[0]
        for w in range(1, unk):
            total = total + inv[m, w, v].astype(F32) * r[w]
        out.append(total)
    return out


def plane_products(cpl, m, k, plane, a):
    unk = len(a)
    out = []
    for v in range(unk):
        total = cpl[m, k, 0, v, plane].astype(F32) * a[0]
        for u in range(1, unk):
            total = total + cpl[m, k, u, v, plane].astype(F32) * a[u]
        out.append(total)
    return out


def two_sweep_payload(cpl, inv, m, src, a):
    planes = a[0].shape[0]
    inner, up0, down0 = local_coupling(cpl, m, a)
    nxt = apply_inverse(inv, m, [s - b for s, b in zip(src, inner)])
    up1 = plane_products(cpl, m, 0, planes - 1, [x[planes - 1] for x in nxt])
    down1 = plane_products(cpl, m, 1, 0, [x[0] for x in nxt])
    return nxt, up0 + up1, down0 + down1


def transfer_blocks(cpl, inv, m, k, plane, unk):
    out = []
    for w in range(unk):
        for v in range(unk):
            total = inv[m, w, 0, plane].astype(F32) * cpl[m, k, 0, v, plane].astype(F32)
            for u in range(1, unk):
                total = total + inv[m, w, u, plane].astype(F32) * cpl[m, k, u, v, plane].astype(F32)
            out.append(total)
    return out


def split3(x):
    hi = x.astype(BF16)
    rest = x - hi.astype(F32)
    mid = rest.astype(BF16)
    lo = (rest - mid.astype(F32)).astype(BF16)
    return hi, mid, lo


def injected(wells, misfit, first, shape):
    members, unk, planes, rows, lanes = shape
    count = planes * rows * lanes
    nwell = wells.shape[1]
    place = wells[...] - first
    inside = (place >= 0) & (place < count)
    line = jnp.where(inside, place // lanes, -1)
    lane = jnp.where(inside, place % lanes, -1)
    lines = lax.broadcasted_iota(jnp.int32, (planes * rows, nwell), 0) == line
    onlane = (lax.broadcasted_iota(jnp.int32, (lanes, nwell), 0) == lane).astype(F32).astype(BF16)
    left = []
    for m in range(members):
        for u in range(unk):
            left.append(jnp.where(lines, misfit[m, u : u + 1, :], 0.0))
    stacked = jnp.concatenate(split3(jnp.concatenate(left, axis=0)), axis=0)
    full = lax.dot_general(stacked, onlane, (((1,), (1,)), ((), ())), preferred_element_type=F32)
    n = members * unk * planes * rows
    total = full[:n] + full[n : 2 * n] + full[2 * n :]
    return total.reshape(shape)


def start_kernel(
    pos, wells_in, misfit_in, later_in, cpl_in, inv_in, src, nxt_out, intra_out, cross_out, cpl, inv, wells, misfit, sems
):
    shape = src.shape
    members, unk, planes = shape[:3]
    moves = ((wells_in, wells), (misfit_in, misfit), (later_in, src), (inv_in, inv), (cpl_in, cpl))
    copies = [pltpu.make_async_copy(a, b, sems.at[i]) for i, (a, b) in enumerate(moves)]
    for c in copies:
        c.start()
    even = pos[0] % 2 == 0
    count = planes * shape[3] * shape[4]
    copies[0].wait()
    copies[1].wait()
    extra = injected(wells, misfit, pos[0] * count, shape)
    copies[2].wait()
    src[...] = src[...] + extra
    copies[3].wait()
    copies[4].wait()
    for m in range(members):
        s = [src[m, u] for u in range(unk)]
        a = apply_inverse(inv, m, s)
        nxt, up, down = two_sweep_payload(cpl, inv, m, s, a)
        up = up + transfer_blocks(cpl, inv, m, 0, planes - 1, unk)
        down = down + transfer_blocks(cpl, inv, m, 1, 0, unk)
        for u in range(unk):
            nxt_out[m, u] = nxt[u]
        for j in range(len(up)):
            intra_out[m, j] = jnp.where(even, up[j], down[j])
            cross_out[m, j] = jnp.where(even, down[j], up[j])


def incoming(pos, last, m, unk, blocks, sent_intra, sent_cross, got_intra, got_cross):
    even = pos[0] % 2 == 0
    has_cross = (pos[0] != 0) & (pos[0] != last)
    out = []
    sides = []
    for sent, got, block in ((sent_intra, got_intra, blocks[0]), (sent_cross, got_cross, blocks[1])):
        first = [got[m, v] for v in range(unk)]
        second = []
        for v in range(unk):
            total = got[m, unk + v]
            for w in range(unk):
                total = total - block[m, 2 * unk + w * unk + v] * sent[m, w]
            second.append(total)
        sides.append((first, second))
    for n in range(2):
        low, high = [], []
        for v in range(unk):
            near = sides[0][n][v]
            far = jnp.where(has_cross, sides[1][n][v], 0.0)
            low.append(jnp.where(even, far, near))
            high.append(jnp.where(even, near, far))
        out.append([jnp.stack([lo, hi], axis=0) for lo, hi in zip(low, high)])
    return out


def finish_two(cpl, inv, m, src, nxt, arrived):
    a1 = [x - d for x, d in zip(nxt, apply_inverse(inv, m, arrived[0]))]
    inner, _, _ = local_coupling(cpl, m, a1)
    return apply_inverse(inv, m, [s - b - p for s, b, p in zip(src, inner, arrived[1])])


def make_middle(last):
    def middle_kernel(pos, src, nxt, sent_intra, sent_cross, got_intra, got_cross, cpl, inv, nxt_out, intra_out, cross_out):
        members, unk = src.shape[:2]
        even = pos[0] % 2 == 0
        for m in range(members):
            arrived = incoming(
                pos, last, m, unk, (got_intra, got_cross), sent_intra, sent_cross, got_intra, got_cross
            )
            s = [src[m, u] for u in range(unk)]
            a = finish_two(cpl, inv, m, s, [nxt[m, u] for u in range(unk)], arrived)
            ahead, up, down = two_sweep_payload(cpl, inv, m, s, a)
            for u in range(unk):
                nxt_out[m, u] = ahead[u]
            for j in range(len(up)):
                intra_out[m, j] = jnp.where(even, up[j], down[j])
                cross_out[m, j] = jnp.where(even, down[j], up[j])

    return middle_kernel


def select_kernel(pos, bmap_in, sens_in, onehot, sens, bmap, sems):
    fetch = pltpu.make_async_copy(sens_in, sens, sems.at[0])
    small = pltpu.make_async_copy(bmap_in, bmap, sems.at[1])
    small.start()
    fetch.start()
    rows, lanes = bmap.shape[1:]
    nblk = onehot.shape[0]
    core = pos[0] % 2
    slot = lax.broadcasted_iota(jnp.int32, (nblk, lanes), 0)
    half_rows = nblk // 2
    parity = jnp.where(slot < half_rows, core, 1 - core)
    within = jnp.where(slot < half_rows, slot, slot - half_rows)
    block = (within // BLK_DEV * 2 + parity) * BLK_DEV + within % BLK_DEV
    small.wait()
    for g in range(bmap.shape[0] * rows):
        row = bmap[g // rows, g % rows : g % rows + 1, :]
        onehot[:, g * lanes : (g + 1) * lanes] = (block == row).astype(F32).astype(BF16)
    fetch.wait()


def make_end(last, nblk):
    def end_kernel(
        pos, src, nxt, block_intra, block_cross, sent_intra, sent_cross, got_intra, got_cross, cpl, inv, onehot, sens,
        adj_out, mine_out, other_out, adj, grads, sems,
    ):
        members, unk, planes, rows, lanes = src.shape
        params = sens.shape[-1]
        groups = planes * rows
        half_rows = nblk // 2
        for m in range(members):
            arrived = incoming(
                pos, last, m, unk, (block_intra, block_cross), sent_intra, sent_cross, got_intra, got_cross
            )
            a = finish_two(
                cpl, inv, m, [src[m, u] for u in range(unk)], [nxt[m, u] for u in range(unk)], arrived
            )
            for u in range(unk):
                adj[m, u] = a[u]
        store = pltpu.make_async_copy(adj, adj_out, sems.at[0])
        store.start()
        turned = adj[...].reshape(members * unk * groups, lanes).T
        for g in range(groups):
            x, y = g // rows, g % rows
            total = None
            for m in range(members):
                for u in range(unk):
                    col = (m * unk + u) * groups + g
                    term = turned[:, col : col + 1] * sens[m, u, x, y].astype(F32)
                    total = term if total is None else total + term
            hi = total.astype(BF16)
            lo = (total - hi.astype(F32)).astype(BF16)
            grads[g * lanes : (g + 1) * lanes, :params] = hi
            grads[g * lanes : (g + 1) * lanes, params:] = lo
        both = jnp.dot(onehot[...], grads[...], preferred_element_type=F32)
        out = both[:, :params] + both[:, params:]
        mine_out[...] = out[:half_rows]
        other_out[...] = out[half_rows:]
        store.wait()

    return end_kernel


VM = pl.BlockSpec(memory_space=pltpu.VMEM)
SM = pl.BlockSpec(memory_space=pltpu.SMEM)
HB = pl.BlockSpec(memory_space=pltpu.HBM)
MIB = 1 << 20


def room(mib):
    return pltpu.CompilerParams(vmem_limit_bytes=mib * MIB)


def shaped(*shape):
    return jax.ShapeDtypeStruct(shape, F32)


def body(later_adjoint, coupling, diag_inverse, sensitivity, well_cells, well_misfit, block_map):
    members, unk, planes, rows, lanes = later_adjoint.shape
    count = planes * rows * lanes
    params = sensitivity.shape[-1]
    ranks = lax.axis_size("cells")
    nblk = ranks * BLK_DEV
    pos = lax.axis_index("cells").astype(jnp.int32).reshape(1)
    intra_pairs = [(i, i ^ 1) for i in range(ranks)]
    cross_pairs = [(i, i + 1 if i % 2 else i - 1) for i in range(1, ranks - 1)] + [(0, 0), (ranks - 1, ranks - 1)]

    def exchange(intra, cross):
        return lax.ppermute(intra, "cells", intra_pairs), lax.ppermute(cross, "cells", cross_pairs)

    field = shaped(members, unk, planes, rows, lanes)
    first_size = 2 * unk + unk * unk
    wells = well_cells.reshape(1, -1)
    dma = pltpu.SemaphoreType.DMA
    with jax.named_scope("start"):
        src, nxt, intra, cross, cpl, inv = pl.pallas_call(
            start_kernel,
            out_shape=(
                field,
                field,
                shaped(members, first_size, rows, lanes),
                shaped(members, first_size, rows, lanes),
                jax.ShapeDtypeStruct(coupling.shape, BF16),
                jax.ShapeDtypeStruct(diag_inverse.shape, BF16),
            ),
            in_specs=[SM] + [HB] * 5,
            out_specs=(VM,) * 6,
            scratch_shapes=[pltpu.VMEM(wells.shape, jnp.int32), pltpu.VMEM(well_misfit.shape, F32), dma((5,))],
            compiler_params=room(6),
        )(pos, wells, well_misfit, later_adjoint, coupling, diag_inverse)
    got_intra, got_cross = exchange(intra, cross)
    with jax.named_scope("select"):
        onehot, sens = pl.pallas_call(
            select_kernel,
            out_shape=(jax.ShapeDtypeStruct((nblk, count), BF16), jax.ShapeDtypeStruct(sensitivity.shape, BF16)),
            in_specs=[SM, HB, HB],
            out_specs=(VM, VM),
            scratch_shapes=[pltpu.VMEM(block_map.shape, jnp.int32), dma((2,))],
            compiler_params=room(10),
        )(pos, block_map, sensitivity)
    with jax.named_scope("middle"):
        nxt2, intra2, cross2 = pl.pallas_call(
            make_middle(ranks - 1),
            out_shape=(field, shaped(members, 2 * unk, rows, lanes), shaped(members, 2 * unk, rows, lanes)),
            in_specs=[SM] + [VM] * 8,
            out_specs=(VM, VM, VM),
            compiler_params=room(6),
        )(pos, src, nxt, intra, cross, got_intra, got_cross, cpl, inv)
    got_intra2, got_cross2 = exchange(intra2, cross2)
    with jax.named_scope("end"):
        adjoint, mine, other = pl.pallas_call(
            make_end(ranks - 1, nblk),
            out_shape=(field, shaped(nblk // 2, params), shaped(nblk // 2, params)),
            in_specs=[SM] + [VM] * 12,
            out_specs=(HB, VM, VM),
            scratch_shapes=[pltpu.VMEM(field.shape, F32), pltpu.VMEM((count, 2 * params), BF16), dma((1,))],
            compiler_params=room(16),
        )(
            pos, src, nxt2, got_intra, got_cross, intra2, cross2, got_intra2, got_cross2, cpl, inv, onehot, sens,
        )
    chips = ranks // 2
    half = mine + lax.ppermute(other, "cells", intra_pairs)
    same_core = [[core + 2 * chip for chip in range(chips)] for core in range(2)]
    parts = lax.all_to_all(
        half.reshape(chips, BLK_DEV, params), "cells", 0, 0, tiled=True, axis_index_groups=same_core
    )
    owned = jnp.sum(parts, axis=0)
    gradient = owned + lax.ppermute(owned, "ens", [(0, 1), (1, 0)])
    return (adjoint, gradient)


def solution(mesh):
    placed = (
        P("ens", None, "cells", None, None),
        P("ens", None, None, None, "cells", None, None),
        P("ens", None, None, "cells", None, None),
        P("ens", None, "cells", None, None, None),
        P(),
        P("ens", None, None),
        P("cells", None, None),
    )
    return jax.shard_map(
        body,
        mesh=mesh,
        in_specs=placed,
        out_specs=(P("ens", None, "cells", None, None), P("cells", None)),
        check_vma=False,
    )
```

```python
import jax
import jax.numpy as jnp
from jax import lax
from jax.experimental import pallas as pl
from jax.experimental.pallas import tpu as pltpu
from jax.sharding import PartitionSpec as P

BLK_DEV = 4
F32 = jnp.float32
BF16 = jnp.bfloat16


def shift_lanes(x, by):
    size = x.shape[2]
    lane = lax.broadcasted_iota(jnp.int32, x.shape, 2)
    keep = lane >= 1 if by == 1 else lane < size - 1
    return jnp.where(keep, pltpu.roll(x, by % size, 2), 0.0)


def shift_rows(x, by):
    size = x.shape[1]
    row = lax.broadcasted_iota(jnp.int32, x.shape, 1)
    keep = row >= 1 if by == 1 else row < size - 1
    return jnp.where(keep, pltpu.roll(x, by % size, 1), 0.0)


def products(cpl, m, k, a):
    unk = len(a)
    out = []
    for v in range(unk):
        total = cpl[m, k, 0, v].astype(F32) * a[0]
        for u in range(1, unk):
            total = total + cpl[m, k, u, v].astype(F32) * a[u]
        out.append(total)
    return out


def local_coupling(cpl, m, a):
    unk = len(a)
    terms = [products(cpl, m, k, a) for k in range(6)]
    inner, up, down = [], [], []
    for v in range(unk):
        t = [terms[k][v] for k in range(6)]
        planes = t[0].shape[0]
        zero = jnp.zeros_like(t[0][:1])
        total = jnp.concatenate([zero, t[0][: planes - 1]], axis=0)
        total = total + jnp.concatenate([t[1][1:], zero], axis=0)
        total = total + shift_rows(t[2], 1) + shift_rows(t[3], -1)
        total = total + shift_lanes(t[4], 1) + shift_lanes(t[5], -1)
        inner.append(total)
        up.append(t[0][planes - 1])
        down.append(t[1][0])
    return inner, up, down


def apply_inverse(inv, m, r):
    unk = len(r)
    out = []
    for v in range(unk):
        total = inv[m, 0, v].astype(F32) * r[0]
        for w in range(1, unk):
            total = total + inv[m, w, v].astype(F32) * r[w]
        out.append(total)
    return out


def plane_products(cpl, m, k, plane, a):
    unk = len(a)
    out = []
    for v in range(unk):
        total = cpl[m, k, 0, v, plane].astype(F32) * a[0]
        for u in range(1, unk):
            total = total + cpl[m, k, u, v, plane].astype(F32) * a[u]
        out.append(total)
    return out


def two_sweep_payload(cpl, inv, m, src, a):
    planes = a[0].shape[0]
    inner, up0, down0 = local_coupling(cpl, m, a)
    nxt = apply_inverse(inv, m, [s - b for s, b in zip(src, inner)])
    up1 = plane_products(cpl, m, 0, planes - 1, [x[planes - 1] for x in nxt])
    down1 = plane_products(cpl, m, 1, 0, [x[0] for x in nxt])
    return nxt, up0 + up1, down0 + down1


def transfer_blocks(cpl, inv, m, k, plane, unk):
    out = []
    for w in range(unk):
        for v in range(unk):
            total = inv[m, w, 0, plane].astype(F32) * cpl[m, k, 0, v, plane].astype(F32)
            for u in range(1, unk):
                total = total + inv[m, w, u, plane].astype(F32) * cpl[m, k, u, v, plane].astype(F32)
            out.append(total)
    return out


def split3(x):
    hi = x.astype(BF16)
    rest = x - hi.astype(F32)
    mid = rest.astype(BF16)
    lo = (rest - mid.astype(F32)).astype(BF16)
    return hi, mid, lo


def injected(wells, misfit, first, shape):
    members, unk, planes, rows, lanes = shape
    count = planes * rows * lanes
    nwell = wells.shape[1]
    place = wells[...] - first
    inside = (place >= 0) & (place < count)
    line = jnp.where(inside, place // lanes, -1)
    lane = jnp.where(inside, place % lanes, -1)
    lines = lax.broadcasted_iota(jnp.int32, (planes * rows, nwell), 0) == line
    onlane = (lax.broadcasted_iota(jnp.int32, (lanes, nwell), 0) == lane).astype(F32).astype(BF16)
    left = []
    for m in range(members):
        for u in range(unk):
            left.append(jnp.where(lines, misfit[m, u : u + 1, :], 0.0))
    stacked = jnp.concatenate(split3(jnp.concatenate(left, axis=0)), axis=0)
    full = lax.dot_general(stacked, onlane, (((1,), (1,)), ((), ())), preferred_element_type=F32)
    n = members * unk * planes * rows
    total = full[:n] + full[n : 2 * n] + full[2 * n :]
    return total.reshape(shape)


def place_kernel(pos, out):
    out[0] = pos[0]


def start_kernel(pos, wells, misfit, later, cpl_in, inv_in, src, nxt_out, intra_out, cross_out, cpl, inv):
    shape = src.shape
    members, unk, planes = shape[:3]
    cpl[...] = cpl_in[...]
    inv[...] = inv_in[...]
    even = pos[0] % 2 == 0
    count = planes * shape[3] * shape[4]
    src[...] = later[...] + injected(wells, misfit, pos[0] * count, shape)
    for m in range(members):
        s = [src[m, u] for u in range(unk)]
        a = apply_inverse(inv, m, s)
        nxt, up, down = two_sweep_payload(cpl, inv, m, s, a)
        up = up + transfer_blocks(cpl, inv, m, 0, planes - 1, unk)
        down = down + transfer_blocks(cpl, inv, m, 1, 0, unk)
        for u in range(unk):
            nxt_out[m, u] = nxt[u]
        for j in range(len(up)):
            intra_out[m, j] = jnp.where(even, up[j], down[j])
            cross_out[m, j] = jnp.where(even, down[j], up[j])


def incoming(pos, last, m, unk, blocks, sent_intra, sent_cross, got_intra, got_cross):
    even = pos[0] % 2 == 0
    has_cross = (pos[0] != 0) & (pos[0] != last)
    out = []
    sides = []
    for sent, got, block in ((sent_intra, got_intra, blocks[0]), (sent_cross, got_cross, blocks[1])):
        first = [got[m, v] for v in range(unk)]
        second = []
        for v in range(unk):
            total = got[m, unk + v]
            for w in range(unk):
                total = total - block[m, 2 * unk + w * unk + v] * sent[m, w]
            second.append(total)
        sides.append((first, second))
    for n in range(2):
        low, high = [], []
        for v in range(unk):
            near = sides[0][n][v]
            far = jnp.where(has_cross, sides[1][n][v], 0.0)
            low.append(jnp.where(even, far, near))
            high.append(jnp.where(even, near, far))
        out.append([jnp.stack([lo, hi], axis=0) for lo, hi in zip(low, high)])
    return out


def finish_two(cpl, inv, m, src, nxt, arrived):
    a1 = [x - d for x, d in zip(nxt, apply_inverse(inv, m, arrived[0]))]
    inner, _, _ = local_coupling(cpl, m, a1)
    return apply_inverse(inv, m, [s - b - p for s, b, p in zip(src, inner, arrived[1])])


def make_middle(last):
    def middle_kernel(pos, src, nxt, sent_intra, sent_cross, got_intra, got_cross, cpl, inv, nxt_out, intra_out, cross_out):
        members, unk = src.shape[:2]
        even = pos[0] % 2 == 0
        for m in range(members):
            arrived = incoming(
                pos, last, m, unk, (got_intra, got_cross), sent_intra, sent_cross, got_intra, got_cross
            )
            s = [src[m, u] for u in range(unk)]
            a = finish_two(cpl, inv, m, s, [nxt[m, u] for u in range(unk)], arrived)
            ahead, up, down = two_sweep_payload(cpl, inv, m, s, a)
            for u in range(unk):
                nxt_out[m, u] = ahead[u]
            for j in range(len(up)):
                intra_out[m, j] = jnp.where(even, up[j], down[j])
                cross_out[m, j] = jnp.where(even, down[j], up[j])

    return middle_kernel


def select_kernel(pos, bmap, onehot):
    rows, lanes = bmap.shape[1:]
    nblk = onehot.shape[0]
    core = pos[0] % 2
    slot = lax.broadcasted_iota(jnp.int32, (nblk, lanes), 0)
    half_rows = nblk // 2
    parity = jnp.where(slot < half_rows, core, 1 - core)
    within = jnp.where(slot < half_rows, slot, slot - half_rows)
    block = (within // BLK_DEV * 2 + parity) * BLK_DEV + within % BLK_DEV
    for g in range(bmap.shape[0] * rows):
        row = bmap[g // rows, g % rows : g % rows + 1, :]
        onehot[:, g * lanes : (g + 1) * lanes] = (block == row).astype(F32).astype(BF16)


def make_end(last, nblk):
    def end_kernel(
        pos, src, nxt, block_intra, block_cross, sent_intra, sent_cross, got_intra, got_cross, cpl, inv, onehot, sens,
        adj_out, mine_out, other_out, adj, grads, sems,
    ):
        members, unk, planes, rows, lanes = src.shape
        params = sens.shape[-1]
        groups = planes * rows
        half_rows = nblk // 2
        for m in range(members):
            arrived = incoming(
                pos, last, m, unk, (block_intra, block_cross), sent_intra, sent_cross, got_intra, got_cross
            )
            a = finish_two(
                cpl, inv, m, [src[m, u] for u in range(unk)], [nxt[m, u] for u in range(unk)], arrived
            )
            for u in range(unk):
                adj[m, u] = a[u]
        store = pltpu.make_async_copy(adj, adj_out, sems.at[0])
        store.start()
        turned = adj[...].reshape(members * unk * groups, lanes).T
        for g in range(groups):
            x, y = g // rows, g % rows
            total = None
            for m in range(members):
                for u in range(unk):
                    col = (m * unk + u) * groups + g
                    term = turned[:, col : col + 1] * sens[m, u, x, y].astype(F32)
                    total = term if total is None else total + term
            hi = total.astype(BF16)
            lo = (total - hi.astype(F32)).astype(BF16)
            grads[g * lanes : (g + 1) * lanes, :params] = hi
            grads[g * lanes : (g + 1) * lanes, params:] = lo
        both = jnp.dot(onehot[...], grads[...], preferred_element_type=F32)
        out = both[:, :params] + both[:, params:]
        mine_out[...] = out[:half_rows]
        other_out[...] = out[half_rows:]
        store.wait()

    return end_kernel


VM = pl.BlockSpec(memory_space=pltpu.VMEM)
SM = pl.BlockSpec(memory_space=pltpu.SMEM)
HB = pl.BlockSpec(memory_space=pltpu.HBM)
MIB = 1 << 20


def room(mib):
    return pltpu.CompilerParams(vmem_limit_bytes=mib * MIB)


def busy(flops):
    return pl.CostEstimate(flops=flops, bytes_accessed=0, transcendentals=0)


def shaped(*shape):
    return jax.ShapeDtypeStruct(shape, F32)


def body(later_adjoint, coupling, diag_inverse, sensitivity, well_cells, well_misfit, block_map):
    members, unk, planes, rows, lanes = later_adjoint.shape
    count = planes * rows * lanes
    params = sensitivity.shape[-1]
    ranks = lax.axis_size("cells")
    nblk = ranks * BLK_DEV
    pos = lax.axis_index("cells").astype(jnp.int32).reshape(1)
    intra_pairs = [(i, i ^ 1) for i in range(ranks)]
    cross_pairs = [(i, i + 1 if i % 2 else i - 1) for i in range(1, ranks - 1)] + [(0, 0), (ranks - 1, ranks - 1)]

    def exchange(intra, cross):
        return lax.ppermute(intra, "cells", intra_pairs), lax.ppermute(cross, "cells", cross_pairs)

    field = shaped(members, unk, planes, rows, lanes)
    first_size = 2 * unk + unk * unk
    wells = well_cells.reshape(1, -1)
    with jax.named_scope("place"):
        pos = pl.pallas_call(
            place_kernel,
            out_shape=jax.ShapeDtypeStruct((1,), jnp.int32),
            in_specs=[SM],
            out_specs=SM,
            compiler_params=room(1),
            cost_estimate=busy(1 << 31),
        )(pos)
    dma = pltpu.SemaphoreType.DMA
    with jax.named_scope("start"):
        src, nxt, intra, cross, cpl, inv = pl.pallas_call(
            start_kernel,
            out_shape=(
                field,
                field,
                shaped(members, first_size, rows, lanes),
                shaped(members, first_size, rows, lanes),
                jax.ShapeDtypeStruct(coupling.shape, BF16),
                jax.ShapeDtypeStruct(diag_inverse.shape, BF16),
            ),
            in_specs=[SM] + [VM] * 5,
            out_specs=(VM,) * 6,
            compiler_params=room(6),
        )(pos, wells, well_misfit, later_adjoint, coupling, diag_inverse)
    got_intra, got_cross = exchange(intra, cross)
    with jax.named_scope("select"):
        onehot = pl.pallas_call(
            select_kernel,
            out_shape=jax.ShapeDtypeStruct((nblk, count), BF16),
            in_specs=[SM, VM],
            out_specs=VM,
            compiler_params=room(6),
            cost_estimate=busy(1 << 24),
        )(pos, block_map)
    with jax.named_scope("middle"):
        nxt2, intra2, cross2 = pl.pallas_call(
            make_middle(ranks - 1),
            out_shape=(field, shaped(members, 2 * unk, rows, lanes), shaped(members, 2 * unk, rows, lanes)),
            in_specs=[SM] + [VM] * 8,
            out_specs=(VM, VM, VM),
            compiler_params=room(6),
        )(pos, src, nxt, intra, cross, got_intra, got_cross, cpl, inv)
    got_intra2, got_cross2 = exchange(intra2, cross2)
    with jax.named_scope("end"):
        adjoint, mine, other = pl.pallas_call(
            make_end(ranks - 1, nblk),
            out_shape=(field, shaped(nblk // 2, params), shaped(nblk // 2, params)),
            in_specs=[SM] + [VM] * 12,
            out_specs=(HB, VM, VM),
            scratch_shapes=[pltpu.VMEM(field.shape, F32), pltpu.VMEM((count, 2 * params), BF16), dma((1,))],
            compiler_params=room(16),
        )(
            pos, src, nxt2, got_intra, got_cross, intra2, cross2, got_intra2, got_cross2, cpl, inv, onehot, sensitivity,
        )
    chips = ranks // 2
    half = mine + lax.ppermute(other, "cells", intra_pairs)
    same_core = [[core + 2 * chip for chip in range(chips)] for core in range(2)]
    parts = lax.all_to_all(
        half.reshape(chips, BLK_DEV, params), "cells", 0, 0, tiled=True, axis_index_groups=same_core
    )
    owned = jnp.sum(parts, axis=0)
    gradient = owned + lax.ppermute(owned, "ens", [(0, 1), (1, 0)])
    return (adjoint, gradient)


def solution(mesh):
    placed = (
        P("ens", None, "cells", None, None),
        P("ens", None, None, None, "cells", None, None),
        P("ens", None, None, "cells", None, None),
        P("ens", None, "cells", None, None, None),
        P(),
        P("ens", None, None),
        P("cells", None, None),
    )
    return jax.shard_map(
        body,
        mesh=mesh,
        in_specs=placed,
        out_specs=(P("ens", None, "cells", None, None), P("cells", None)),
        check_vma=False,
    )
```

```python
import jax
import jax.numpy as jnp
from jax import lax
from jax.experimental import pallas as pl
from jax.experimental.pallas import tpu as pltpu
from jax.sharding import PartitionSpec as P

BLK_DEV = 4
F32 = jnp.float32
BF16 = jnp.bfloat16


def shift_lanes(x, by):
    size = x.shape[2]
    lane = lax.broadcasted_iota(jnp.int32, x.shape, 2)
    keep = lane >= 1 if by == 1 else lane < size - 1
    return jnp.where(keep, pltpu.roll(x, by % size, 2), 0.0)


def shift_rows(x, by):
    size = x.shape[1]
    row = lax.broadcasted_iota(jnp.int32, x.shape, 1)
    keep = row >= 1 if by == 1 else row < size - 1
    return jnp.where(keep, pltpu.roll(x, by % size, 1), 0.0)


def products(cpl, m, k, a):
    unk = len(a)
    out = []
    for v in range(unk):
        total = cpl[m, k, 0, v].astype(F32) * a[0]
        for u in range(1, unk):
            total = total + cpl[m, k, u, v].astype(F32) * a[u]
        out.append(total)
    return out


def local_coupling(cpl, m, a):
    unk = len(a)
    terms = [products(cpl, m, k, a) for k in range(6)]
    inner, up, down = [], [], []
    for v in range(unk):
        t = [terms[k][v] for k in range(6)]
        planes = t[0].shape[0]
        zero = jnp.zeros_like(t[0][:1])
        total = jnp.concatenate([zero, t[0][: planes - 1]], axis=0)
        total = total + jnp.concatenate([t[1][1:], zero], axis=0)
        total = total + shift_rows(t[2], 1) + shift_rows(t[3], -1)
        total = total + shift_lanes(t[4], 1) + shift_lanes(t[5], -1)
        inner.append(total)
        up.append(t[0][planes - 1])
        down.append(t[1][0])
    return inner, up, down


def apply_inverse(inv, m, r):
    unk = len(r)
    out = []
    for v in range(unk):
        total = inv[m, 0, v].astype(F32) * r[0]
        for w in range(1, unk):
            total = total + inv[m, w, v].astype(F32) * r[w]
        out.append(total)
    return out


def plane_products(cpl, m, k, plane, a):
    unk = len(a)
    out = []
    for v in range(unk):
        total = cpl[m, k, 0, v, plane].astype(F32) * a[0]
        for u in range(1, unk):
            total = total + cpl[m, k, u, v, plane].astype(F32) * a[u]
        out.append(total)
    return out


def two_sweep_payload(cpl, inv, m, src, a):
    planes = a[0].shape[0]
    inner, up0, down0 = local_coupling(cpl, m, a)
    nxt = apply_inverse(inv, m, [s - b for s, b in zip(src, inner)])
    up1 = plane_products(cpl, m, 0, planes - 1, [x[planes - 1] for x in nxt])
    down1 = plane_products(cpl, m, 1, 0, [x[0] for x in nxt])
    return nxt, up0 + up1, down0 + down1


def transfer_blocks(cpl, inv, m, k, plane, unk):
    out = []
    for w in range(unk):
        for v in range(unk):
            total = inv[m, w, 0, plane].astype(F32) * cpl[m, k, 0, v, plane].astype(F32)
            for u in range(1, unk):
                total = total + inv[m, w, u, plane].astype(F32) * cpl[m, k, u, v, plane].astype(F32)
            out.append(total)
    return out


def split3(x):
    hi = x.astype(BF16)
    rest = x - hi.astype(F32)
    mid = rest.astype(BF16)
    lo = (rest - mid.astype(F32)).astype(BF16)
    return hi, mid, lo


def injected(wells, misfit, first, shape):
    members, unk, planes, rows, lanes = shape
    count = planes * rows * lanes
    nwell = wells.shape[1]
    place = wells[...] - first
    inside = (place >= 0) & (place < count)
    line = jnp.where(inside, place // lanes, -1)
    lane = jnp.where(inside, place % lanes, -1)
    lines = lax.broadcasted_iota(jnp.int32, (planes * rows, nwell), 0) == line
    onlane = (lax.broadcasted_iota(jnp.int32, (lanes, nwell), 0) == lane).astype(F32).astype(BF16)
    left = []
    for m in range(members):
        for u in range(unk):
            left.append(jnp.where(lines, misfit[m, u : u + 1, :], 0.0))
    stacked = jnp.concatenate(split3(jnp.concatenate(left, axis=0)), axis=0)
    full = lax.dot_general(stacked, onlane, (((1,), (1,)), ((), ())), preferred_element_type=F32)
    n = members * unk * planes * rows
    total = full[:n] + full[n : 2 * n] + full[2 * n :]
    return total.reshape(shape)


def first_kernel(out):
    out[...] = jnp.zeros_like(out)


def start_kernel(pos, _, wells, misfit, later, cpl_in, inv_in, src, nxt_out, intra_out, cross_out, cpl, inv):
    shape = src.shape
    members, unk, planes = shape[:3]
    cpl[...] = cpl_in[...]
    inv[...] = inv_in[...]
    even = pos[0] % 2 == 0
    count = planes * shape[3] * shape[4]
    src[...] = later[...] + injected(wells, misfit, pos[0] * count, shape)
    for m in range(members):
        s = [src[m, u] for u in range(unk)]
        a = apply_inverse(inv, m, s)
        nxt, up, down = two_sweep_payload(cpl, inv, m, s, a)
        up = up + transfer_blocks(cpl, inv, m, 0, planes - 1, unk)
        down = down + transfer_blocks(cpl, inv, m, 1, 0, unk)
        for u in range(unk):
            nxt_out[m, u] = nxt[u]
        for j in range(len(up)):
            intra_out[m, j] = jnp.where(even, up[j], down[j])
            cross_out[m, j] = jnp.where(even, down[j], up[j])


def incoming(pos, last, m, unk, blocks, sent_intra, sent_cross, got_intra, got_cross):
    even = pos[0] % 2 == 0
    has_cross = (pos[0] != 0) & (pos[0] != last)
    out = []
    sides = []
    for sent, got, block in ((sent_intra, got_intra, blocks[0]), (sent_cross, got_cross, blocks[1])):
        first = [got[m, v] for v in range(unk)]
        second = []
        for v in range(unk):
            total = got[m, unk + v]
            for w in range(unk):
                total = total - block[m, 2 * unk + w * unk + v] * sent[m, w]
            second.append(total)
        sides.append((first, second))
    for n in range(2):
        low, high = [], []
        for v in range(unk):
            near = sides[0][n][v]
            far = jnp.where(has_cross, sides[1][n][v], 0.0)
            low.append(jnp.where(even, far, near))
            high.append(jnp.where(even, near, far))
        out.append([jnp.stack([lo, hi], axis=0) for lo, hi in zip(low, high)])
    return out


def finish_two(cpl, inv, m, src, nxt, arrived):
    a1 = [x - d for x, d in zip(nxt, apply_inverse(inv, m, arrived[0]))]
    inner, _, _ = local_coupling(cpl, m, a1)
    return apply_inverse(inv, m, [s - b - p for s, b, p in zip(src, inner, arrived[1])])


def make_middle(last):
    def middle_kernel(pos, src, nxt, sent_intra, sent_cross, got_intra, got_cross, cpl, inv, nxt_out, intra_out, cross_out):
        members, unk = src.shape[:2]
        even = pos[0] % 2 == 0
        for m in range(members):
            arrived = incoming(
                pos, last, m, unk, (got_intra, got_cross), sent_intra, sent_cross, got_intra, got_cross
            )
            s = [src[m, u] for u in range(unk)]
            a = finish_two(cpl, inv, m, s, [nxt[m, u] for u in range(unk)], arrived)
            ahead, up, down = two_sweep_payload(cpl, inv, m, s, a)
            for u in range(unk):
                nxt_out[m, u] = ahead[u]
            for j in range(len(up)):
                intra_out[m, j] = jnp.where(even, up[j], down[j])
                cross_out[m, j] = jnp.where(even, down[j], up[j])

    return middle_kernel


def select_kernel(pos, bmap, onehot):
    rows, lanes = bmap.shape[1:]
    nblk = onehot.shape[0]
    core = pos[0] % 2
    slot = lax.broadcasted_iota(jnp.int32, (nblk, lanes), 0)
    half_rows = nblk // 2
    parity = jnp.where(slot < half_rows, core, 1 - core)
    within = jnp.where(slot < half_rows, slot, slot - half_rows)
    block = (within // BLK_DEV * 2 + parity) * BLK_DEV + within % BLK_DEV
    for g in range(bmap.shape[0] * rows):
        row = bmap[g // rows, g % rows : g % rows + 1, :]
        onehot[:, g * lanes : (g + 1) * lanes] = (block == row).astype(F32).astype(BF16)


def make_end(last, nblk):
    def end_kernel(
        pos, src, nxt, block_intra, block_cross, sent_intra, sent_cross, got_intra, got_cross, cpl, inv, onehot, sens,
        adj_out, mine_out, other_out, adj, grads, sems,
    ):
        members, unk, planes, rows, lanes = src.shape
        params = sens.shape[-1]
        groups = planes * rows
        half_rows = nblk // 2
        for m in range(members):
            arrived = incoming(
                pos, last, m, unk, (block_intra, block_cross), sent_intra, sent_cross, got_intra, got_cross
            )
            a = finish_two(
                cpl, inv, m, [src[m, u] for u in range(unk)], [nxt[m, u] for u in range(unk)], arrived
            )
            for u in range(unk):
                adj[m, u] = a[u]
        store = pltpu.make_async_copy(adj, adj_out, sems.at[0])
        store.start()
        turned = adj[...].reshape(members * unk * groups, lanes).T
        for g in range(groups):
            x, y = g // rows, g % rows
            total = None
            for m in range(members):
                for u in range(unk):
                    col = (m * unk + u) * groups + g
                    term = turned[:, col : col + 1] * sens[m, u, x, y].astype(F32)
                    total = term if total is None else total + term
            hi = total.astype(BF16)
            lo = (total - hi.astype(F32)).astype(BF16)
            grads[g * lanes : (g + 1) * lanes, :params] = hi
            grads[g * lanes : (g + 1) * lanes, params:] = lo
        both = jnp.dot(onehot[...], grads[...], preferred_element_type=F32)
        out = both[:, :params] + both[:, params:]
        mine_out[...] = out[:half_rows]
        other_out[...] = out[half_rows:]
        store.wait()

    return end_kernel


VM = pl.BlockSpec(memory_space=pltpu.VMEM)
SM = pl.BlockSpec(memory_space=pltpu.SMEM)
HB = pl.BlockSpec(memory_space=pltpu.HBM)
MIB = 1 << 20


def room(mib):
    return pltpu.CompilerParams(vmem_limit_bytes=mib * MIB)


def busy(flops):
    return pl.CostEstimate(flops=flops, bytes_accessed=0, transcendentals=0)


def shaped(*shape):
    return jax.ShapeDtypeStruct(shape, F32)


def body(later_adjoint, coupling, diag_inverse, sensitivity, well_cells, well_misfit, block_map):
    members, unk, planes, rows, lanes = later_adjoint.shape
    count = planes * rows * lanes
    params = sensitivity.shape[-1]
    ranks = lax.axis_size("cells")
    nblk = ranks * BLK_DEV
    pos = lax.axis_index("cells").astype(jnp.int32).reshape(1)
    intra_pairs = [(i, i ^ 1) for i in range(ranks)]
    cross_pairs = [(i, i + 1 if i % 2 else i - 1) for i in range(1, ranks - 1)] + [(0, 0), (ranks - 1, ranks - 1)]

    def exchange(intra, cross):
        return lax.ppermute(intra, "cells", intra_pairs), lax.ppermute(cross, "cells", cross_pairs)

    field = shaped(members, unk, planes, rows, lanes)
    first_size = 2 * unk + unk * unk
    wells = well_cells.reshape(1, -1)
    dma = pltpu.SemaphoreType.DMA
    with jax.named_scope("first"):
        token = pl.pallas_call(
            first_kernel,
            out_shape=shaped(8, 128),
            out_specs=VM,
            compiler_params=room(1),
            cost_estimate=busy(1 << 31),
        )()
    with jax.named_scope("start"):
        src, nxt, intra, cross, cpl, inv = pl.pallas_call(
            start_kernel,
            out_shape=(
                field,
                field,
                shaped(members, first_size, rows, lanes),
                shaped(members, first_size, rows, lanes),
                jax.ShapeDtypeStruct(coupling.shape, BF16),
                jax.ShapeDtypeStruct(diag_inverse.shape, BF16),
            ),
            in_specs=[SM] + [VM] * 6,
            out_specs=(VM,) * 6,
            compiler_params=room(6),
        )(pos, token, wells, well_misfit, later_adjoint, coupling, diag_inverse)
    got_intra, got_cross = exchange(intra, cross)
    with jax.named_scope("select"):
        onehot = pl.pallas_call(
            select_kernel,
            out_shape=jax.ShapeDtypeStruct((nblk, count), BF16),
            in_specs=[SM, VM],
            out_specs=VM,
            compiler_params=room(6),
            cost_estimate=busy(1 << 24),
        )(pos, block_map)
    with jax.named_scope("middle"):
        nxt2, intra2, cross2 = pl.pallas_call(
            make_middle(ranks - 1),
            out_shape=(field, shaped(members, 2 * unk, rows, lanes), shaped(members, 2 * unk, rows, lanes)),
            in_specs=[SM] + [VM] * 8,
            out_specs=(VM, VM, VM),
            compiler_params=room(6),
        )(pos, src, nxt, intra, cross, got_intra, got_cross, cpl, inv)
    got_intra2, got_cross2 = exchange(intra2, cross2)
    with jax.named_scope("end"):
        adjoint, mine, other = pl.pallas_call(
            make_end(ranks - 1, nblk),
            out_shape=(field, shaped(nblk // 2, params), shaped(nblk // 2, params)),
            in_specs=[SM] + [VM] * 12,
            out_specs=(HB, VM, VM),
            scratch_shapes=[pltpu.VMEM(field.shape, F32), pltpu.VMEM((count, 2 * params), BF16), dma((1,))],
            compiler_params=room(16),
        )(
            pos, src, nxt2, got_intra, got_cross, intra2, cross2, got_intra2, got_cross2, cpl, inv, onehot, sensitivity,
        )
    chips = ranks // 2
    half = mine + lax.ppermute(other, "cells", intra_pairs)
    same_core = [[core + 2 * chip for chip in range(chips)] for core in range(2)]
    parts = lax.all_to_all(
        half.reshape(chips, BLK_DEV, params), "cells", 0, 0, tiled=True, axis_index_groups=same_core
    )
    owned = jnp.sum(parts, axis=0)
    gradient = owned + lax.ppermute(owned, "ens", [(0, 1), (1, 0)])
    return (adjoint, gradient)


def solution(mesh):
    placed = (
        P("ens", None, "cells", None, None),
        P("ens", None, None, None, "cells", None, None),
        P("ens", None, None, "cells", None, None),
        P("ens", None, "cells", None, None, None),
        P(),
        P("ens", None, None),
        P("cells", None, None),
    )
    return jax.shard_map(
        body,
        mesh=mesh,
        in_specs=placed,
        out_specs=(P("ens", None, "cells", None, None), P("cells", None)),
        check_vma=False,
    )
```

```python
import jax
import jax.numpy as jnp
from jax import lax
from jax.experimental import pallas as pl
from jax.experimental.pallas import tpu as pltpu
from jax.sharding import PartitionSpec as P

BLK_DEV = 4
F32 = jnp.float32
BF16 = jnp.bfloat16


def shift_lanes(x, by):
    size = x.shape[2]
    lane = lax.broadcasted_iota(jnp.int32, x.shape, 2)
    keep = lane >= 1 if by == 1 else lane < size - 1
    return jnp.where(keep, pltpu.roll(x, by % size, 2), 0.0)


def shift_rows(x, by):
    size = x.shape[1]
    row = lax.broadcasted_iota(jnp.int32, x.shape, 1)
    keep = row >= 1 if by == 1 else row < size - 1
    return jnp.where(keep, pltpu.roll(x, by % size, 1), 0.0)


def products(cpl, m, k, a):
    unk = len(a)
    out = []
    for v in range(unk):
        total = cpl[m, k, 0, v].astype(F32) * a[0]
        for u in range(1, unk):
            total = total + cpl[m, k, u, v].astype(F32) * a[u]
        out.append(total)
    return out


def local_coupling(cpl, m, a):
    unk = len(a)
    terms = [products(cpl, m, k, a) for k in range(6)]
    inner, up, down = [], [], []
    for v in range(unk):
        t = [terms[k][v] for k in range(6)]
        planes = t[0].shape[0]
        zero = jnp.zeros_like(t[0][:1])
        total = jnp.concatenate([zero, t[0][: planes - 1]], axis=0)
        total = total + jnp.concatenate([t[1][1:], zero], axis=0)
        total = total + shift_rows(t[2], 1) + shift_rows(t[3], -1)
        total = total + shift_lanes(t[4], 1) + shift_lanes(t[5], -1)
        inner.append(total)
        up.append(t[0][planes - 1])
        down.append(t[1][0])
    return inner, up, down


def apply_inverse(inv, m, r):
    unk = len(r)
    out = []
    for v in range(unk):
        total = inv[m, 0, v].astype(F32) * r[0]
        for w in range(1, unk):
            total = total + inv[m, w, v].astype(F32) * r[w]
        out.append(total)
    return out


def plane_products(cpl, m, k, plane, a):
    unk = len(a)
    out = []
    for v in range(unk):
        total = cpl[m, k, 0, v, plane].astype(F32) * a[0]
        for u in range(1, unk):
            total = total + cpl[m, k, u, v, plane].astype(F32) * a[u]
        out.append(total)
    return out


def two_sweep_payload(cpl, inv, m, src, a):
    planes = a[0].shape[0]
    inner, up0, down0 = local_coupling(cpl, m, a)
    nxt = apply_inverse(inv, m, [s - b for s, b in zip(src, inner)])
    up1 = plane_products(cpl, m, 0, planes - 1, [x[planes - 1] for x in nxt])
    down1 = plane_products(cpl, m, 1, 0, [x[0] for x in nxt])
    return nxt, up0 + up1, down0 + down1


def transfer_blocks(cpl, inv, m, k, plane, unk):
    out = []
    for w in range(unk):
        for v in range(unk):
            total = inv[m, w, 0, plane].astype(F32) * cpl[m, k, 0, v, plane].astype(F32)
            for u in range(1, unk):
                total = total + inv[m, w, u, plane].astype(F32) * cpl[m, k, u, v, plane].astype(F32)
            out.append(total)
    return out


def split3(x):
    hi = x.astype(BF16)
    rest = x - hi.astype(F32)
    mid = rest.astype(BF16)
    lo = (rest - mid.astype(F32)).astype(BF16)
    return hi, mid, lo


def injected(wells, misfit, first, shape):
    members, unk, planes, rows, lanes = shape
    count = planes * rows * lanes
    nwell = wells.shape[1]
    place = wells[...] - first
    inside = (place >= 0) & (place < count)
    line = jnp.where(inside, place // lanes, -1)
    lane = jnp.where(inside, place % lanes, -1)
    lines = lax.broadcasted_iota(jnp.int32, (planes * rows, nwell), 0) == line
    onlane = (lax.broadcasted_iota(jnp.int32, (lanes, nwell), 0) == lane).astype(F32).astype(BF16)
    left = []
    for m in range(members):
        for u in range(unk):
            left.append(jnp.where(lines, misfit[m, u : u + 1, :], 0.0))
    stacked = jnp.concatenate(split3(jnp.concatenate(left, axis=0)), axis=0)
    full = lax.dot_general(stacked, onlane, (((1,), (1,)), ((), ())), preferred_element_type=F32)
    n = members * unk * planes * rows
    total = full[:n] + full[n : 2 * n] + full[2 * n :]
    return total.reshape(shape)


def first_kernel(out):
    out[...] = jnp.zeros_like(out)


def start_kernel(pos, _, wells, misfit, later, cpl_in, inv_in, src, nxt_out, intra_out, cross_out, cpl, inv):
    shape = src.shape
    members, unk, planes = shape[:3]
    cpl[...] = cpl_in[...]
    inv[...] = inv_in[...]
    even = pos[0] % 2 == 0
    count = planes * shape[3] * shape[4]
    src[...] = later[...] + injected(wells, misfit, pos[0] * count, shape)
    for m in range(members):
        s = [src[m, u] for u in range(unk)]
        a = apply_inverse(inv, m, s)
        nxt, up, down = two_sweep_payload(cpl, inv, m, s, a)
        up = up + transfer_blocks(cpl, inv, m, 0, planes - 1, unk)
        down = down + transfer_blocks(cpl, inv, m, 1, 0, unk)
        for u in range(unk):
            nxt_out[m, u] = nxt[u]
        for j in range(len(up)):
            intra_out[m, j] = jnp.where(even, up[j], down[j])
            cross_out[m, j] = jnp.where(even, down[j], up[j])


def incoming(pos, last, m, unk, near, far):
    even = pos[0] % 2 == 0
    has_cross = (pos[0] != 0) & (pos[0] != last)
    sides = []
    for sent, got, block in (near, far):
        first = [got(m, v) for v in range(unk)]
        second = []
        for v in range(unk):
            total = got(m, unk + v)
            for w in range(unk):
                total = total - block(m, 2 * unk + w * unk + v) * sent(m, w)
            second.append(total)
        sides.append((first, second))
    out = []
    for n in range(2):
        low, high = [], []
        for v in range(unk):
            near_v = sides[0][n][v]
            far_v = jnp.where(has_cross, sides[1][n][v], 0.0)
            low.append(jnp.where(even, far_v, near_v))
            high.append(jnp.where(even, near_v, far_v))
        out.append([jnp.stack([lo, hi], axis=0) for lo, hi in zip(low, high)])
    return out


def reader(ref):
    return lambda m, j: ref[m, j]


def either(pos, if_even, if_odd):
    even = pos[0] % 2 == 0
    return lambda m, j: jnp.where(even, if_even[m, j], if_odd[m, j])


def finish_two(cpl, inv, m, src, nxt, arrived):
    a1 = [x - d for x, d in zip(nxt, apply_inverse(inv, m, arrived[0]))]
    inner, _, _ = local_coupling(cpl, m, a1)
    return apply_inverse(inv, m, [s - b - p for s, b, p in zip(src, inner, arrived[1])])


def advance(pos, last, src, nxt, sent_near, sent_far, got_near, got_far, cpl, inv, nxt_out, near_out, far_out):
    members, unk = src.shape[:2]
    even = pos[0] % 2 == 0
    near = (reader(sent_near), reader(got_near), reader(got_near))
    far = (reader(sent_far), reader(got_far), reader(got_far))
    for m in range(members):
        arrived = incoming(pos, last, m, unk, near, far)
        s = [src[m, u] for u in range(unk)]
        a = finish_two(cpl, inv, m, s, [nxt[m, u] for u in range(unk)], arrived)
        ahead, up, down = two_sweep_payload(cpl, inv, m, s, a)
        for u in range(unk):
            nxt_out[m, u] = ahead[u]
        for j in range(len(up)):
            near_out[m, j] = jnp.where(even, up[j], down[j])
            far_out[m, j] = jnp.where(even, down[j], up[j])


def make_even_middle(last):
    def even_middle(*refs):
        pos, outs = refs[0], refs[9:]

        @pl.when(pos[0] % 2 == 0)
        def _():
            advance(pos, last, *refs[1:9], *outs)

        @pl.when(pos[0] % 2 == 1)
        def _():
            for out in outs:
                out[...] = jnp.zeros_like(out)

    return even_middle


def make_odd_middle(last):
    def odd_middle(*refs):
        pos, (nxt_even, near_even), outs = refs[0], refs[9:11], refs[11:]

        @pl.when(pos[0] % 2 == 1)
        def _():
            advance(pos, last, *refs[1:9], *outs)

        @pl.when(pos[0] % 2 == 0)
        def _():
            outs[0][...] = nxt_even[...]
            outs[1][...] = near_even[...]
            outs[2][...] = jnp.zeros_like(outs[2])

    return odd_middle


def select_kernel(pos, bmap, onehot):
    rows, lanes = bmap.shape[1:]
    nblk = onehot.shape[0]
    core = pos[0] % 2
    slot = lax.broadcasted_iota(jnp.int32, (nblk, lanes), 0)
    half_rows = nblk // 2
    parity = jnp.where(slot < half_rows, core, 1 - core)
    within = jnp.where(slot < half_rows, slot, slot - half_rows)
    block = (within // BLK_DEV * 2 + parity) * BLK_DEV + within % BLK_DEV
    for g in range(bmap.shape[0] * rows):
        row = bmap[g // rows, g % rows : g % rows + 1, :]
        onehot[:, g * lanes : (g + 1) * lanes] = (block == row).astype(F32).astype(BF16)


def make_end(last, nblk):
    def end_kernel(
        pos, src, nxt, block_near, block_even, block_odd, sent_near, sent_even, sent_odd, got_near, got_even, got_odd,
        cpl, inv, onehot, sens, adj_out, mine_out, other_out, adj, grads, sems,
    ):
        members, unk, planes, rows, lanes = src.shape
        params = sens.shape[-1]
        groups = planes * rows
        half_rows = nblk // 2
        near = (reader(sent_near), reader(got_near), reader(block_near))
        far = (
            either(pos, sent_even, sent_odd), either(pos, got_even, got_odd), either(pos, block_even, block_odd),
        )
        for m in range(members):
            arrived = incoming(pos, last, m, unk, near, far)
            a = finish_two(
                cpl, inv, m, [src[m, u] for u in range(unk)], [nxt[m, u] for u in range(unk)], arrived
            )
            for u in range(unk):
                adj[m, u] = a[u]
        store = pltpu.make_async_copy(adj, adj_out, sems.at[0])
        store.start()
        turned = adj[...].reshape(members * unk * groups, lanes).T
        for g in range(groups):
            x, y = g // rows, g % rows
            total = None
            for m in range(members):
                for u in range(unk):
                    col = (m * unk + u) * groups + g
                    term = turned[:, col : col + 1] * sens[m, u, x, y].astype(F32)
                    total = term if total is None else total + term
            hi = total.astype(BF16)
            lo = (total - hi.astype(F32)).astype(BF16)
            grads[g * lanes : (g + 1) * lanes, :params] = hi
            grads[g * lanes : (g + 1) * lanes, params:] = lo
        both = jnp.dot(onehot[...], grads[...], preferred_element_type=F32)
        out = both[:, :params] + both[:, params:]
        mine_out[...] = out[:half_rows]
        other_out[...] = out[half_rows:]
        store.wait()

    return end_kernel


VM = pl.BlockSpec(memory_space=pltpu.VMEM)
SM = pl.BlockSpec(memory_space=pltpu.SMEM)
HB = pl.BlockSpec(memory_space=pltpu.HBM)
MIB = 1 << 20


def room(mib):
    return pltpu.CompilerParams(vmem_limit_bytes=mib * MIB)


def busy(flops):
    return pl.CostEstimate(flops=flops, bytes_accessed=0, transcendentals=0)


def shaped(*shape):
    return jax.ShapeDtypeStruct(shape, F32)


def body(later_adjoint, coupling, diag_inverse, sensitivity, well_cells, well_misfit, block_map):
    members, unk, planes, rows, lanes = later_adjoint.shape
    count = planes * rows * lanes
    params = sensitivity.shape[-1]
    ranks = lax.axis_size("cells")
    nblk = ranks * BLK_DEV
    pos = lax.axis_index("cells").astype(jnp.int32).reshape(1)
    intra_pairs = [(i, i ^ 1) for i in range(ranks)]
    up_pairs = [(i, i + 1) for i in range(1, ranks - 1, 2)]
    down_pairs = [(i + 1, i) for i in range(1, ranks - 1, 2)]

    field = shaped(members, unk, planes, rows, lanes)
    first_size = 2 * unk + unk * unk
    wells = well_cells.reshape(1, -1)
    dma = pltpu.SemaphoreType.DMA
    with jax.named_scope("first"):
        token = pl.pallas_call(
            first_kernel,
            out_shape=shaped(8, 128),
            out_specs=VM,
            compiler_params=room(1),
            cost_estimate=busy(1 << 31),
        )()
    with jax.named_scope("start"):
        src, nxt, near, far, cpl, inv = pl.pallas_call(
            start_kernel,
            out_shape=(
                field,
                field,
                shaped(members, first_size, rows, lanes),
                shaped(members, first_size, rows, lanes),
                jax.ShapeDtypeStruct(coupling.shape, BF16),
                jax.ShapeDtypeStruct(diag_inverse.shape, BF16),
            ),
            in_specs=[SM] + [VM] * 6,
            out_specs=(VM,) * 6,
            compiler_params=room(6),
        )(pos, token, wells, well_misfit, later_adjoint, coupling, diag_inverse)
    got_near = lax.ppermute(near, "cells", intra_pairs)
    got_up = lax.ppermute(far, "cells", up_pairs)
    got_down = lax.ppermute(far, "cells", down_pairs)
    with jax.named_scope("select"):
        onehot = pl.pallas_call(
            select_kernel,
            out_shape=jax.ShapeDtypeStruct((nblk, count), BF16),
            in_specs=[SM, VM],
            out_specs=VM,
            compiler_params=room(6),
            cost_estimate=busy(1 << 24),
        )(pos, block_map)
    wide = shaped(members, 2 * unk, rows, lanes)
    with jax.named_scope("even"):
        nxt_even, near_even, far_even = pl.pallas_call(
            make_even_middle(ranks - 1),
            out_shape=(field, wide, wide),
            in_specs=[SM] + [VM] * 8,
            out_specs=(VM, VM, VM),
            compiler_params=room(6),
        )(pos, src, nxt, near, far, got_near, got_up, cpl, inv)
    got_down2 = lax.ppermute(far_even, "cells", down_pairs)
    with jax.named_scope("odd"):
        nxt2, near2, far_odd = pl.pallas_call(
            make_odd_middle(ranks - 1),
            out_shape=(field, wide, wide),
            in_specs=[SM] + [VM] * 10,
            out_specs=(VM, VM, VM),
            compiler_params=room(6),
        )(pos, src, nxt, near, far, got_near, got_down, cpl, inv, nxt_even, near_even)
    got_near2 = lax.ppermute(near2, "cells", intra_pairs)
    got_up2 = lax.ppermute(far_odd, "cells", up_pairs)
    with jax.named_scope("end"):
        adjoint, mine, other = pl.pallas_call(
            make_end(ranks - 1, nblk),
            out_shape=(field, shaped(nblk // 2, params), shaped(nblk // 2, params)),
            in_specs=[SM] + [VM] * 15,
            out_specs=(HB, VM, VM),
            scratch_shapes=[pltpu.VMEM(field.shape, F32), pltpu.VMEM((count, 2 * params), BF16), dma((1,))],
            compiler_params=room(16),
        )(
            pos, src, nxt2, got_near, got_up, got_down, near2, far_even, far_odd, got_near2, got_up2, got_down2,
            cpl, inv, onehot, sensitivity,
        )
    chips = ranks // 2
    half = mine + lax.ppermute(other, "cells", intra_pairs)
    same_core = [[core + 2 * chip for chip in range(chips)] for core in range(2)]
    parts = lax.all_to_all(
        half.reshape(chips, BLK_DEV, params), "cells", 0, 0, tiled=True, axis_index_groups=same_core
    )
    owned = jnp.sum(parts, axis=0)
    gradient = owned + lax.ppermute(owned, "ens", [(0, 1), (1, 0)])
    return (adjoint, gradient)


def solution(mesh):
    placed = (
        P("ens", None, "cells", None, None),
        P("ens", None, None, None, "cells", None, None),
        P("ens", None, None, "cells", None, None),
        P("ens", None, "cells", None, None, None),
        P(),
        P("ens", None, None),
        P("cells", None, None),
    )
    return jax.shard_map(
        body,
        mesh=mesh,
        in_specs=placed,
        out_specs=(P("ens", None, "cells", None, None), P("cells", None)),
        check_vma=False,
    )
```

```python
import jax
import jax.numpy as jnp
from jax import lax
from jax.experimental import pallas as pl
from jax.experimental.pallas import tpu as pltpu
from jax.sharding import PartitionSpec as P

BLK_DEV = 4
F32 = jnp.float32
BF16 = jnp.bfloat16


def shift_lanes(x, by):
    size = x.shape[2]
    lane = lax.broadcasted_iota(jnp.int32, x.shape, 2)
    keep = lane >= 1 if by == 1 else lane < size - 1
    return jnp.where(keep, pltpu.roll(x, by % size, 2), 0.0)


def shift_rows(x, by):
    size = x.shape[1]
    row = lax.broadcasted_iota(jnp.int32, x.shape, 1)
    keep = row >= 1 if by == 1 else row < size - 1
    return jnp.where(keep, pltpu.roll(x, by % size, 1), 0.0)


def products(cpl, m, k, a):
    unk = len(a)
    out = []
    for v in range(unk):
        total = cpl[m, k, 0, v].astype(F32) * a[0]
        for u in range(1, unk):
            total = total + cpl[m, k, u, v].astype(F32) * a[u]
        out.append(total)
    return out


def local_coupling(cpl, m, a):
    unk = len(a)
    terms = [products(cpl, m, k, a) for k in range(6)]
    inner, up, down = [], [], []
    for v in range(unk):
        t = [terms[k][v] for k in range(6)]
        planes = t[0].shape[0]
        zero = jnp.zeros_like(t[0][:1])
        total = jnp.concatenate([zero, t[0][: planes - 1]], axis=0)
        total = total + jnp.concatenate([t[1][1:], zero], axis=0)
        total = total + shift_rows(t[2], 1) + shift_rows(t[3], -1)
        total = total + shift_lanes(t[4], 1) + shift_lanes(t[5], -1)
        inner.append(total)
        up.append(t[0][planes - 1])
        down.append(t[1][0])
    return inner, up, down


def apply_inverse(inv, m, r):
    unk = len(r)
    out = []
    for v in range(unk):
        total = inv[m, 0, v].astype(F32) * r[0]
        for w in range(1, unk):
            total = total + inv[m, w, v].astype(F32) * r[w]
        out.append(total)
    return out


def plane_products(cpl, m, k, plane, a):
    unk = len(a)
    out = []
    for v in range(unk):
        total = cpl[m, k, 0, v, plane].astype(F32) * a[0]
        for u in range(1, unk):
            total = total + cpl[m, k, u, v, plane].astype(F32) * a[u]
        out.append(total)
    return out


def two_sweep_payload(cpl, inv, m, src, a):
    planes = a[0].shape[0]
    inner, up0, down0 = local_coupling(cpl, m, a)
    nxt = apply_inverse(inv, m, [s - b for s, b in zip(src, inner)])
    up1 = plane_products(cpl, m, 0, planes - 1, [x[planes - 1] for x in nxt])
    down1 = plane_products(cpl, m, 1, 0, [x[0] for x in nxt])
    return nxt, up0 + up1, down0 + down1


def transfer_blocks(cpl, inv, m, k, plane, unk):
    out = []
    for w in range(unk):
        for v in range(unk):
            total = inv[m, w, 0, plane].astype(F32) * cpl[m, k, 0, v, plane].astype(F32)
            for u in range(1, unk):
                total = total + inv[m, w, u, plane].astype(F32) * cpl[m, k, u, v, plane].astype(F32)
            out.append(total)
    return out


def split3(x):
    hi = x.astype(BF16)
    rest = x - hi.astype(F32)
    mid = rest.astype(BF16)
    lo = (rest - mid.astype(F32)).astype(BF16)
    return hi, mid, lo


def injected(wells, misfit, first, shape):
    members, unk, planes, rows, lanes = shape
    count = planes * rows * lanes
    nwell = wells.shape[1]
    place = wells[...] - first
    inside = (place >= 0) & (place < count)
    line = jnp.where(inside, place // lanes, -1)
    lane = jnp.where(inside, place % lanes, -1)
    lines = lax.broadcasted_iota(jnp.int32, (planes * rows, nwell), 0) == line
    onlane = (lax.broadcasted_iota(jnp.int32, (lanes, nwell), 0) == lane).astype(F32).astype(BF16)
    left = []
    for m in range(members):
        for u in range(unk):
            left.append(jnp.where(lines, misfit[m, u : u + 1, :], 0.0))
    stacked = jnp.concatenate(split3(jnp.concatenate(left, axis=0)), axis=0)
    full = lax.dot_general(stacked, onlane, (((1,), (1,)), ((), ())), preferred_element_type=F32)
    n = members * unk * planes * rows
    total = full[:n] + full[n : 2 * n] + full[2 * n :]
    return total.reshape(shape)


def first_kernel(out):
    out[...] = jnp.zeros_like(out)


def start_kernel(pos, _, wells, misfit, later, cpl_in, inv_in, src, nxt_out, intra_out, cross_out, cpl, inv):
    shape = src.shape
    members, unk, planes = shape[:3]
    cpl[...] = cpl_in[...]
    inv[...] = inv_in[...]
    even = pos[0] % 2 == 0
    count = planes * shape[3] * shape[4]
    src[...] = later[...] + injected(wells, misfit, pos[0] * count, shape)
    for m in range(members):
        s = [src[m, u] for u in range(unk)]
        a = apply_inverse(inv, m, s)
        nxt, up, down = two_sweep_payload(cpl, inv, m, s, a)
        up = up + transfer_blocks(cpl, inv, m, 0, planes - 1, unk)
        down = down + transfer_blocks(cpl, inv, m, 1, 0, unk)
        for u in range(unk):
            nxt_out[m, u] = nxt[u]
        for j in range(len(up)):
            intra_out[m, j] = jnp.where(even, up[j], down[j])
            cross_out[m, j] = jnp.where(even, down[j], up[j])


def incoming(pos, last, m, unk, near, far):
    even = pos[0] % 2 == 0
    has_cross = (pos[0] != 0) & (pos[0] != last)
    sides = []
    for sent, got, block in (near, far):
        first = [got(m, v) for v in range(unk)]
        second = []
        for v in range(unk):
            total = got(m, unk + v)
            for w in range(unk):
                total = total - block(m, 2 * unk + w * unk + v) * sent(m, w)
            second.append(total)
        sides.append((first, second))
    out = []
    for n in range(2):
        low, high = [], []
        for v in range(unk):
            near_v = sides[0][n][v]
            far_v = jnp.where(has_cross, sides[1][n][v], 0.0)
            low.append(jnp.where(even, far_v, near_v))
            high.append(jnp.where(even, near_v, far_v))
        out.append([jnp.stack([lo, hi], axis=0) for lo, hi in zip(low, high)])
    return out


def reader(ref):
    return lambda m, j: ref[m, j]


def either(pos, if_even, if_odd):
    even = pos[0] % 2 == 0
    return lambda m, j: jnp.where(even, if_even[m, j], if_odd[m, j])


def finish_two(cpl, inv, m, src, nxt, arrived):
    a1 = [x - d for x, d in zip(nxt, apply_inverse(inv, m, arrived[0]))]
    inner, _, _ = local_coupling(cpl, m, a1)
    return apply_inverse(inv, m, [s - b - p for s, b, p in zip(src, inner, arrived[1])])


def advance(pos, last, src, nxt, sent_near, sent_far, got_near, got_far, cpl, inv, nxt_out, near_out, far_out):
    members, unk = src.shape[:2]
    even = pos[0] % 2 == 0
    near = (reader(sent_near), reader(got_near), reader(got_near))
    far = (reader(sent_far), reader(got_far), reader(got_far))
    for m in range(members):
        arrived = incoming(pos, last, m, unk, near, far)
        s = [src[m, u] for u in range(unk)]
        a = finish_two(cpl, inv, m, s, [nxt[m, u] for u in range(unk)], arrived)
        ahead, up, down = two_sweep_payload(cpl, inv, m, s, a)
        for u in range(unk):
            nxt_out[m, u] = ahead[u]
        for j in range(len(up)):
            near_out[m, j] = jnp.where(even, up[j], down[j])
            far_out[m, j] = jnp.where(even, down[j], up[j])


def make_even_middle(last):
    def even_middle(*refs):
        pos, outs = refs[0], refs[9:]

        @pl.when(pos[0] % 2 == 0)
        def _():
            advance(pos, last, *refs[1:9], *outs)

        @pl.when(pos[0] % 2 == 1)
        def _():
            for out in outs:
                out[...] = jnp.zeros_like(out)

    return even_middle


def make_odd_middle(last):
    def odd_middle(*refs):
        pos, (nxt_even, near_even), outs = refs[0], refs[9:11], refs[11:]

        @pl.when(pos[0] % 2 == 1)
        def _():
            advance(pos, last, *refs[1:9], *outs)

        @pl.when(pos[0] % 2 == 0)
        def _():
            outs[0][...] = nxt_even[...]
            outs[1][...] = near_even[...]
            outs[2][...] = jnp.zeros_like(outs[2])

    return odd_middle


def select_kernel(pos, bmap, onehot):
    rows, lanes = bmap.shape[1:]
    nblk = onehot.shape[0]
    core = pos[0] % 2
    slot = lax.broadcasted_iota(jnp.int32, (nblk, lanes), 0)
    half_rows = nblk // 2
    parity = jnp.where(slot < half_rows, core, 1 - core)
    within = jnp.where(slot < half_rows, slot, slot - half_rows)
    block = (within // BLK_DEV * 2 + parity) * BLK_DEV + within % BLK_DEV
    for g in range(bmap.shape[0] * rows):
        row = bmap[g // rows, g % rows : g % rows + 1, :]
        onehot[:, g * lanes : (g + 1) * lanes] = (block == row).astype(F32).astype(BF16)


def make_end(last, nblk):
    def end_kernel(
        pos, src, nxt, block_near, block_even, block_odd, sent_near, sent_even, sent_odd, got_near, got_even, got_odd,
        cpl, inv, onehot, sens, adj_out, mine_out, other_out, adj, grads, sems,
    ):
        members, unk, planes, rows, lanes = src.shape
        params = sens.shape[-1]
        groups = planes * rows
        half_rows = nblk // 2
        near = (reader(sent_near), reader(got_near), reader(block_near))
        far = (
            either(pos, sent_even, sent_odd), either(pos, got_even, got_odd), either(pos, block_even, block_odd),
        )
        for m in range(members):
            arrived = incoming(pos, last, m, unk, near, far)
            a = finish_two(
                cpl, inv, m, [src[m, u] for u in range(unk)], [nxt[m, u] for u in range(unk)], arrived
            )
            for u in range(unk):
                adj[m, u] = a[u]
        store = pltpu.make_async_copy(adj, adj_out, sems.at[0])
        store.start()
        turned = adj[...].reshape(members * unk * groups, lanes).T
        for g in range(groups):
            x, y = g // rows, g % rows
            total = None
            for m in range(members):
                for u in range(unk):
                    col = (m * unk + u) * groups + g
                    term = turned[:, col : col + 1] * sens[m, u, x, y].astype(F32)
                    total = term if total is None else total + term
            hi = total.astype(BF16)
            lo = (total - hi.astype(F32)).astype(BF16)
            grads[g * lanes : (g + 1) * lanes, :params] = hi
            grads[g * lanes : (g + 1) * lanes, params:] = lo
        both = jnp.dot(onehot[...], grads[...], preferred_element_type=F32)
        out = both[:, :params] + both[:, params:]
        mine_out[...] = out[:half_rows]
        other_out[...] = out[half_rows:]
        store.wait()

    return end_kernel


VM = pl.BlockSpec(memory_space=pltpu.VMEM)
SM = pl.BlockSpec(memory_space=pltpu.SMEM)
HB = pl.BlockSpec(memory_space=pltpu.HBM)
MIB = 1 << 20


def room(mib):
    return pltpu.CompilerParams(vmem_limit_bytes=mib * MIB)


def busy(flops):
    return pl.CostEstimate(flops=flops, bytes_accessed=0, transcendentals=0)


def shaped(*shape):
    return jax.ShapeDtypeStruct(shape, F32)


def body(later_adjoint, coupling, diag_inverse, sensitivity, well_cells, well_misfit, block_map):
    members, unk, planes, rows, lanes = later_adjoint.shape
    count = planes * rows * lanes
    params = sensitivity.shape[-1]
    ranks = lax.axis_size("cells")
    nblk = ranks * BLK_DEV
    pos = lax.axis_index("cells").astype(jnp.int32).reshape(1)
    intra_pairs = [(i, i ^ 1) for i in range(ranks)]
    up_pairs = [(i, (i + 1) % ranks) for i in range(ranks)]
    down_pairs = [((i + 1) % ranks, i) for i in range(ranks)]

    field = shaped(members, unk, planes, rows, lanes)
    first_size = 2 * unk + unk * unk
    wells = well_cells.reshape(1, -1)
    dma = pltpu.SemaphoreType.DMA
    with jax.named_scope("first"):
        token = pl.pallas_call(
            first_kernel,
            out_shape=shaped(8, 128),
            out_specs=VM,
            compiler_params=room(1),
            cost_estimate=busy(1 << 31),
        )()
    with jax.named_scope("start"):
        src, nxt, near, far, cpl, inv = pl.pallas_call(
            start_kernel,
            out_shape=(
                field,
                field,
                shaped(members, first_size, rows, lanes),
                shaped(members, first_size, rows, lanes),
                jax.ShapeDtypeStruct(coupling.shape, BF16),
                jax.ShapeDtypeStruct(diag_inverse.shape, BF16),
            ),
            in_specs=[SM] + [VM] * 6,
            out_specs=(VM,) * 6,
            compiler_params=room(6),
        )(pos, token, wells, well_misfit, later_adjoint, coupling, diag_inverse)
    got_near = lax.ppermute(near, "cells", intra_pairs)
    got_up = lax.ppermute(far, "cells", up_pairs)
    got_down = lax.ppermute(far, "cells", down_pairs)
    with jax.named_scope("select"):
        onehot = pl.pallas_call(
            select_kernel,
            out_shape=jax.ShapeDtypeStruct((nblk, count), BF16),
            in_specs=[SM, VM],
            out_specs=VM,
            compiler_params=room(6),
            cost_estimate=busy(1 << 24),
        )(pos, block_map)
    wide = shaped(members, 2 * unk, rows, lanes)
    with jax.named_scope("even"):
        nxt_even, near_even, far_even = pl.pallas_call(
            make_even_middle(ranks - 1),
            out_shape=(field, wide, wide),
            in_specs=[SM] + [VM] * 8,
            out_specs=(VM, VM, VM),
            compiler_params=room(6),
        )(pos, src, nxt, near, far, got_near, got_up, cpl, inv)
    got_down2 = lax.ppermute(far_even, "cells", down_pairs)
    with jax.named_scope("odd"):
        nxt2, near2, far_odd = pl.pallas_call(
            make_odd_middle(ranks - 1),
            out_shape=(field, wide, wide),
            in_specs=[SM] + [VM] * 10,
            out_specs=(VM, VM, VM),
            compiler_params=room(6),
        )(pos, src, nxt, near, far, got_near, got_down, cpl, inv, nxt_even, near_even)
    got_near2 = lax.ppermute(near2, "cells", intra_pairs)
    got_up2 = lax.ppermute(far_odd, "cells", up_pairs)
    with jax.named_scope("end"):
        adjoint, mine, other = pl.pallas_call(
            make_end(ranks - 1, nblk),
            out_shape=(field, shaped(nblk // 2, params), shaped(nblk // 2, params)),
            in_specs=[SM] + [VM] * 15,
            out_specs=(HB, VM, VM),
            scratch_shapes=[pltpu.VMEM(field.shape, F32), pltpu.VMEM((count, 2 * params), BF16), dma((1,))],
            compiler_params=room(16),
        )(
            pos, src, nxt2, got_near, got_up, got_down, near2, far_even, far_odd, got_near2, got_up2, got_down2,
            cpl, inv, onehot, sensitivity,
        )
    chips = ranks // 2
    half = mine + lax.ppermute(other, "cells", intra_pairs)
    same_core = [[core + 2 * chip for chip in range(chips)] for core in range(2)]
    parts = lax.all_to_all(
        half.reshape(chips, BLK_DEV, params), "cells", 0, 0, tiled=True, axis_index_groups=same_core
    )
    owned = jnp.sum(parts, axis=0)
    gradient = owned + lax.ppermute(owned, "ens", [(0, 1), (1, 0)])
    return (adjoint, gradient)


def solution(mesh):
    placed = (
        P("ens", None, "cells", None, None),
        P("ens", None, None, None, "cells", None, None),
        P("ens", None, None, "cells", None, None),
        P("ens", None, "cells", None, None, None),
        P(),
        P("ens", None, None),
        P("cells", None, None),
    )
    return jax.shard_map(
        body,
        mesh=mesh,
        in_specs=placed,
        out_specs=(P("ens", None, "cells", None, None), P("cells", None)),
        check_vma=False,
    )
```

```python
import jax
import jax.numpy as jnp
from jax import lax
from jax.experimental import pallas as pl
from jax.experimental.pallas import tpu as pltpu
from jax.sharding import PartitionSpec as P


BLK_DEV = 4
F32 = jnp.float32
BF16 = jnp.bfloat16


def shift_lanes(x, by):
    size = x.shape[2]
    lane = lax.broadcasted_iota(jnp.int32, x.shape, 2)
    keep = lane >= 1 if by == 1 else lane < size - 1
    return jnp.where(keep, pltpu.roll(x, by % size, 2), 0.0)


def shift_rows(x, by):
    size = x.shape[1]
    row = lax.broadcasted_iota(jnp.int32, x.shape, 1)
    keep = row >= 1 if by == 1 else row < size - 1
    return jnp.where(keep, pltpu.roll(x, by % size, 1), 0.0)


def products(cpl, m, k, a):
    unk = len(a)
    out = []
    for v in range(unk):
        total = cpl[m, k, 0, v].astype(F32) * a[0]
        for u in range(1, unk):
            total = total + cpl[m, k, u, v].astype(F32) * a[u]
        out.append(total)
    return out


def local_coupling(cpl, m, a):
    unk = len(a)
    terms = [products(cpl, m, k, a) for k in range(6)]
    inner, up, down = [], [], []
    for v in range(unk):
        t = [terms[k][v] for k in range(6)]
        planes = t[0].shape[0]
        zero = jnp.zeros_like(t[0][:1])
        total = jnp.concatenate([zero, t[0][: planes - 1]], axis=0)
        total = total + jnp.concatenate([t[1][1:], zero], axis=0)
        total = total + shift_rows(t[2], 1) + shift_rows(t[3], -1)
        total = total + shift_lanes(t[4], 1) + shift_lanes(t[5], -1)
        inner.append(total)
        up.append(t[0][planes - 1])
        down.append(t[1][0])
    return inner, up, down


def apply_inverse(inv, m, r):
    unk = len(r)
    out = []
    for v in range(unk):
        total = inv[m, 0, v].astype(F32) * r[0]
        for w in range(1, unk):
            total = total + inv[m, w, v].astype(F32) * r[w]
        out.append(total)
    return out


def plane_products(cpl, m, k, plane, a):
    unk = len(a)
    out = []
    for v in range(unk):
        total = cpl[m, k, 0, v, plane].astype(F32) * a[0]
        for u in range(1, unk):
            total = total + cpl[m, k, u, v, plane].astype(F32) * a[u]
        out.append(total)
    return out


def two_sweep_payload(cpl, inv, m, src, a):
    planes = a[0].shape[0]
    inner, up0, down0 = local_coupling(cpl, m, a)
    nxt = apply_inverse(inv, m, [s - b for s, b in zip(src, inner)])
    up1 = plane_products(cpl, m, 0, planes - 1, [x[planes - 1] for x in nxt])
    down1 = plane_products(cpl, m, 1, 0, [x[0] for x in nxt])
    return nxt, up0 + up1, down0 + down1


def transfer_blocks(cpl, inv, m, k, plane, unk):
    out = []
    for w in range(unk):
        for v in range(unk):
            total = inv[m, w, 0, plane].astype(F32) * cpl[m, k, 0, v, plane].astype(F32)
            for u in range(1, unk):
                total = total + inv[m, w, u, plane].astype(F32) * cpl[m, k, u, v, plane].astype(F32)
            out.append(total)
    return out


def split3(x):
    hi = x.astype(BF16)
    rest = x - hi.astype(F32)
    mid = rest.astype(BF16)
    lo = (rest - mid.astype(F32)).astype(BF16)
    return hi, mid, lo


def injected(wells, misfit, first, shape):
    members, unk, planes, rows, lanes = shape
    count = planes * rows * lanes
    nwell = wells.shape[1]
    place = wells[...] - first
    inside = (place >= 0) & (place < count)
    line = jnp.where(inside, place // lanes, -1)
    lane = jnp.where(inside, place % lanes, -1)
    lines = lax.broadcasted_iota(jnp.int32, (planes * rows, nwell), 0) == line
    onlane = (lax.broadcasted_iota(jnp.int32, (lanes, nwell), 0) == lane).astype(F32).astype(BF16)
    left = []
    for m in range(members):
        for u in range(unk):
            left.append(jnp.where(lines, misfit[m, u : u + 1, :], 0.0))
    stacked = jnp.concatenate(split3(jnp.concatenate(left, axis=0)), axis=0)
    full = lax.dot_general(stacked, onlane, (((1,), (1,)), ((), ())), preferred_element_type=F32)
    n = members * unk * planes * rows
    total = full[:n] + full[n : 2 * n] + full[2 * n :]
    return total.reshape(shape)


def first_kernel(out):
    out[...] = jnp.zeros_like(out)


def start_kernel(pos, _, wells, misfit, later, cpl_in, inv_in, src, nxt_out, intra_out, cross_out, cpl, inv):
    shape = src.shape
    members, unk, planes = shape[:3]
    cpl[...] = cpl_in[...]
    inv[...] = inv_in[...]
    even = pos[0] % 2 == 0
    count = planes * shape[3] * shape[4]
    src[...] = later[...] + injected(wells, misfit, pos[0] * count, shape)
    for m in range(members):
        s = [src[m, u] for u in range(unk)]
        a = apply_inverse(inv, m, s)
        nxt, up, down = two_sweep_payload(cpl, inv, m, s, a)
        up = up + transfer_blocks(cpl, inv, m, 0, planes - 1, unk)
        down = down + transfer_blocks(cpl, inv, m, 1, 0, unk)
        for u in range(unk):
            nxt_out[m, u] = nxt[u]
        for j in range(len(up)):
            intra_out[m, j] = jnp.where(even, up[j], down[j])
            cross_out[m, j] = jnp.where(even, down[j], up[j])


def incoming(pos, last, m, unk, near, far):
    even = pos[0] % 2 == 0
    has_cross = (pos[0] != 0) & (pos[0] != last)
    sides = []
    for sent, got, block in (near, far):
        first = [got(m, v) for v in range(unk)]
        second = []
        for v in range(unk):
            total = got(m, unk + v)
            for w in range(unk):
                total = total - block(m, 2 * unk + w * unk + v) * sent(m, w)
            second.append(total)
        sides.append((first, second))
    out = []
    for n in range(2):
        low, high = [], []
        for v in range(unk):
            near_v = sides[0][n][v]
            far_v = jnp.where(has_cross, sides[1][n][v], 0.0)
            low.append(jnp.where(even, far_v, near_v))
            high.append(jnp.where(even, near_v, far_v))
        out.append([jnp.stack([lo, hi], axis=0) for lo, hi in zip(low, high)])
    return out


def reader(ref):
    return lambda m, j: ref[m, j]


def either(pos, if_even, if_odd):
    even = pos[0] % 2 == 0
    return lambda m, j: jnp.where(even, if_even[m, j], if_odd[m, j])


def finish_two(cpl, inv, m, src, nxt, arrived):
    a1 = [x - d for x, d in zip(nxt, apply_inverse(inv, m, arrived[0]))]
    inner, _, _ = local_coupling(cpl, m, a1)
    return apply_inverse(inv, m, [s - b - p for s, b, p in zip(src, inner, arrived[1])])


def advance(pos, last, src, nxt, sent_near, sent_far, got_near, got_far, cpl, inv, nxt_out, near_out, far_out):
    members, unk = src.shape[:2]
    even = pos[0] % 2 == 0
    near = (reader(sent_near), reader(got_near), reader(got_near))
    far = (reader(sent_far), reader(got_far), reader(got_far))
    for m in range(members):
        arrived = incoming(pos, last, m, unk, near, far)
        s = [src[m, u] for u in range(unk)]
        a = finish_two(cpl, inv, m, s, [nxt[m, u] for u in range(unk)], arrived)
        ahead, up, down = two_sweep_payload(cpl, inv, m, s, a)
        for u in range(unk):
            nxt_out[m, u] = ahead[u]
        for j in range(len(up)):
            near_out[m, j] = jnp.where(even, up[j], down[j])
            far_out[m, j] = jnp.where(even, down[j], up[j])


def make_even_middle(last):
    def even_middle(*refs):
        pos, outs = refs[0], refs[9:]

        @pl.when(pos[0] % 2 == 0)
        def _():
            advance(pos, last, *refs[1:9], *outs)

        @pl.when(pos[0] % 2 == 1)
        def _():
            for out in outs:
                out[...] = jnp.zeros_like(out)

    return even_middle


def make_odd_middle(last):
    def odd_middle(*refs):
        pos, (nxt_even, near_even), outs = refs[0], refs[9:11], refs[11:]

        @pl.when(pos[0] % 2 == 1)
        def _():
            advance(pos, last, *refs[1:9], *outs)

        @pl.when(pos[0] % 2 == 0)
        def _():
            outs[0][...] = nxt_even[...]
            outs[1][...] = near_even[...]
            outs[2][...] = jnp.zeros_like(outs[2])

    return odd_middle


def select_kernel(pos, bmap, onehot):
    rows, lanes = bmap.shape[1:]
    nblk = onehot.shape[0]
    core = pos[0] % 2
    slot = lax.broadcasted_iota(jnp.int32, (nblk, lanes), 0)
    half_rows = nblk // 2
    parity = jnp.where(slot < half_rows, core, 1 - core)
    within = jnp.where(slot < half_rows, slot, slot - half_rows)
    block = (within // BLK_DEV * 2 + parity) * BLK_DEV + within % BLK_DEV
    for g in range(bmap.shape[0] * rows):
        row = bmap[g // rows, g % rows : g % rows + 1, :]
        onehot[:, g * lanes : (g + 1) * lanes] = (block == row).astype(F32).astype(BF16)


def make_end(last, nblk):
    def end_kernel(
        pos, src, nxt, block_near, block_even, block_odd, sent_near, sent_even, sent_odd, got_near, got_even, got_odd,
        cpl, inv, onehot, sens, adj_out, mine_out, other_out, adj, grads, sems,
    ):
        members, unk, planes, rows, lanes = src.shape
        params = sens.shape[-1]
        groups = planes * rows
        half_rows = nblk // 2
        near = (reader(sent_near), reader(got_near), reader(block_near))
        far = (
            either(pos, sent_even, sent_odd), either(pos, got_even, got_odd), either(pos, block_even, block_odd),
        )
        for m in range(members):
            arrived = incoming(pos, last, m, unk, near, far)
            a = finish_two(
                cpl, inv, m, [src[m, u] for u in range(unk)], [nxt[m, u] for u in range(unk)], arrived
            )
            for u in range(unk):
                adj[m, u] = a[u]
        store = pltpu.make_async_copy(adj, adj_out, sems.at[0])
        store.start()
        turned = adj[...].reshape(members * unk * groups, lanes).T
        for g in range(groups):
            x, y = g // rows, g % rows
            total = None
            for m in range(members):
                for u in range(unk):
                    col = (m * unk + u) * groups + g
                    term = turned[:, col : col + 1] * sens[m, u, x, y].astype(F32)
                    total = term if total is None else total + term
            hi = total.astype(BF16)
            lo = (total - hi.astype(F32)).astype(BF16)
            grads[g * lanes : (g + 1) * lanes, :params] = hi
            grads[g * lanes : (g + 1) * lanes, params:] = lo
        both = jnp.dot(onehot[...], grads[...], preferred_element_type=F32)
        out = both[:, :params] + both[:, params:]
        mine_out[...] = out[:half_rows]
        other_out[...] = out[half_rows:]
        store.wait()

    return end_kernel


VM = pl.BlockSpec(memory_space=pltpu.VMEM)
SM = pl.BlockSpec(memory_space=pltpu.SMEM)
HB = pl.BlockSpec(memory_space=pltpu.HBM)
MIB = 1 << 20


def room(mib):
    return pltpu.CompilerParams(vmem_limit_bytes=mib * MIB)


def busy(flops):
    return pl.CostEstimate(flops=flops, bytes_accessed=0, transcendentals=0)


def shaped(*shape):
    return jax.ShapeDtypeStruct(shape, F32)


def timestep(later_adjoint, coupling, diag_inverse, sensitivity, well_cells, well_misfit, block_map):
    members, unk, planes, rows, lanes = later_adjoint.shape
    count = planes * rows * lanes
    params = sensitivity.shape[-1]
    ranks = lax.axis_size("cells")
    nblk = ranks * BLK_DEV
    pos = lax.axis_index("cells").astype(jnp.int32).reshape(1)
    intra_pairs = [(i, i ^ 1) for i in range(ranks)]
    up_pairs = [(i, (i + 1) % ranks) for i in range(ranks)]
    down_pairs = [((i + 1) % ranks, i) for i in range(ranks)]

    field = shaped(members, unk, planes, rows, lanes)
    first_size = 2 * unk + unk * unk
    wells = well_cells.reshape(1, -1)
    dma = pltpu.SemaphoreType.DMA
    token = pl.pallas_call(
        first_kernel,
        out_shape=shaped(8, 128),
        out_specs=VM,
        compiler_params=room(1),
        cost_estimate=busy(1 << 31),
    )()
    src, nxt, near, far, cpl, inv = pl.pallas_call(
        start_kernel,
        out_shape=(
            field,
            field,
            shaped(members, first_size, rows, lanes),
            shaped(members, first_size, rows, lanes),
            jax.ShapeDtypeStruct(coupling.shape, BF16),
            jax.ShapeDtypeStruct(diag_inverse.shape, BF16),
        ),
        in_specs=[SM] + [VM] * 6,
        out_specs=(VM,) * 6,
        compiler_params=room(6),
    )(pos, token, wells, well_misfit, later_adjoint, coupling, diag_inverse)
    got_up = lax.ppermute(far, "cells", up_pairs)
    got_down = lax.ppermute(far, "cells", down_pairs)
    got_near = lax.ppermute(near, "cells", intra_pairs)
    onehot = pl.pallas_call(
        select_kernel,
        out_shape=jax.ShapeDtypeStruct((nblk, count), BF16),
        in_specs=[SM, VM],
        out_specs=VM,
        compiler_params=room(6),
        cost_estimate=busy(1 << 24),
    )(pos, block_map)
    wide = shaped(members, 2 * unk, rows, lanes)
    nxt_even, near_even, far_even = pl.pallas_call(
        make_even_middle(ranks - 1),
        out_shape=(field, wide, wide),
        in_specs=[SM] + [VM] * 8,
        out_specs=(VM, VM, VM),
        compiler_params=room(6),
    )(pos, src, nxt, near, far, got_near, got_up, cpl, inv)
    got_down2 = lax.ppermute(far_even, "cells", down_pairs)
    nxt2, near2, far_odd = pl.pallas_call(
        make_odd_middle(ranks - 1),
        out_shape=(field, wide, wide),
        in_specs=[SM] + [VM] * 10,
        out_specs=(VM, VM, VM),
        compiler_params=room(6),
    )(pos, src, nxt, near, far, got_near, got_down, cpl, inv, nxt_even, near_even)
    got_up2 = lax.ppermute(far_odd, "cells", up_pairs)
    got_near2 = lax.ppermute(near2, "cells", intra_pairs)
    adjoint, mine, other = pl.pallas_call(
        make_end(ranks - 1, nblk),
        out_shape=(field, shaped(nblk // 2, params), shaped(nblk // 2, params)),
        in_specs=[SM] + [VM] * 15,
        out_specs=(HB, VM, VM),
        scratch_shapes=[pltpu.VMEM(field.shape, F32), pltpu.VMEM((count, 2 * params), BF16), dma((1,))],
        compiler_params=room(16),
    )(
        pos, src, nxt2, got_near, got_up, got_down, near2, far_even, far_odd, got_near2, got_up2, got_down2,
        cpl, inv, onehot, sensitivity,
    )
    chips = ranks // 2
    half = mine + lax.ppermute(other, "cells", intra_pairs)
    same_core = [[core + 2 * chip for chip in range(chips)] for core in range(2)]
    parts = lax.all_to_all(
        half.reshape(chips, BLK_DEV, params), "cells", 0, 0, tiled=True, axis_index_groups=same_core
    )
    owned = jnp.sum(parts, axis=0)
    gradient = owned + lax.ppermute(owned, "ens", [(0, 1), (1, 0)])
    return (adjoint, gradient)


def solution(mesh):
    placed = (
        P("ens", None, "cells", None, None),
        P("ens", None, None, None, "cells", None, None),
        P("ens", None, None, "cells", None, None),
        P("ens", None, "cells", None, None, None),
        P(),
        P("ens", None, None),
        P("cells", None, None),
    )
    return jax.shard_map(
        timestep,
        mesh=mesh,
        in_specs=placed,
        out_specs=(P("ens", None, "cells", None, None), P("cells", None)),
        check_vma=False,
    )
```

```python
import jax
import jax.numpy as jnp
from jax import lax
from jax.experimental import pallas as pl
from jax.experimental.pallas import tpu as pltpu
from jax.sharding import PartitionSpec as P


BLK_DEV = 4
F32 = jnp.float32
BF16 = jnp.bfloat16


def shift_lanes(x, by):
    size = x.shape[2]
    lane = lax.broadcasted_iota(jnp.int32, x.shape, 2)
    keep = lane >= 1 if by == 1 else lane < size - 1
    return jnp.where(keep, pltpu.roll(x, by % size, 2), 0.0)


def shift_rows(x, by):
    size = x.shape[1]
    row = lax.broadcasted_iota(jnp.int32, x.shape, 1)
    keep = row >= 1 if by == 1 else row < size - 1
    return jnp.where(keep, pltpu.roll(x, by % size, 1), 0.0)


def products(cpl, m, k, a):
    unk = len(a)
    out = []
    for v in range(unk):
        total = cpl[m, k, 0, v].astype(F32) * a[0]
        for u in range(1, unk):
            total = total + cpl[m, k, u, v].astype(F32) * a[u]
        out.append(total)
    return out


def local_coupling(cpl, m, a):
    unk = len(a)
    terms = [products(cpl, m, k, a) for k in range(6)]
    inner, up, down = [], [], []
    for v in range(unk):
        t = [terms[k][v] for k in range(6)]
        planes = t[0].shape[0]
        zero = jnp.zeros_like(t[0][:1])
        total = jnp.concatenate([zero, t[0][: planes - 1]], axis=0)
        total = total + jnp.concatenate([t[1][1:], zero], axis=0)
        total = total + shift_rows(t[2], 1) + shift_rows(t[3], -1)
        total = total + shift_lanes(t[4], 1) + shift_lanes(t[5], -1)
        inner.append(total)
        up.append(t[0][planes - 1])
        down.append(t[1][0])
    return inner, up, down


def apply_inverse(inv, m, r):
    unk = len(r)
    out = []
    for v in range(unk):
        total = inv[m, 0, v].astype(F32) * r[0]
        for w in range(1, unk):
            total = total + inv[m, w, v].astype(F32) * r[w]
        out.append(total)
    return out


def plane_products(cpl, m, k, plane, a):
    unk = len(a)
    out = []
    for v in range(unk):
        total = cpl[m, k, 0, v, plane].astype(F32) * a[0]
        for u in range(1, unk):
            total = total + cpl[m, k, u, v, plane].astype(F32) * a[u]
        out.append(total)
    return out


def two_sweep_payload(cpl, inv, m, src, a):
    planes = a[0].shape[0]
    inner, up0, down0 = local_coupling(cpl, m, a)
    nxt = apply_inverse(inv, m, [s - b for s, b in zip(src, inner)])
    up1 = plane_products(cpl, m, 0, planes - 1, [x[planes - 1] for x in nxt])
    down1 = plane_products(cpl, m, 1, 0, [x[0] for x in nxt])
    return nxt, up0 + up1, down0 + down1


def transfer_blocks(cpl, inv, m, k, plane, unk):
    out = []
    for w in range(unk):
        for v in range(unk):
            total = inv[m, w, 0, plane].astype(F32) * cpl[m, k, 0, v, plane].astype(F32)
            for u in range(1, unk):
                total = total + inv[m, w, u, plane].astype(F32) * cpl[m, k, u, v, plane].astype(F32)
            out.append(total)
    return out


def split3(x):
    hi = x.astype(BF16)
    rest = x - hi.astype(F32)
    mid = rest.astype(BF16)
    lo = (rest - mid.astype(F32)).astype(BF16)
    return hi, mid, lo


def injected(wells, misfit, first, shape):
    members, unk, planes, rows, lanes = shape
    count = planes * rows * lanes
    nwell = wells.shape[1]
    place = wells[...] - first
    inside = (place >= 0) & (place < count)
    line = jnp.where(inside, place // lanes, -1)
    lane = jnp.where(inside, place % lanes, -1)
    lines = lax.broadcasted_iota(jnp.int32, (planes * rows, nwell), 0) == line
    onlane = (lax.broadcasted_iota(jnp.int32, (lanes, nwell), 0) == lane).astype(F32).astype(BF16)
    left = []
    for m in range(members):
        for u in range(unk):
            left.append(jnp.where(lines, misfit[m, u : u + 1, :], 0.0))
    stacked = jnp.concatenate(split3(jnp.concatenate(left, axis=0)), axis=0)
    full = lax.dot_general(stacked, onlane, (((1,), (1,)), ((), ())), preferred_element_type=F32)
    n = members * unk * planes * rows
    total = full[:n] + full[n : 2 * n] + full[2 * n :]
    return total.reshape(shape)


def first_kernel(out):
    out[...] = jnp.zeros_like(out)


def start_kernel(pos, _, wells, misfit, later, cpl_in, inv_in, src, nxt_out, intra_out, cross_out, cpl, inv):
    shape = src.shape
    members, unk, planes = shape[:3]
    cpl[...] = cpl_in[...]
    inv[...] = inv_in[...]
    even = pos[0] % 2 == 0
    count = planes * shape[3] * shape[4]
    src[...] = later[...] + injected(wells, misfit, pos[0] * count, shape)
    for m in range(members):
        s = [src[m, u] for u in range(unk)]
        a = apply_inverse(inv, m, s)
        nxt, up, down = two_sweep_payload(cpl, inv, m, s, a)
        up = up + transfer_blocks(cpl, inv, m, 0, planes - 1, unk)
        down = down + transfer_blocks(cpl, inv, m, 1, 0, unk)
        for u in range(unk):
            nxt_out[m, u] = nxt[u]
        for j in range(len(up)):
            intra_out[m, j] = jnp.where(even, up[j], down[j])
            cross_out[m, j] = jnp.where(even, down[j], up[j])


def incoming(pos, last, m, unk, near, far):
    even = pos[0] % 2 == 0
    has_cross = (pos[0] != 0) & (pos[0] != last)
    sides = []
    for sent, got, block in (near, far):
        first = [got(m, v) for v in range(unk)]
        second = []
        for v in range(unk):
            total = got(m, unk + v)
            for w in range(unk):
                total = total - block(m, 2 * unk + w * unk + v) * sent(m, w)
            second.append(total)
        sides.append((first, second))
    out = []
    for n in range(2):
        low, high = [], []
        for v in range(unk):
            near_v = sides[0][n][v]
            far_v = jnp.where(has_cross, sides[1][n][v], 0.0)
            low.append(jnp.where(even, far_v, near_v))
            high.append(jnp.where(even, near_v, far_v))
        out.append([jnp.stack([lo, hi], axis=0) for lo, hi in zip(low, high)])
    return out


def reader(ref):
    return lambda m, j: ref[m, j]


def either(pos, if_even, if_odd):
    even = pos[0] % 2 == 0
    return lambda m, j: jnp.where(even, if_even[m, j], if_odd[m, j])


def finish_two(cpl, inv, m, src, nxt, arrived):
    a1 = [x - d for x, d in zip(nxt, apply_inverse(inv, m, arrived[0]))]
    inner, _, _ = local_coupling(cpl, m, a1)
    return apply_inverse(inv, m, [s - b - p for s, b, p in zip(src, inner, arrived[1])])


def advance(pos, last, src, nxt, sent_near, sent_far, got_near, got_far, cpl, inv, nxt_out, near_out, far_out):
    members, unk = src.shape[:2]
    even = pos[0] % 2 == 0
    near = (reader(sent_near), reader(got_near), reader(got_near))
    far = (reader(sent_far), reader(got_far), reader(got_far))
    for m in range(members):
        arrived = incoming(pos, last, m, unk, near, far)
        s = [src[m, u] for u in range(unk)]
        a = finish_two(cpl, inv, m, s, [nxt[m, u] for u in range(unk)], arrived)
        ahead, up, down = two_sweep_payload(cpl, inv, m, s, a)
        for u in range(unk):
            nxt_out[m, u] = ahead[u]
        for j in range(len(up)):
            near_out[m, j] = jnp.where(even, up[j], down[j])
            far_out[m, j] = jnp.where(even, down[j], up[j])


def make_even_middle(last):
    def even_middle(*refs):
        pos, outs = refs[0], refs[9:]

        @pl.when(pos[0] % 2 == 0)
        def _():
            advance(pos, last, *refs[1:9], *outs)

        @pl.when(pos[0] % 2 == 1)
        def _():
            for out in outs:
                out[...] = jnp.zeros_like(out)

    return even_middle


def make_odd_middle(last):
    def odd_middle(*refs):
        pos, (nxt_even, near_even), outs = refs[0], refs[9:11], refs[11:]

        @pl.when(pos[0] % 2 == 1)
        def _():
            advance(pos, last, *refs[1:9], *outs)

        @pl.when(pos[0] % 2 == 0)
        def _():
            outs[0][...] = nxt_even[...]
            outs[1][...] = near_even[...]
            outs[2][...] = jnp.zeros_like(outs[2])

    return odd_middle


def select_kernel(pos, bmap, sens, onehot, turned):
    rows, lanes = bmap.shape[1:]
    nblk = onehot.shape[0]
    core = pos[0] % 2
    slot = lax.broadcasted_iota(jnp.int32, (nblk, lanes), 0)
    half_rows = nblk // 2
    parity = jnp.where(slot < half_rows, core, 1 - core)
    within = jnp.where(slot < half_rows, slot, slot - half_rows)
    block = (within // BLK_DEV * 2 + parity) * BLK_DEV + within % BLK_DEV
    for g in range(bmap.shape[0] * rows):
        row = bmap[g // rows, g % rows : g % rows + 1, :]
        onehot[:, g * lanes : (g + 1) * lanes] = (block == row).astype(F32).astype(BF16)
    for m in range(sens.shape[0]):
        for u in range(sens.shape[1]):
            for g in range(bmap.shape[0] * rows):
                turned[m, u, g] = sens[m, u, g // rows, g % rows].astype(F32).T


def make_end(last, nblk):
    def end_kernel(
        pos, src, nxt, block_near, block_even, block_odd, sent_near, sent_even, sent_odd, got_near, got_even, got_odd,
        cpl, inv, onehot, turned, adj_out, mine_out, other_out, adj, grads, sems,
    ):
        members, unk, planes, rows, lanes = src.shape
        params = turned.shape[-2]
        groups = planes * rows
        half_rows = nblk // 2
        near = (reader(sent_near), reader(got_near), reader(block_near))
        far = (
            either(pos, sent_even, sent_odd), either(pos, got_even, got_odd), either(pos, block_even, block_odd),
        )
        for m in range(members):
            arrived = incoming(pos, last, m, unk, near, far)
            a = finish_two(
                cpl, inv, m, [src[m, u] for u in range(unk)], [nxt[m, u] for u in range(unk)], arrived
            )
            for u in range(unk):
                adj[m, u] = a[u]
        store = pltpu.make_async_copy(adj, adj_out, sems.at[0])
        store.start()
        step = 32
        for g in range(groups):
            x, y = g // rows, g % rows
            for p in range(0, params, step):
                total = None
                for m in range(members):
                    for u in range(unk):
                        term = adj[m, u, x, y : y + 1] * turned[m, u, g, p : p + step]
                        total = term if total is None else total + term
                hi = total.astype(BF16)
                lo = (total - hi.astype(F32)).astype(BF16)
                grads[p : p + step, g * lanes : (g + 1) * lanes] = hi
                grads[params + p : params + p + step, g * lanes : (g + 1) * lanes] = lo
        both = lax.dot_general(
            onehot[...], grads[...], (((1,), (1,)), ((), ())), preferred_element_type=F32
        )
        out = both[:, :params] + both[:, params:]
        mine_out[...] = out[:half_rows]
        other_out[...] = out[half_rows:]
        store.wait()

    return end_kernel


VM = pl.BlockSpec(memory_space=pltpu.VMEM)
SM = pl.BlockSpec(memory_space=pltpu.SMEM)
HB = pl.BlockSpec(memory_space=pltpu.HBM)
MIB = 1 << 20


def room(mib):
    return pltpu.CompilerParams(vmem_limit_bytes=mib * MIB)


def busy(flops):
    return pl.CostEstimate(flops=flops, bytes_accessed=0, transcendentals=0)


def shaped(*shape):
    return jax.ShapeDtypeStruct(shape, F32)


def timestep(later_adjoint, coupling, diag_inverse, sensitivity, well_cells, well_misfit, block_map):
    members, unk, planes, rows, lanes = later_adjoint.shape
    count = planes * rows * lanes
    params = sensitivity.shape[-1]
    ranks = lax.axis_size("cells")
    nblk = ranks * BLK_DEV
    pos = lax.axis_index("cells").astype(jnp.int32).reshape(1)
    intra_pairs = [(i, i ^ 1) for i in range(ranks)]
    up_pairs = [(i, (i + 1) % ranks) for i in range(ranks)]
    down_pairs = [((i + 1) % ranks, i) for i in range(ranks)]

    field = shaped(members, unk, planes, rows, lanes)
    first_size = 2 * unk + unk * unk
    wells = well_cells.reshape(1, -1)
    dma = pltpu.SemaphoreType.DMA
    token = pl.pallas_call(
        first_kernel,
        out_shape=shaped(8, 128),
        out_specs=VM,
        compiler_params=room(1),
        cost_estimate=busy(1 << 31),
    )()
    src, nxt, near, far, cpl, inv = pl.pallas_call(
        start_kernel,
        out_shape=(
            field,
            field,
            shaped(members, first_size, rows, lanes),
            shaped(members, first_size, rows, lanes),
            jax.ShapeDtypeStruct(coupling.shape, BF16),
            jax.ShapeDtypeStruct(diag_inverse.shape, BF16),
        ),
        in_specs=[SM] + [VM] * 6,
        out_specs=(VM,) * 6,
        compiler_params=room(6),
    )(pos, token, wells, well_misfit, later_adjoint, coupling, diag_inverse)
    got_up = lax.ppermute(far, "cells", up_pairs)
    got_down = lax.ppermute(far, "cells", down_pairs)
    got_near = lax.ppermute(near, "cells", intra_pairs)
    onehot, turned = pl.pallas_call(
        select_kernel,
        out_shape=(
            jax.ShapeDtypeStruct((nblk, count), BF16), shaped(members, unk, planes * rows, params, lanes)
        ),
        in_specs=[SM, VM, VM],
        out_specs=(VM, VM),
        compiler_params=room(6),
        cost_estimate=busy(1 << 24),
    )(pos, block_map, sensitivity)
    wide = shaped(members, 2 * unk, rows, lanes)
    nxt_even, near_even, far_even = pl.pallas_call(
        make_even_middle(ranks - 1),
        out_shape=(field, wide, wide),
        in_specs=[SM] + [VM] * 8,
        out_specs=(VM, VM, VM),
        compiler_params=room(6),
    )(pos, src, nxt, near, far, got_near, got_up, cpl, inv)
    got_down2 = lax.ppermute(far_even, "cells", down_pairs)
    nxt2, near2, far_odd = pl.pallas_call(
        make_odd_middle(ranks - 1),
        out_shape=(field, wide, wide),
        in_specs=[SM] + [VM] * 10,
        out_specs=(VM, VM, VM),
        compiler_params=room(6),
    )(pos, src, nxt, near, far, got_near, got_down, cpl, inv, nxt_even, near_even)
    got_up2 = lax.ppermute(far_odd, "cells", up_pairs)
    got_near2 = lax.ppermute(near2, "cells", intra_pairs)
    adjoint, mine, other = pl.pallas_call(
        make_end(ranks - 1, nblk),
        out_shape=(field, shaped(nblk // 2, params), shaped(nblk // 2, params)),
        in_specs=[SM] + [VM] * 15,
        out_specs=(HB, VM, VM),
        scratch_shapes=[pltpu.VMEM(field.shape, F32), pltpu.VMEM((2 * params, count), BF16), dma((1,))],
        compiler_params=room(16),
    )(
        pos, src, nxt2, got_near, got_up, got_down, near2, far_even, far_odd, got_near2, got_up2, got_down2,
        cpl, inv, onehot, turned,
    )
    chips = ranks // 2
    half = mine + lax.ppermute(other, "cells", intra_pairs)
    same_core = [[core + 2 * chip for chip in range(chips)] for core in range(2)]
    parts = lax.all_to_all(
        half.reshape(chips, BLK_DEV, params), "cells", 0, 0, tiled=True, axis_index_groups=same_core
    )
    owned = jnp.sum(parts, axis=0)
    gradient = owned + lax.ppermute(owned, "ens", [(0, 1), (1, 0)])
    return (adjoint, gradient)


def solution(mesh):
    placed = (
        P("ens", None, "cells", None, None),
        P("ens", None, None, None, "cells", None, None),
        P("ens", None, None, "cells", None, None),
        P("ens", None, "cells", None, None, None),
        P(),
        P("ens", None, None),
        P("cells", None, None),
    )
    return jax.shard_map(
        timestep,
        mesh=mesh,
        in_specs=placed,
        out_specs=(P("ens", None, "cells", None, None), P("cells", None)),
        check_vma=False,
    )
```

```python
import jax
import jax.numpy as jnp
from jax import lax
from jax.experimental import pallas as pl
from jax.experimental.pallas import tpu as pltpu
from jax.sharding import PartitionSpec as P


BLK_DEV = 4
F32 = jnp.float32
BF16 = jnp.bfloat16


def shift_lanes(x, by):
    size = x.shape[2]
    lane = lax.broadcasted_iota(jnp.int32, x.shape, 2)
    keep = lane >= 1 if by == 1 else lane < size - 1
    return jnp.where(keep, pltpu.roll(x, by % size, 2), 0.0)


def shift_rows(x, by):
    size = x.shape[1]
    row = lax.broadcasted_iota(jnp.int32, x.shape, 1)
    keep = row >= 1 if by == 1 else row < size - 1
    return jnp.where(keep, pltpu.roll(x, by % size, 1), 0.0)


def products(cpl, m, k, a):
    unk = len(a)
    out = []
    for v in range(unk):
        total = cpl[m, k, 0, v].astype(F32) * a[0]
        for u in range(1, unk):
            total = total + cpl[m, k, u, v].astype(F32) * a[u]
        out.append(total)
    return out


def local_coupling(cpl, m, a):
    unk = len(a)
    terms = [products(cpl, m, k, a) for k in range(6)]
    inner, up, down = [], [], []
    for v in range(unk):
        t = [terms[k][v] for k in range(6)]
        planes = t[0].shape[0]
        zero = jnp.zeros_like(t[0][:1])
        total = jnp.concatenate([zero, t[0][: planes - 1]], axis=0)
        total = total + jnp.concatenate([t[1][1:], zero], axis=0)
        total = total + shift_rows(t[2], 1) + shift_rows(t[3], -1)
        total = total + shift_lanes(t[4], 1) + shift_lanes(t[5], -1)
        inner.append(total)
        up.append(t[0][planes - 1])
        down.append(t[1][0])
    return inner, up, down


def apply_inverse(inv, m, r):
    unk = len(r)
    out = []
    for v in range(unk):
        total = inv[m, 0, v].astype(F32) * r[0]
        for w in range(1, unk):
            total = total + inv[m, w, v].astype(F32) * r[w]
        out.append(total)
    return out


def plane_products(cpl, m, k, plane, a):
    unk = len(a)
    out = []
    for v in range(unk):
        total = cpl[m, k, 0, v, plane].astype(F32) * a[0]
        for u in range(1, unk):
            total = total + cpl[m, k, u, v, plane].astype(F32) * a[u]
        out.append(total)
    return out


def two_sweep_payload(cpl, inv, m, src, a):
    planes = a[0].shape[0]
    inner, up0, down0 = local_coupling(cpl, m, a)
    nxt = apply_inverse(inv, m, [s - b for s, b in zip(src, inner)])
    up1 = plane_products(cpl, m, 0, planes - 1, [x[planes - 1] for x in nxt])
    down1 = plane_products(cpl, m, 1, 0, [x[0] for x in nxt])
    return nxt, up0 + up1, down0 + down1


def transfer_blocks(cpl, inv, m, k, plane, unk):
    out = []
    for w in range(unk):
        for v in range(unk):
            total = inv[m, w, 0, plane].astype(F32) * cpl[m, k, 0, v, plane].astype(F32)
            for u in range(1, unk):
                total = total + inv[m, w, u, plane].astype(F32) * cpl[m, k, u, v, plane].astype(F32)
            out.append(total)
    return out


def split3(x):
    hi = x.astype(BF16)
    rest = x - hi.astype(F32)
    mid = rest.astype(BF16)
    lo = (rest - mid.astype(F32)).astype(BF16)
    return hi, mid, lo


def injected(wells, misfit, first, shape):
    members, unk, planes, rows, lanes = shape
    count = planes * rows * lanes
    nwell = wells.shape[1]
    place = wells[...] - first
    inside = (place >= 0) & (place < count)
    line = jnp.where(inside, place // lanes, -1)
    lane = jnp.where(inside, place % lanes, -1)
    lines = lax.broadcasted_iota(jnp.int32, (planes * rows, nwell), 0) == line
    onlane = (lax.broadcasted_iota(jnp.int32, (lanes, nwell), 0) == lane).astype(F32).astype(BF16)
    left = []
    for m in range(members):
        for u in range(unk):
            left.append(jnp.where(lines, misfit[m, u : u + 1, :], 0.0))
    stacked = jnp.concatenate(split3(jnp.concatenate(left, axis=0)), axis=0)
    full = lax.dot_general(stacked, onlane, (((1,), (1,)), ((), ())), preferred_element_type=F32)
    n = members * unk * planes * rows
    total = full[:n] + full[n : 2 * n] + full[2 * n :]
    return total.reshape(shape)


def first_kernel(out):
    out[...] = jnp.zeros_like(out)


def start_kernel(pos, _, wells, misfit, later, cpl, inv, src, nxt_out, intra_out, cross_out):
    shape = src.shape
    members, unk, planes = shape[:3]
    even = pos[0] % 2 == 0
    count = planes * shape[3] * shape[4]
    src[...] = later[...] + injected(wells, misfit, pos[0] * count, shape)
    for m in range(members):
        s = [src[m, u] for u in range(unk)]
        a = apply_inverse(inv, m, s)
        nxt, up, down = two_sweep_payload(cpl, inv, m, s, a)
        up = up + transfer_blocks(cpl, inv, m, 0, planes - 1, unk)
        down = down + transfer_blocks(cpl, inv, m, 1, 0, unk)
        for u in range(unk):
            nxt_out[m, u] = nxt[u]
        for j in range(len(up)):
            intra_out[m, j] = jnp.where(even, up[j], down[j])
            cross_out[m, j] = jnp.where(even, down[j], up[j])


def incoming(pos, last, m, unk, near, far):
    even = pos[0] % 2 == 0
    has_cross = (pos[0] != 0) & (pos[0] != last)
    sides = []
    for sent, got, block in (near, far):
        first = [got(m, v) for v in range(unk)]
        second = []
        for v in range(unk):
            total = got(m, unk + v)
            for w in range(unk):
                total = total - block(m, 2 * unk + w * unk + v) * sent(m, w)
            second.append(total)
        sides.append((first, second))
    out = []
    for n in range(2):
        low, high = [], []
        for v in range(unk):
            near_v = sides[0][n][v]
            far_v = jnp.where(has_cross, sides[1][n][v], 0.0)
            low.append(jnp.where(even, far_v, near_v))
            high.append(jnp.where(even, near_v, far_v))
        out.append([jnp.stack([lo, hi], axis=0) for lo, hi in zip(low, high)])
    return out


def reader(ref):
    return lambda m, j: ref[m, j]


def either(pos, if_even, if_odd):
    even = pos[0] % 2 == 0
    return lambda m, j: jnp.where(even, if_even[m, j], if_odd[m, j])


def finish_two(cpl, inv, m, src, nxt, arrived):
    a1 = [x - d for x, d in zip(nxt, apply_inverse(inv, m, arrived[0]))]
    inner, _, _ = local_coupling(cpl, m, a1)
    return apply_inverse(inv, m, [s - b - p for s, b, p in zip(src, inner, arrived[1])])


def advance(pos, last, src, nxt, sent_near, sent_far, got_near, got_far, cpl, inv, nxt_out, near_out, far_out):
    members, unk = src.shape[:2]
    even = pos[0] % 2 == 0
    near = (reader(sent_near), reader(got_near), reader(got_near))
    far = (reader(sent_far), reader(got_far), reader(got_far))
    for m in range(members):
        arrived = incoming(pos, last, m, unk, near, far)
        s = [src[m, u] for u in range(unk)]
        a = finish_two(cpl, inv, m, s, [nxt[m, u] for u in range(unk)], arrived)
        ahead, up, down = two_sweep_payload(cpl, inv, m, s, a)
        for u in range(unk):
            nxt_out[m, u] = ahead[u]
        for j in range(len(up)):
            near_out[m, j] = jnp.where(even, up[j], down[j])
            far_out[m, j] = jnp.where(even, down[j], up[j])


def make_even_middle(last):
    def even_middle(*refs):
        pos, outs = refs[0], refs[9:]

        @pl.when(pos[0] % 2 == 0)
        def _():
            advance(pos, last, *refs[1:9], *outs)

        @pl.when(pos[0] % 2 == 1)
        def _():
            for out in outs:
                out[...] = jnp.zeros_like(out)

    return even_middle


def make_odd_middle(last):
    def odd_middle(*refs):
        pos, (nxt_even, near_even), outs = refs[0], refs[9:11], refs[11:]

        @pl.when(pos[0] % 2 == 1)
        def _():
            advance(pos, last, *refs[1:9], *outs)

        @pl.when(pos[0] % 2 == 0)
        def _():
            outs[0][...] = nxt_even[...]
            outs[1][...] = near_even[...]
            outs[2][...] = jnp.zeros_like(outs[2])

    return odd_middle


def select_kernel(pos, bmap, sens, onehot, turned):
    rows, lanes = bmap.shape[1:]
    nblk = onehot.shape[0]
    core = pos[0] % 2
    slot = lax.broadcasted_iota(jnp.int32, (nblk, lanes), 0)
    half_rows = nblk // 2
    parity = jnp.where(slot < half_rows, core, 1 - core)
    within = jnp.where(slot < half_rows, slot, slot - half_rows)
    block = (within // BLK_DEV * 2 + parity) * BLK_DEV + within % BLK_DEV
    for g in range(bmap.shape[0] * rows):
        row = bmap[g // rows, g % rows : g % rows + 1, :]
        onehot[:, g * lanes : (g + 1) * lanes] = (block == row).astype(F32).astype(BF16)
    for m in range(sens.shape[0]):
        for u in range(sens.shape[1]):
            for g in range(bmap.shape[0] * rows):
                turned[m, u, g] = sens[m, u, g // rows, g % rows].astype(F32).T


def make_end(last, nblk):
    def end_kernel(
        pos, src, nxt, block_near, block_even, block_odd, sent_near, sent_even, sent_odd, got_near, got_even, got_odd,
        cpl, inv, onehot, turned, adj_out, mine_out, other_out, adj, grads, sems,
    ):
        members, unk, planes, rows, lanes = src.shape
        params = turned.shape[-2]
        groups = planes * rows
        half_rows = nblk // 2
        near = (reader(sent_near), reader(got_near), reader(block_near))
        far = (
            either(pos, sent_even, sent_odd), either(pos, got_even, got_odd), either(pos, block_even, block_odd),
        )
        for m in range(members):
            arrived = incoming(pos, last, m, unk, near, far)
            a = finish_two(
                cpl, inv, m, [src[m, u] for u in range(unk)], [nxt[m, u] for u in range(unk)], arrived
            )
            for u in range(unk):
                adj[m, u] = a[u]
        store = pltpu.make_async_copy(adj, adj_out, sems.at[0])
        store.start()
        step = 32
        for g in range(groups):
            x, y = g // rows, g % rows
            for p in range(0, params, step):
                total = None
                for m in range(members):
                    for u in range(unk):
                        term = adj[m, u, x, y : y + 1] * turned[m, u, g, p : p + step]
                        total = term if total is None else total + term
                hi = total.astype(BF16)
                lo = (total - hi.astype(F32)).astype(BF16)
                grads[p : p + step, g * lanes : (g + 1) * lanes] = hi
                grads[params + p : params + p + step, g * lanes : (g + 1) * lanes] = lo
        both = lax.dot_general(
            onehot[...], grads[...], (((1,), (1,)), ((), ())), preferred_element_type=F32
        )
        out = both[:, :params] + both[:, params:]
        mine_out[...] = out[:half_rows]
        other_out[...] = out[half_rows:]
        store.wait()

    return end_kernel


VM = pl.BlockSpec(memory_space=pltpu.VMEM)
SM = pl.BlockSpec(memory_space=pltpu.SMEM)
HB = pl.BlockSpec(memory_space=pltpu.HBM)
MIB = 1 << 20


def room(mib):
    return pltpu.CompilerParams(vmem_limit_bytes=mib * MIB)


def busy(flops):
    return pl.CostEstimate(flops=flops, bytes_accessed=0, transcendentals=0)


def shaped(*shape):
    return jax.ShapeDtypeStruct(shape, F32)


def timestep(later_adjoint, coupling, diag_inverse, sensitivity, well_cells, well_misfit, block_map):
    members, unk, planes, rows, lanes = later_adjoint.shape
    count = planes * rows * lanes
    params = sensitivity.shape[-1]
    ranks = lax.axis_size("cells")
    nblk = ranks * BLK_DEV
    pos = lax.axis_index("cells").astype(jnp.int32).reshape(1)
    intra_pairs = [(i, i ^ 1) for i in range(ranks)]
    up_pairs = [(i, (i + 1) % ranks) for i in range(ranks)]
    down_pairs = [((i + 1) % ranks, i) for i in range(ranks)]

    field = shaped(members, unk, planes, rows, lanes)
    first_size = 2 * unk + unk * unk
    wells = well_cells.reshape(1, -1)
    cpl, inv = coupling, diag_inverse
    dma = pltpu.SemaphoreType.DMA
    token = pl.pallas_call(
        first_kernel,
        out_shape=shaped(8, 128),
        out_specs=VM,
        compiler_params=room(1),
        cost_estimate=busy(1 << 31),
    )()
    src, nxt, near, far = pl.pallas_call(
        start_kernel,
        out_shape=(field, field, shaped(members, first_size, rows, lanes), shaped(members, first_size, rows, lanes)),
        in_specs=[SM] + [VM] * 6,
        out_specs=(VM,) * 4,
        compiler_params=room(6),
    )(pos, token, wells, well_misfit, later_adjoint, coupling, diag_inverse)
    got_up = lax.ppermute(far, "cells", up_pairs)
    got_down = lax.ppermute(far, "cells", down_pairs)
    got_near = lax.ppermute(near, "cells", intra_pairs)
    onehot, turned = pl.pallas_call(
        select_kernel,
        out_shape=(
            jax.ShapeDtypeStruct((nblk, count), BF16), shaped(members, unk, planes * rows, params, lanes)
        ),
        in_specs=[SM, VM, VM],
        out_specs=(VM, VM),
        compiler_params=room(6),
        cost_estimate=busy(1 << 24),
    )(pos, block_map, sensitivity)
    wide = shaped(members, 2 * unk, rows, lanes)
    nxt_even, near_even, far_even = pl.pallas_call(
        make_even_middle(ranks - 1),
        out_shape=(field, wide, wide),
        in_specs=[SM] + [VM] * 8,
        out_specs=(VM, VM, VM),
        compiler_params=room(6),
        cost_estimate=busy(1 << 31),
    )(pos, src, nxt, near, far, got_near, got_up, cpl, inv)
    got_down2 = lax.ppermute(far_even, "cells", down_pairs)
    nxt2, near2, far_odd = pl.pallas_call(
        make_odd_middle(ranks - 1),
        out_shape=(field, wide, wide),
        in_specs=[SM] + [VM] * 10,
        out_specs=(VM, VM, VM),
        compiler_params=room(6),
        cost_estimate=busy(1 << 31),
    )(pos, src, nxt, near, far, got_near, got_down, cpl, inv, nxt_even, near_even)
    got_up2 = lax.ppermute(far_odd, "cells", up_pairs)
    got_near2 = lax.ppermute(near2, "cells", intra_pairs)
    adjoint, mine, other = pl.pallas_call(
        make_end(ranks - 1, nblk),
        out_shape=(field, shaped(nblk // 2, params), shaped(nblk // 2, params)),
        in_specs=[SM] + [VM] * 15,
        out_specs=(HB, VM, VM),
        scratch_shapes=[pltpu.VMEM(field.shape, F32), pltpu.VMEM((2 * params, count), BF16), dma((1,))],
        compiler_params=room(16),
    )(
        pos, src, nxt2, got_near, got_up, got_down, near2, far_even, far_odd, got_near2, got_up2, got_down2,
        cpl, inv, onehot, turned,
    )
    chips = ranks // 2
    half = mine + lax.ppermute(other, "cells", intra_pairs)
    same_core = [[core + 2 * chip for chip in range(chips)] for core in range(2)]
    parts = lax.all_to_all(
        half.reshape(chips, BLK_DEV, params), "cells", 0, 0, tiled=True, axis_index_groups=same_core
    )
    owned = jnp.sum(parts, axis=0)
    gradient = owned + lax.ppermute(owned, "ens", [(0, 1), (1, 0)])
    return (adjoint, gradient)


def solution(mesh):
    placed = (
        P("ens", None, "cells", None, None),
        P("ens", None, None, None, "cells", None, None),
        P("ens", None, None, "cells", None, None),
        P("ens", None, "cells", None, None, None),
        P(),
        P("ens", None, None),
        P("cells", None, None),
    )
    return jax.shard_map(
        timestep,
        mesh=mesh,
        in_specs=placed,
        out_specs=(P("ens", None, "cells", None, None), P("cells", None)),
        check_vma=False,
    )
```

```python
import jax
import jax.numpy as jnp
from jax import lax
from jax.experimental import pallas as pl
from jax.experimental.pallas import tpu as pltpu
from jax.sharding import PartitionSpec as P


BLK_DEV = 4
F32 = jnp.float32
BF16 = jnp.bfloat16


def shift_lanes(x, by):
    size = x.shape[2]
    lane = lax.broadcasted_iota(jnp.int32, x.shape, 2)
    keep = lane >= 1 if by == 1 else lane < size - 1
    return jnp.where(keep, pltpu.roll(x, by % size, 2), 0.0)


def shift_rows(x, by):
    size = x.shape[1]
    row = lax.broadcasted_iota(jnp.int32, x.shape, 1)
    keep = row >= 1 if by == 1 else row < size - 1
    return jnp.where(keep, pltpu.roll(x, by % size, 1), 0.0)


def products(cpl, m, k, a):
    unk = len(a)
    out = []
    for v in range(unk):
        total = cpl[m, k, 0, v].astype(F32) * a[0]
        for u in range(1, unk):
            total = total + cpl[m, k, u, v].astype(F32) * a[u]
        out.append(total)
    return out


def local_coupling(cpl, m, a):
    unk = len(a)
    terms = [products(cpl, m, k, a) for k in range(6)]
    inner, up, down = [], [], []
    for v in range(unk):
        t = [terms[k][v] for k in range(6)]
        planes = t[0].shape[0]
        zero = jnp.zeros_like(t[0][:1])
        total = jnp.concatenate([zero, t[0][: planes - 1]], axis=0)
        total = total + jnp.concatenate([t[1][1:], zero], axis=0)
        total = total + shift_rows(t[2], 1) + shift_rows(t[3], -1)
        total = total + shift_lanes(t[4], 1) + shift_lanes(t[5], -1)
        inner.append(total)
        up.append(t[0][planes - 1])
        down.append(t[1][0])
    return inner, up, down


def apply_inverse(inv, m, r):
    unk = len(r)
    out = []
    for v in range(unk):
        total = inv[m, 0, v].astype(F32) * r[0]
        for w in range(1, unk):
            total = total + inv[m, w, v].astype(F32) * r[w]
        out.append(total)
    return out


def plane_products(cpl, m, k, plane, a):
    unk = len(a)
    out = []
    for v in range(unk):
        total = cpl[m, k, 0, v, plane].astype(F32) * a[0]
        for u in range(1, unk):
            total = total + cpl[m, k, u, v, plane].astype(F32) * a[u]
        out.append(total)
    return out


def two_sweep_payload(cpl, inv, m, src, a):
    planes = a[0].shape[0]
    inner, up0, down0 = local_coupling(cpl, m, a)
    nxt = apply_inverse(inv, m, [s - b for s, b in zip(src, inner)])
    up1 = plane_products(cpl, m, 0, planes - 1, [x[planes - 1] for x in nxt])
    down1 = plane_products(cpl, m, 1, 0, [x[0] for x in nxt])
    return nxt, up0 + up1, down0 + down1


def transfer_blocks(cpl, inv, m, k, plane, unk):
    out = []
    for w in range(unk):
        for v in range(unk):
            total = inv[m, w, 0, plane].astype(F32) * cpl[m, k, 0, v, plane].astype(F32)
            for u in range(1, unk):
                total = total + inv[m, w, u, plane].astype(F32) * cpl[m, k, u, v, plane].astype(F32)
            out.append(total)
    return out


def split3(x):
    hi = x.astype(BF16)
    rest = x - hi.astype(F32)
    mid = rest.astype(BF16)
    lo = (rest - mid.astype(F32)).astype(BF16)
    return hi, mid, lo


def injected(wells, misfit, first, shape):
    members, unk, planes, rows, lanes = shape
    count = planes * rows * lanes
    nwell = wells.shape[1]
    place = wells[...] - first
    inside = (place >= 0) & (place < count)
    line = jnp.where(inside, place // lanes, -1)
    lane = jnp.where(inside, place % lanes, -1)
    lines = lax.broadcasted_iota(jnp.int32, (planes * rows, nwell), 0) == line
    onlane = (lax.broadcasted_iota(jnp.int32, (lanes, nwell), 0) == lane).astype(F32).astype(BF16)
    left = []
    for m in range(members):
        for u in range(unk):
            left.append(jnp.where(lines, misfit[m, u : u + 1, :], 0.0))
    stacked = jnp.concatenate(split3(jnp.concatenate(left, axis=0)), axis=0)
    full = lax.dot_general(stacked, onlane, (((1,), (1,)), ((), ())), preferred_element_type=F32)
    n = members * unk * planes * rows
    total = full[:n] + full[n : 2 * n] + full[2 * n :]
    return total.reshape(shape)


def first_kernel(out):
    out[...] = jnp.zeros_like(out)


def start_kernel(pos, _, wells, misfit, later, cpl, inv, src, nxt_out, intra_out, cross_out):
    shape = src.shape
    members, unk, planes = shape[:3]
    even = pos[0] % 2 == 0
    count = planes * shape[3] * shape[4]
    src[...] = later[...] + injected(wells, misfit, pos[0] * count, shape)
    for m in range(members):
        s = [src[m, u] for u in range(unk)]
        a = apply_inverse(inv, m, s)
        nxt, up, down = two_sweep_payload(cpl, inv, m, s, a)
        up = up + transfer_blocks(cpl, inv, m, 0, planes - 1, unk)
        down = down + transfer_blocks(cpl, inv, m, 1, 0, unk)
        for u in range(unk):
            nxt_out[m, u] = nxt[u]
        for j in range(len(up)):
            intra_out[m, j] = jnp.where(even, up[j], down[j])
            cross_out[m, j] = jnp.where(even, down[j], up[j])


def incoming(pos, last, m, unk, near, far):
    even = pos[0] % 2 == 0
    has_cross = (pos[0] != 0) & (pos[0] != last)
    sides = []
    for sent, got, block in (near, far):
        first = [got(m, v) for v in range(unk)]
        second = []
        for v in range(unk):
            total = got(m, unk + v)
            for w in range(unk):
                total = total - block(m, 2 * unk + w * unk + v) * sent(m, w)
            second.append(total)
        sides.append((first, second))
    out = []
    for n in range(2):
        low, high = [], []
        for v in range(unk):
            near_v = sides[0][n][v]
            far_v = jnp.where(has_cross, sides[1][n][v], 0.0)
            low.append(jnp.where(even, far_v, near_v))
            high.append(jnp.where(even, near_v, far_v))
        out.append([jnp.stack([lo, hi], axis=0) for lo, hi in zip(low, high)])
    return out


def reader(ref):
    return lambda m, j: ref[m, j]


def either(pos, if_even, if_odd):
    even = pos[0] % 2 == 0
    return lambda m, j: jnp.where(even, if_even[m, j], if_odd[m, j])


def finish_two(cpl, inv, m, src, nxt, arrived):
    a1 = [x - d for x, d in zip(nxt, apply_inverse(inv, m, arrived[0]))]
    inner, _, _ = local_coupling(cpl, m, a1)
    return apply_inverse(inv, m, [s - b - p for s, b, p in zip(src, inner, arrived[1])])


def advance(pos, last, src, nxt, sent_near, sent_far, got_near, got_far, cpl, inv, nxt_out, near_out, far_out):
    members, unk = src.shape[:2]
    even = pos[0] % 2 == 0
    near = (reader(sent_near), reader(got_near), reader(got_near))
    far = (reader(sent_far), reader(got_far), reader(got_far))
    for m in range(members):
        arrived = incoming(pos, last, m, unk, near, far)
        s = [src[m, u] for u in range(unk)]
        a = finish_two(cpl, inv, m, s, [nxt[m, u] for u in range(unk)], arrived)
        ahead, up, down = two_sweep_payload(cpl, inv, m, s, a)
        for u in range(unk):
            nxt_out[m, u] = ahead[u]
        for j in range(len(up)):
            near_out[m, j] = jnp.where(even, up[j], down[j])
            far_out[m, j] = jnp.where(even, down[j], up[j])


def make_even_middle(last):
    def even_middle(*refs):
        pos, outs = refs[0], refs[9:]

        @pl.when(pos[0] % 2 == 0)
        def _():
            advance(pos, last, *refs[1:9], *outs)

        @pl.when(pos[0] % 2 == 1)
        def _():
            for out in outs:
                out[...] = jnp.zeros_like(out)

    return even_middle


def make_odd_middle(last):
    def odd_middle(*refs):
        pos, (nxt_even, near_even), outs = refs[0], refs[9:11], refs[11:]

        @pl.when(pos[0] % 2 == 1)
        def _():
            advance(pos, last, *refs[1:9], *outs)

        @pl.when(pos[0] % 2 == 0)
        def _():
            outs[0][...] = nxt_even[...]
            outs[1][...] = near_even[...]
            outs[2][...] = jnp.zeros_like(outs[2])

    return odd_middle


def select_kernel(pos, bmap, sens, onehot, turned):
    rows, lanes = bmap.shape[1:]
    nblk = onehot.shape[0]
    core = pos[0] % 2
    slot = lax.broadcasted_iota(jnp.int32, (nblk, lanes), 0)
    half_rows = nblk // 2
    parity = jnp.where(slot < half_rows, core, 1 - core)
    within = jnp.where(slot < half_rows, slot, slot - half_rows)
    block = (within // BLK_DEV * 2 + parity) * BLK_DEV + within % BLK_DEV
    for g in range(bmap.shape[0] * rows):
        row = bmap[g // rows, g % rows : g % rows + 1, :]
        onehot[:, g * lanes : (g + 1) * lanes] = (block == row).astype(F32).astype(BF16)
    for m in range(sens.shape[0]):
        for u in range(sens.shape[1]):
            for g in range(bmap.shape[0] * rows):
                turned[m, u, g] = sens[m, u, g // rows, g % rows].astype(F32).T


def make_end(last, nblk):
    def end_kernel(
        pos, src, nxt, block_near, block_even, block_odd, sent_near, sent_even, sent_odd, got_near, got_even, got_odd,
        cpl, inv, onehot, turned, adj_out, mine_out, other_out, adj, grads, sems,
    ):
        members, unk, planes, rows, lanes = src.shape
        params = turned.shape[-2]
        groups = planes * rows
        half_rows = nblk // 2
        near = (reader(sent_near), reader(got_near), reader(block_near))
        far = (
            either(pos, sent_even, sent_odd), either(pos, got_even, got_odd), either(pos, block_even, block_odd),
        )
        for m in range(members):
            arrived = incoming(pos, last, m, unk, near, far)
            a = finish_two(
                cpl, inv, m, [src[m, u] for u in range(unk)], [nxt[m, u] for u in range(unk)], arrived
            )
            for u in range(unk):
                adj[m, u] = a[u]
        store = pltpu.make_async_copy(adj, adj_out, sems.at[0])
        store.start()
        step = 32
        for g in range(groups):
            x, y = g // rows, g % rows
            for p in range(0, params, step):
                total = None
                for m in range(members):
                    for u in range(unk):
                        term = adj[m, u, x, y : y + 1] * turned[m, u, g, p : p + step]
                        total = term if total is None else total + term
                hi = total.astype(BF16)
                lo = (total - hi.astype(F32)).astype(BF16)
                grads[p : p + step, g * lanes : (g + 1) * lanes] = hi
                grads[params + p : params + p + step, g * lanes : (g + 1) * lanes] = lo
        both = lax.dot_general(
            onehot[...], grads[...], (((1,), (1,)), ((), ())), preferred_element_type=F32
        )
        out = both[:, :params] + both[:, params:]
        mine_out[...] = out[:half_rows]
        other_out[...] = out[half_rows:]
        store.wait()

    return end_kernel


VM = pl.BlockSpec(memory_space=pltpu.VMEM)
SM = pl.BlockSpec(memory_space=pltpu.SMEM)
HB = pl.BlockSpec(memory_space=pltpu.HBM)
MIB = 1 << 20


def room(mib):
    return pltpu.CompilerParams(vmem_limit_bytes=mib * MIB)


def busy(flops):
    return pl.CostEstimate(flops=flops, bytes_accessed=0, transcendentals=0)


def shaped(*shape):
    return jax.ShapeDtypeStruct(shape, F32)


def closed_ring(ranks):
    target = {i: i + 1 for i in range(ranks - 1)}
    row = ranks // 8
    if ranks % 64 or row < 8:
        target[ranks - 1] = 0
        return sorted(target.items())
    spare = ranks - 1
    stops = [row * k + row - 2 for k in range(3, -1, -1)] + list(range(row - 6, 0, -4))
    for even in stops:
        target[spare] = even + 1
        spare = even
    target[spare] = 0
    return sorted(target.items())


def timestep(later_adjoint, coupling, diag_inverse, sensitivity, well_cells, well_misfit, block_map):
    members, unk, planes, rows, lanes = later_adjoint.shape
    count = planes * rows * lanes
    params = sensitivity.shape[-1]
    ranks = lax.axis_size("cells")
    nblk = ranks * BLK_DEV
    pos = lax.axis_index("cells").astype(jnp.int32).reshape(1)
    intra_pairs = [(i, i ^ 1) for i in range(ranks)]
    up_pairs = closed_ring(ranks)
    down_pairs = [(there, here) for here, there in up_pairs]

    field = shaped(members, unk, planes, rows, lanes)
    first_size = 2 * unk + unk * unk
    wells = well_cells.reshape(1, -1)
    cpl, inv = coupling, diag_inverse
    dma = pltpu.SemaphoreType.DMA
    token = pl.pallas_call(
        first_kernel,
        out_shape=shaped(8, 128),
        out_specs=VM,
        compiler_params=room(1),
        cost_estimate=busy(1 << 31),
    )()
    src, nxt, near, far = pl.pallas_call(
        start_kernel,
        out_shape=(field, field, shaped(members, first_size, rows, lanes), shaped(members, first_size, rows, lanes)),
        in_specs=[SM] + [VM] * 6,
        out_specs=(VM,) * 4,
        compiler_params=room(6),
    )(pos, token, wells, well_misfit, later_adjoint, coupling, diag_inverse)
    got_up = lax.ppermute(far, "cells", up_pairs)
    got_down = lax.ppermute(far, "cells", down_pairs)
    got_near = lax.ppermute(near, "cells", intra_pairs)
    onehot, turned = pl.pallas_call(
        select_kernel,
        out_shape=(
            jax.ShapeDtypeStruct((nblk, count), BF16), shaped(members, unk, planes * rows, params, lanes)
        ),
        in_specs=[SM, VM, VM],
        out_specs=(VM, VM),
        compiler_params=room(6),
        cost_estimate=busy(1 << 24),
    )(pos, block_map, sensitivity)
    wide = shaped(members, 2 * unk, rows, lanes)
    nxt_even, near_even, far_even = pl.pallas_call(
        make_even_middle(ranks - 1),
        out_shape=(field, wide, wide),
        in_specs=[SM] + [VM] * 8,
        out_specs=(VM, VM, VM),
        compiler_params=room(6),
        cost_estimate=busy(1 << 31),
    )(pos, src, nxt, near, far, got_near, got_up, cpl, inv)
    got_down2 = lax.ppermute(far_even, "cells", down_pairs)
    nxt2, near2, far_odd = pl.pallas_call(
        make_odd_middle(ranks - 1),
        out_shape=(field, wide, wide),
        in_specs=[SM] + [VM] * 10,
        out_specs=(VM, VM, VM),
        compiler_params=room(6),
        cost_estimate=busy(1 << 31),
    )(pos, src, nxt, near, far, got_near, got_down, cpl, inv, nxt_even, near_even)
    got_up2 = lax.ppermute(far_odd, "cells", up_pairs)
    got_near2 = lax.ppermute(near2, "cells", intra_pairs)
    adjoint, mine, other = pl.pallas_call(
        make_end(ranks - 1, nblk),
        out_shape=(field, shaped(nblk // 2, params), shaped(nblk // 2, params)),
        in_specs=[SM] + [VM] * 15,
        out_specs=(HB, VM, VM),
        scratch_shapes=[pltpu.VMEM(field.shape, F32), pltpu.VMEM((2 * params, count), BF16), dma((1,))],
        compiler_params=room(16),
    )(
        pos, src, nxt2, got_near, got_up, got_down, near2, far_even, far_odd, got_near2, got_up2, got_down2,
        cpl, inv, onehot, turned,
    )
    chips = ranks // 2
    half = mine + lax.ppermute(other, "cells", intra_pairs)
    same_core = [[core + 2 * chip for chip in range(chips)] for core in range(2)]
    parts = lax.all_to_all(
        half.reshape(chips, BLK_DEV, params), "cells", 0, 0, tiled=True, axis_index_groups=same_core
    )
    owned = jnp.sum(parts, axis=0)
    gradient = owned + lax.ppermute(owned, "ens", [(0, 1), (1, 0)])
    return (adjoint, gradient)


def solution(mesh):
    placed = (
        P("ens", None, "cells", None, None),
        P("ens", None, None, None, "cells", None, None),
        P("ens", None, None, "cells", None, None),
        P("ens", None, "cells", None, None, None),
        P(),
        P("ens", None, None),
        P("cells", None, None),
    )
    return jax.shard_map(
        timestep,
        mesh=mesh,
        in_specs=placed,
        out_specs=(P("ens", None, "cells", None, None), P("cells", None)),
        check_vma=False,
    )
```

```python
import jax
import jax.numpy as jnp
from jax import lax
from jax.experimental import pallas as pl
from jax.experimental.pallas import tpu as pltpu
from jax.sharding import PartitionSpec as P


BLK_DEV = 4
F32 = jnp.float32
BF16 = jnp.bfloat16


def shift_lanes(x, by):
    size = x.shape[2]
    lane = lax.broadcasted_iota(jnp.int32, x.shape, 2)
    keep = lane >= 1 if by == 1 else lane < size - 1
    return jnp.where(keep, pltpu.roll(x, by % size, 2), 0.0)


def shift_rows(x, by):
    size = x.shape[1]
    row = lax.broadcasted_iota(jnp.int32, x.shape, 1)
    keep = row >= 1 if by == 1 else row < size - 1
    return jnp.where(keep, pltpu.roll(x, by % size, 1), 0.0)


def products(cpl, m, k, a):
    unk = len(a)
    out = []
    for v in range(unk):
        total = cpl[m, k, 0, v].astype(F32) * a[0]
        for u in range(1, unk):
            total = total + cpl[m, k, u, v].astype(F32) * a[u]
        out.append(total)
    return out


def local_coupling(cpl, m, a):
    unk = len(a)
    terms = [products(cpl, m, k, a) for k in range(6)]
    inner, up, down = [], [], []
    for v in range(unk):
        t = [terms[k][v] for k in range(6)]
        planes = t[0].shape[0]
        zero = jnp.zeros_like(t[0][:1])
        total = jnp.concatenate([zero, t[0][: planes - 1]], axis=0)
        total = total + jnp.concatenate([t[1][1:], zero], axis=0)
        total = total + shift_rows(t[2], 1) + shift_rows(t[3], -1)
        total = total + shift_lanes(t[4], 1) + shift_lanes(t[5], -1)
        inner.append(total)
        up.append(t[0][planes - 1])
        down.append(t[1][0])
    return inner, up, down


def apply_inverse(inv, m, r):
    unk = len(r)
    out = []
    for v in range(unk):
        total = inv[m, 0, v].astype(F32) * r[0]
        for w in range(1, unk):
            total = total + inv[m, w, v].astype(F32) * r[w]
        out.append(total)
    return out


def plane_products(cpl, m, k, plane, a):
    unk = len(a)
    out = []
    for v in range(unk):
        total = cpl[m, k, 0, v, plane].astype(F32) * a[0]
        for u in range(1, unk):
            total = total + cpl[m, k, u, v, plane].astype(F32) * a[u]
        out.append(total)
    return out


def two_sweep_payload(cpl, inv, m, src, a):
    planes = a[0].shape[0]
    inner, up0, down0 = local_coupling(cpl, m, a)
    nxt = apply_inverse(inv, m, [s - b for s, b in zip(src, inner)])
    up1 = plane_products(cpl, m, 0, planes - 1, [x[planes - 1] for x in nxt])
    down1 = plane_products(cpl, m, 1, 0, [x[0] for x in nxt])
    return nxt, up0 + up1, down0 + down1


def transfer_blocks(cpl, inv, m, k, plane, unk):
    out = []
    for w in range(unk):
        for v in range(unk):
            total = inv[m, w, 0, plane].astype(F32) * cpl[m, k, 0, v, plane].astype(F32)
            for u in range(1, unk):
                total = total + inv[m, w, u, plane].astype(F32) * cpl[m, k, u, v, plane].astype(F32)
            out.append(total)
    return out


def split3(x):
    hi = x.astype(BF16)
    rest = x - hi.astype(F32)
    mid = rest.astype(BF16)
    lo = (rest - mid.astype(F32)).astype(BF16)
    return hi, mid, lo


def injected(wells, misfit, first, shape):
    members, unk, planes, rows, lanes = shape
    count = planes * rows * lanes
    nwell = wells.shape[1]
    place = wells[...] - first
    inside = (place >= 0) & (place < count)
    line = jnp.where(inside, place // lanes, -1)
    lane = jnp.where(inside, place % lanes, -1)
    lines = lax.broadcasted_iota(jnp.int32, (planes * rows, nwell), 0) == line
    onlane = (lax.broadcasted_iota(jnp.int32, (lanes, nwell), 0) == lane).astype(F32).astype(BF16)
    left = []
    for m in range(members):
        for u in range(unk):
            left.append(jnp.where(lines, misfit[m, u : u + 1, :], 0.0))
    stacked = jnp.concatenate(split3(jnp.concatenate(left, axis=0)), axis=0)
    full = lax.dot_general(stacked, onlane, (((1,), (1,)), ((), ())), preferred_element_type=F32)
    n = members * unk * planes * rows
    total = full[:n] + full[n : 2 * n] + full[2 * n :]
    return total.reshape(shape)


def first_kernel(out):
    out[...] = jnp.zeros_like(out)


def start_kernel(pos, _, wells, misfit, later, cpl, inv, src, nxt_out, intra_out, cross_out):
    shape = src.shape
    members, unk, planes = shape[:3]
    even = pos[0] % 2 == 0
    count = planes * shape[3] * shape[4]
    src[...] = later[...] + injected(wells, misfit, pos[0] * count, shape)
    for m in range(members):
        s = [src[m, u] for u in range(unk)]
        a = apply_inverse(inv, m, s)
        nxt, up, down = two_sweep_payload(cpl, inv, m, s, a)
        up = up + transfer_blocks(cpl, inv, m, 0, planes - 1, unk)
        down = down + transfer_blocks(cpl, inv, m, 1, 0, unk)
        for u in range(unk):
            nxt_out[m, u] = nxt[u]
        for j in range(len(up)):
            intra_out[m, j] = jnp.where(even, up[j], down[j])
            cross_out[m, j] = jnp.where(even, down[j], up[j])


def incoming(pos, last, m, unk, near, far):
    even = pos[0] % 2 == 0
    has_cross = (pos[0] != 0) & (pos[0] != last)
    sides = []
    for sent, got, block in (near, far):
        first = [got(m, v) for v in range(unk)]
        second = []
        for v in range(unk):
            total = got(m, unk + v)
            for w in range(unk):
                total = total - block(m, 2 * unk + w * unk + v) * sent(m, w)
            second.append(total)
        sides.append((first, second))
    out = []
    for n in range(2):
        low, high = [], []
        for v in range(unk):
            near_v = sides[0][n][v]
            far_v = jnp.where(has_cross, sides[1][n][v], 0.0)
            low.append(jnp.where(even, far_v, near_v))
            high.append(jnp.where(even, near_v, far_v))
        out.append([jnp.stack([lo, hi], axis=0) for lo, hi in zip(low, high)])
    return out


def reader(ref):
    return lambda m, j: ref[m, j]


def either(pos, if_even, if_odd):
    even = pos[0] % 2 == 0
    return lambda m, j: jnp.where(even, if_even[m, j], if_odd[m, j])


def finish_two(cpl, inv, m, src, nxt, arrived):
    a1 = [x - d for x, d in zip(nxt, apply_inverse(inv, m, arrived[0]))]
    inner, _, _ = local_coupling(cpl, m, a1)
    return apply_inverse(inv, m, [s - b - p for s, b, p in zip(src, inner, arrived[1])])


def advance(pos, last, src, nxt, sent_near, sent_far, got_near, got_far, cpl, inv, nxt_out, near_out, far_out):
    members, unk = src.shape[:2]
    even = pos[0] % 2 == 0
    near = (reader(sent_near), reader(got_near), reader(got_near))
    far = (reader(sent_far), reader(got_far), reader(got_far))
    for m in range(members):
        arrived = incoming(pos, last, m, unk, near, far)
        s = [src[m, u] for u in range(unk)]
        a = finish_two(cpl, inv, m, s, [nxt[m, u] for u in range(unk)], arrived)
        ahead, up, down = two_sweep_payload(cpl, inv, m, s, a)
        for u in range(unk):
            nxt_out[m, u] = ahead[u]
        for j in range(len(up)):
            near_out[m, j] = jnp.where(even, up[j], down[j])
            far_out[m, j] = jnp.where(even, down[j], up[j])


def make_even_middle(last):
    def even_middle(*refs):
        pos, outs = refs[0], refs[9:]

        @pl.when(pos[0] % 2 == 0)
        def _():
            advance(pos, last, *refs[1:9], *outs)

        @pl.when(pos[0] % 2 == 1)
        def _():
            for out in outs:
                out[...] = jnp.zeros_like(out)

    return even_middle


def make_odd_middle(last):
    def odd_middle(*refs):
        pos, (nxt_even, near_even), outs = refs[0], refs[9:11], refs[11:]

        @pl.when(pos[0] % 2 == 1)
        def _():
            advance(pos, last, *refs[1:9], *outs)

        @pl.when(pos[0] % 2 == 0)
        def _():
            outs[0][...] = nxt_even[...]
            outs[1][...] = near_even[...]
            outs[2][...] = jnp.zeros_like(outs[2])

    return odd_middle


def select_kernel(pos, bmap, sens, onehot, turned):
    rows, lanes = bmap.shape[1:]
    nblk = onehot.shape[0]
    core = pos[0] % 2
    slot = lax.broadcasted_iota(jnp.int32, (nblk, lanes), 0)
    half_rows = nblk // 2
    parity = jnp.where(slot < half_rows, core, 1 - core)
    within = jnp.where(slot < half_rows, slot, slot - half_rows)
    block = (within // BLK_DEV * 2 + parity) * BLK_DEV + within % BLK_DEV
    for g in range(bmap.shape[0] * rows):
        row = bmap[g // rows, g % rows : g % rows + 1, :]
        onehot[:, g * lanes : (g + 1) * lanes] = (block == row).astype(F32).astype(BF16)
    for m in range(sens.shape[0]):
        for u in range(sens.shape[1]):
            for g in range(bmap.shape[0] * rows):
                turned[m, u, g] = sens[m, u, g // rows, g % rows].astype(F32).T


def block_sums(rows, grads, params):
    both = lax.dot_general(rows, grads, (((1,), (1,)), ((), ())), preferred_element_type=F32)
    return both[:, :params] + both[:, params:]


def own_kernel(onehot, grads, out):
    out[...] = block_sums(onehot[: out.shape[0]], grads[...], out.shape[1])


def make_end(last, nblk):
    def end_kernel(
        pos, src, nxt, block_near, block_even, block_odd, sent_near, sent_even, sent_odd, got_near, got_even, got_odd,
        cpl, inv, onehot, turned, adj_out, other_out, grads, adj, sems,
    ):
        members, unk, planes, rows, lanes = src.shape
        params = turned.shape[-2]
        groups = planes * rows
        half_rows = nblk // 2
        near = (reader(sent_near), reader(got_near), reader(block_near))
        far = (
            either(pos, sent_even, sent_odd), either(pos, got_even, got_odd), either(pos, block_even, block_odd),
        )
        for m in range(members):
            arrived = incoming(pos, last, m, unk, near, far)
            a = finish_two(
                cpl, inv, m, [src[m, u] for u in range(unk)], [nxt[m, u] for u in range(unk)], arrived
            )
            for u in range(unk):
                adj[m, u] = a[u]
        store = pltpu.make_async_copy(adj, adj_out, sems.at[0])
        store.start()
        step = 32
        for g in range(groups):
            x, y = g // rows, g % rows
            for p in range(0, params, step):
                total = None
                for m in range(members):
                    for u in range(unk):
                        term = adj[m, u, x, y : y + 1] * turned[m, u, g, p : p + step]
                        total = term if total is None else total + term
                hi = total.astype(BF16)
                lo = (total - hi.astype(F32)).astype(BF16)
                grads[p : p + step, g * lanes : (g + 1) * lanes] = hi
                grads[params + p : params + p + step, g * lanes : (g + 1) * lanes] = lo
        other_out[...] = block_sums(onehot[half_rows:], grads[...], params)
        store.wait()

    return end_kernel


VM = pl.BlockSpec(memory_space=pltpu.VMEM)
SM = pl.BlockSpec(memory_space=pltpu.SMEM)
HB = pl.BlockSpec(memory_space=pltpu.HBM)
MIB = 1 << 20


def room(mib):
    return pltpu.CompilerParams(vmem_limit_bytes=mib * MIB)


def busy(flops):
    return pl.CostEstimate(flops=flops, bytes_accessed=0, transcendentals=0)


def shaped(*shape):
    return jax.ShapeDtypeStruct(shape, F32)


def closed_ring(ranks):
    target = {i: i + 1 for i in range(ranks - 1)}
    row = ranks // 8
    if ranks % 64 or row < 8:
        target[ranks - 1] = 0
        return sorted(target.items())
    spare = ranks - 1
    near_end = row - 4
    stops = [ranks - 4] + [row * k + near_end for k in range(3, -1, -1)] + list(range(near_end - 4, 3, -4))
    for even in stops:
        target[spare] = even + 1
        spare = even
    target[spare] = 3
    spare = 2
    target[spare] = 0
    return sorted(target.items())


def timestep(later_adjoint, coupling, diag_inverse, sensitivity, well_cells, well_misfit, block_map):
    members, unk, planes, rows, lanes = later_adjoint.shape
    count = planes * rows * lanes
    params = sensitivity.shape[-1]
    ranks = lax.axis_size("cells")
    nblk = ranks * BLK_DEV
    pos = lax.axis_index("cells").astype(jnp.int32).reshape(1)
    intra_pairs = [(i, i ^ 1) for i in range(ranks)]
    up_pairs = closed_ring(ranks)
    down_pairs = [(there, here) for here, there in up_pairs]

    field = shaped(members, unk, planes, rows, lanes)
    first_size = 2 * unk + unk * unk
    wells = well_cells.reshape(1, -1)
    cpl, inv = coupling, diag_inverse
    dma = pltpu.SemaphoreType.DMA
    token = pl.pallas_call(
        first_kernel,
        out_shape=shaped(8, 128),
        out_specs=VM,
        compiler_params=room(1),
        cost_estimate=busy(1 << 31),
    )()
    src, nxt, near, far = pl.pallas_call(
        start_kernel,
        out_shape=(field, field, shaped(members, first_size, rows, lanes), shaped(members, first_size, rows, lanes)),
        in_specs=[SM] + [VM] * 6,
        out_specs=(VM,) * 4,
        compiler_params=room(6),
    )(pos, token, wells, well_misfit, later_adjoint, coupling, diag_inverse)
    got_up = lax.ppermute(far, "cells", up_pairs)
    got_down = lax.ppermute(far, "cells", down_pairs)
    got_near = lax.ppermute(near, "cells", intra_pairs)
    onehot, turned = pl.pallas_call(
        select_kernel,
        out_shape=(
            jax.ShapeDtypeStruct((nblk, count), BF16), shaped(members, unk, planes * rows, params, lanes)
        ),
        in_specs=[SM, VM, VM],
        out_specs=(VM, VM),
        compiler_params=room(6),
        cost_estimate=busy(1 << 24),
    )(pos, block_map, sensitivity)
    wide = shaped(members, 2 * unk, rows, lanes)
    nxt_even, near_even, far_even = pl.pallas_call(
        make_even_middle(ranks - 1),
        out_shape=(field, wide, wide),
        in_specs=[SM] + [VM] * 8,
        out_specs=(VM, VM, VM),
        compiler_params=room(6),
        cost_estimate=busy(1 << 31),
    )(pos, src, nxt, near, far, got_near, got_up, cpl, inv)
    got_down2 = lax.ppermute(far_even, "cells", down_pairs)
    nxt2, near2, far_odd = pl.pallas_call(
        make_odd_middle(ranks - 1),
        out_shape=(field, wide, wide),
        in_specs=[SM] + [VM] * 10,
        out_specs=(VM, VM, VM),
        compiler_params=room(6),
        cost_estimate=busy(1 << 31),
    )(pos, src, nxt, near, far, got_near, got_down, cpl, inv, nxt_even, near_even)
    got_up2 = lax.ppermute(far_odd, "cells", up_pairs)
    got_near2 = lax.ppermute(near2, "cells", intra_pairs)
    adjoint, other, grads = pl.pallas_call(
        make_end(ranks - 1, nblk),
        out_shape=(
            field, shaped(nblk // 2, params), jax.ShapeDtypeStruct((2 * params, count), BF16)
        ),
        in_specs=[SM] + [VM] * 15,
        out_specs=(HB, VM, VM),
        scratch_shapes=[pltpu.VMEM(field.shape, F32), dma((1,))],
        compiler_params=room(16),
    )(
        pos, src, nxt2, got_near, got_up, got_down, near2, far_even, far_odd, got_near2, got_up2, got_down2,
        cpl, inv, onehot, turned,
    )
    chips = ranks // 2
    got_half = lax.ppermute(other, "cells", intra_pairs)
    mine = pl.pallas_call(
        own_kernel,
        out_shape=shaped(nblk // 2, params),
        in_specs=[VM, VM],
        out_specs=VM,
        compiler_params=room(6),
    )(onehot, grads)
    half = mine + got_half
    same_core = [[core + 2 * chip for chip in range(chips)] for core in range(2)]
    parts = lax.all_to_all(
        half.reshape(chips, BLK_DEV, params), "cells", 0, 0, tiled=True, axis_index_groups=same_core
    )
    owned = jnp.sum(parts, axis=0)
    gradient = owned + lax.ppermute(owned, "ens", [(0, 1), (1, 0)])
    return (adjoint, gradient)


def solution(mesh):
    placed = (
        P("ens", None, "cells", None, None),
        P("ens", None, None, None, "cells", None, None),
        P("ens", None, None, "cells", None, None),
        P("ens", None, "cells", None, None, None),
        P(),
        P("ens", None, None),
        P("cells", None, None),
    )
    return jax.shard_map(
        timestep,
        mesh=mesh,
        in_specs=placed,
        out_specs=(P("ens", None, "cells", None, None), P("cells", None)),
        check_vma=False,
    )
```

```python
import jax
import jax.numpy as jnp
from jax import lax
from jax.experimental import pallas as pl
from jax.experimental.pallas import tpu as pltpu
from jax.sharding import PartitionSpec as P


BLK_DEV = 4
F32 = jnp.float32
BF16 = jnp.bfloat16


def shift_lanes(x, by):
    size = x.shape[2]
    lane = lax.broadcasted_iota(jnp.int32, x.shape, 2)
    keep = lane >= 1 if by == 1 else lane < size - 1
    return jnp.where(keep, pltpu.roll(x, by % size, 2), 0.0)


def shift_rows(x, by):
    size = x.shape[1]
    row = lax.broadcasted_iota(jnp.int32, x.shape, 1)
    keep = row >= 1 if by == 1 else row < size - 1
    return jnp.where(keep, pltpu.roll(x, by % size, 1), 0.0)


def products(cpl, m, k, a):
    unk = len(a)
    out = []
    for v in range(unk):
        total = cpl[m, k, 0, v].astype(F32) * a[0]
        for u in range(1, unk):
            total = total + cpl[m, k, u, v].astype(F32) * a[u]
        out.append(total)
    return out


def local_coupling(cpl, m, a):
    unk = len(a)
    terms = [products(cpl, m, k, a) for k in range(6)]
    inner, up, down = [], [], []
    for v in range(unk):
        t = [terms[k][v] for k in range(6)]
        planes = t[0].shape[0]
        zero = jnp.zeros_like(t[0][:1])
        total = jnp.concatenate([zero, t[0][: planes - 1]], axis=0)
        total = total + jnp.concatenate([t[1][1:], zero], axis=0)
        total = total + shift_rows(t[2], 1) + shift_rows(t[3], -1)
        total = total + shift_lanes(t[4], 1) + shift_lanes(t[5], -1)
        inner.append(total)
        up.append(t[0][planes - 1])
        down.append(t[1][0])
    return inner, up, down


def apply_inverse(inv, m, r):
    unk = len(r)
    out = []
    for v in range(unk):
        total = inv[m, 0, v].astype(F32) * r[0]
        for w in range(1, unk):
            total = total + inv[m, w, v].astype(F32) * r[w]
        out.append(total)
    return out


def plane_products(cpl, m, k, plane, a):
    unk = len(a)
    out = []
    for v in range(unk):
        total = cpl[m, k, 0, v, plane].astype(F32) * a[0]
        for u in range(1, unk):
            total = total + cpl[m, k, u, v, plane].astype(F32) * a[u]
        out.append(total)
    return out


def two_sweep_payload(cpl, inv, m, src, a):
    planes = a[0].shape[0]
    inner, up0, down0 = local_coupling(cpl, m, a)
    nxt = apply_inverse(inv, m, [s - b for s, b in zip(src, inner)])
    up1 = plane_products(cpl, m, 0, planes - 1, [x[planes - 1] for x in nxt])
    down1 = plane_products(cpl, m, 1, 0, [x[0] for x in nxt])
    return nxt, up0 + up1, down0 + down1


def transfer_blocks(cpl, inv, m, k, plane, unk):
    out = []
    for w in range(unk):
        for v in range(unk):
            total = inv[m, w, 0, plane].astype(F32) * cpl[m, k, 0, v, plane].astype(F32)
            for u in range(1, unk):
                total = total + inv[m, w, u, plane].astype(F32) * cpl[m, k, u, v, plane].astype(F32)
            out.append(total)
    return out


def split3(x):
    hi = x.astype(BF16)
    rest = x - hi.astype(F32)
    mid = rest.astype(BF16)
    lo = (rest - mid.astype(F32)).astype(BF16)
    return hi, mid, lo


def injected(wells, misfit, first, shape):
    members, unk, planes, rows, lanes = shape
    count = planes * rows * lanes
    nwell = wells.shape[1]
    place = wells[...] - first
    inside = (place >= 0) & (place < count)
    line = jnp.where(inside, place // lanes, -1)
    lane = jnp.where(inside, place % lanes, -1)
    lines = lax.broadcasted_iota(jnp.int32, (planes * rows, nwell), 0) == line
    onlane = (lax.broadcasted_iota(jnp.int32, (lanes, nwell), 0) == lane).astype(F32).astype(BF16)
    left = []
    for m in range(members):
        for u in range(unk):
            left.append(jnp.where(lines, misfit[m, u : u + 1, :], 0.0))
    stacked = jnp.concatenate(split3(jnp.concatenate(left, axis=0)), axis=0)
    full = lax.dot_general(stacked, onlane, (((1,), (1,)), ((), ())), preferred_element_type=F32)
    n = members * unk * planes * rows
    total = full[:n] + full[n : 2 * n] + full[2 * n :]
    return total.reshape(shape)


def first_kernel(out):
    out[...] = jnp.zeros_like(out)


def start_kernel(pos, _, wells, misfit, later, cpl, inv, src, nxt_out, intra_out, cross_out):
    shape = src.shape
    members, unk, planes = shape[:3]
    even = pos[0] % 2 == 0
    count = planes * shape[3] * shape[4]
    src[...] = later[...] + injected(wells, misfit, pos[0] * count, shape)
    for m in range(members):
        s = [src[m, u] for u in range(unk)]
        a = apply_inverse(inv, m, s)
        nxt, up, down = two_sweep_payload(cpl, inv, m, s, a)
        up = up + transfer_blocks(cpl, inv, m, 0, planes - 1, unk)
        down = down + transfer_blocks(cpl, inv, m, 1, 0, unk)
        for u in range(unk):
            nxt_out[m, u] = nxt[u]
        for j in range(len(up)):
            intra_out[m, j] = jnp.where(even, up[j], down[j])
            cross_out[m, j] = jnp.where(even, down[j], up[j])


def incoming(pos, last, m, unk, near, far):
    even = pos[0] % 2 == 0
    has_cross = (pos[0] != 0) & (pos[0] != last)
    sides = []
    for sent, got, block in (near, far):
        first = [got(m, v) for v in range(unk)]
        second = []
        for v in range(unk):
            total = got(m, unk + v)
            for w in range(unk):
                total = total - block(m, 2 * unk + w * unk + v) * sent(m, w)
            second.append(total)
        sides.append((first, second))
    out = []
    for n in range(2):
        low, high = [], []
        for v in range(unk):
            near_v = sides[0][n][v]
            far_v = jnp.where(has_cross, sides[1][n][v], 0.0)
            low.append(jnp.where(even, far_v, near_v))
            high.append(jnp.where(even, near_v, far_v))
        out.append([jnp.stack([lo, hi], axis=0) for lo, hi in zip(low, high)])
    return out


def reader(ref):
    return lambda m, j: ref[m, j]


def either(pos, if_even, if_odd):
    even = pos[0] % 2 == 0
    return lambda m, j: jnp.where(even, if_even[m, j], if_odd[m, j])


def finish_two(cpl, inv, m, src, nxt, arrived):
    a1 = [x - d for x, d in zip(nxt, apply_inverse(inv, m, arrived[0]))]
    inner, _, _ = local_coupling(cpl, m, a1)
    return apply_inverse(inv, m, [s - b - p for s, b, p in zip(src, inner, arrived[1])])


def advance(pos, last, src, nxt, sent_near, sent_far, got_near, got_far, cpl, inv, nxt_out, near_out, far_out):
    members, unk = src.shape[:2]
    even = pos[0] % 2 == 0
    near = (reader(sent_near), reader(got_near), reader(got_near))
    far = (reader(sent_far), reader(got_far), reader(got_far))
    for m in range(members):
        arrived = incoming(pos, last, m, unk, near, far)
        s = [src[m, u] for u in range(unk)]
        a = finish_two(cpl, inv, m, s, [nxt[m, u] for u in range(unk)], arrived)
        ahead, up, down = two_sweep_payload(cpl, inv, m, s, a)
        for u in range(unk):
            nxt_out[m, u] = ahead[u]
        for j in range(len(up)):
            near_out[m, j] = jnp.where(even, up[j], down[j])
            far_out[m, j] = jnp.where(even, down[j], up[j])


def make_even_middle(last):
    def even_middle(*refs):
        pos, outs = refs[0], refs[9:]

        @pl.when(pos[0] % 2 == 0)
        def _():
            advance(pos, last, *refs[1:9], *outs)

        @pl.when(pos[0] % 2 == 1)
        def _():
            for out in outs:
                out[...] = jnp.zeros_like(out)

    return even_middle


def make_odd_middle(last):
    def odd_middle(*refs):
        pos, (nxt_even, near_even), outs = refs[0], refs[9:11], refs[11:]

        @pl.when(pos[0] % 2 == 1)
        def _():
            advance(pos, last, *refs[1:9], *outs)

        @pl.when(pos[0] % 2 == 0)
        def _():
            outs[0][...] = nxt_even[...]
            outs[1][...] = near_even[...]
            outs[2][...] = jnp.zeros_like(outs[2])

    return odd_middle


def select_kernel(pos, bmap, sens, onehot, turned):
    rows, lanes = bmap.shape[1:]
    nblk = onehot.shape[0]
    core = pos[0] % 2
    slot = lax.broadcasted_iota(jnp.int32, (nblk, lanes), 0)
    half_rows = nblk // 2
    parity = jnp.where(slot < half_rows, core, 1 - core)
    within = jnp.where(slot < half_rows, slot, slot - half_rows)
    block = (within // BLK_DEV * 2 + parity) * BLK_DEV + within % BLK_DEV
    for g in range(bmap.shape[0] * rows):
        row = bmap[g // rows, g % rows : g % rows + 1, :]
        onehot[:, g * lanes : (g + 1) * lanes] = (block == row).astype(F32).astype(BF16)
    for m in range(sens.shape[0]):
        for u in range(sens.shape[1]):
            for g in range(bmap.shape[0] * rows):
                turned[m, u, g] = sens[m, u, g // rows, g % rows].astype(F32).T


def block_sums(rows, grads, params):
    both = lax.dot_general(rows, grads, (((1,), (1,)), ((), ())), preferred_element_type=F32)
    return both[:, :params] + both[:, params:]


def own_kernel(onehot, grads, adj, out, adj_out, sems):
    store = pltpu.make_async_copy(adj, adj_out, sems.at[0])
    store.start()
    out[...] = block_sums(onehot[: out.shape[0]], grads[...], out.shape[1])
    store.wait()


def make_end(last, nblk):
    def end_kernel(
        pos, src, nxt, block_near, block_even, block_odd, sent_near, sent_even, sent_odd, got_near, got_even, got_odd,
        cpl, inv, onehot, turned, adj, other_out, grads,
    ):
        members, unk, planes, rows, lanes = src.shape
        params = turned.shape[-2]
        groups = planes * rows
        half_rows = nblk // 2
        near = (reader(sent_near), reader(got_near), reader(block_near))
        far = (
            either(pos, sent_even, sent_odd), either(pos, got_even, got_odd), either(pos, block_even, block_odd),
        )
        for m in range(members):
            arrived = incoming(pos, last, m, unk, near, far)
            a = finish_two(
                cpl, inv, m, [src[m, u] for u in range(unk)], [nxt[m, u] for u in range(unk)], arrived
            )
            for u in range(unk):
                adj[m, u] = a[u]
        step = 32
        for g in range(groups):
            x, y = g // rows, g % rows
            for p in range(0, params, step):
                total = None
                for m in range(members):
                    for u in range(unk):
                        term = adj[m, u, x, y : y + 1] * turned[m, u, g, p : p + step]
                        total = term if total is None else total + term
                hi = total.astype(BF16)
                lo = (total - hi.astype(F32)).astype(BF16)
                grads[p : p + step, g * lanes : (g + 1) * lanes] = hi
                grads[params + p : params + p + step, g * lanes : (g + 1) * lanes] = lo
        other_out[...] = block_sums(onehot[half_rows:], grads[...], params)

    return end_kernel


VM = pl.BlockSpec(memory_space=pltpu.VMEM)
SM = pl.BlockSpec(memory_space=pltpu.SMEM)
MIB = 1 << 20


def room(mib):
    return pltpu.CompilerParams(vmem_limit_bytes=mib * MIB)


def busy(flops):
    return pl.CostEstimate(flops=flops, bytes_accessed=0, transcendentals=0)


def shaped(*shape):
    return jax.ShapeDtypeStruct(shape, F32)


def timestep(later_adjoint, coupling, diag_inverse, sensitivity, well_cells, well_misfit, block_map):
    members, unk, planes, rows, lanes = later_adjoint.shape
    count = planes * rows * lanes
    params = sensitivity.shape[-1]
    ranks = lax.axis_size("cells")
    nblk = ranks * BLK_DEV
    pos = lax.axis_index("cells").astype(jnp.int32).reshape(1)
    intra_pairs = [(i, i ^ 1) for i in range(ranks)]
    up_pairs = [(i, (i + 1) % ranks) for i in range(ranks)]
    down_pairs = [((i + 1) % ranks, i) for i in range(ranks)]

    field = shaped(members, unk, planes, rows, lanes)
    first_size = 2 * unk + unk * unk
    wells = well_cells.reshape(1, -1)
    cpl, inv = coupling, diag_inverse
    token = pl.pallas_call(
        first_kernel,
        out_shape=shaped(8, 128),
        out_specs=VM,
        compiler_params=room(1),
        cost_estimate=busy(1 << 31),
    )()
    src, nxt, near, far = pl.pallas_call(
        start_kernel,
        out_shape=(field, field, shaped(members, first_size, rows, lanes), shaped(members, first_size, rows, lanes)),
        in_specs=[SM] + [VM] * 6,
        out_specs=(VM,) * 4,
        compiler_params=room(6),
    )(pos, token, wells, well_misfit, later_adjoint, coupling, diag_inverse)
    got_up = lax.ppermute(far, "cells", up_pairs)
    got_down = lax.ppermute(far, "cells", down_pairs)
    got_near = lax.ppermute(near, "cells", intra_pairs)
    onehot, turned = pl.pallas_call(
        select_kernel,
        out_shape=(
            jax.ShapeDtypeStruct((nblk, count), BF16), shaped(members, unk, planes * rows, params, lanes)
        ),
        in_specs=[SM, VM, VM],
        out_specs=(VM, VM),
        compiler_params=room(6),
        cost_estimate=busy(1 << 24),
    )(pos, block_map, sensitivity)
    wide = shaped(members, 2 * unk, rows, lanes)
    nxt_even, near_even, far_even = pl.pallas_call(
        make_even_middle(ranks - 1),
        out_shape=(field, wide, wide),
        in_specs=[SM] + [VM] * 8,
        out_specs=(VM, VM, VM),
        compiler_params=room(6),
        cost_estimate=busy(1 << 31),
    )(pos, src, nxt, near, far, got_near, got_up, cpl, inv)
    got_down2 = lax.ppermute(far_even, "cells", down_pairs)
    nxt2, near2, far_odd = pl.pallas_call(
        make_odd_middle(ranks - 1),
        out_shape=(field, wide, wide),
        in_specs=[SM] + [VM] * 10,
        out_specs=(VM, VM, VM),
        compiler_params=room(6),
        cost_estimate=busy(1 << 31),
    )(pos, src, nxt, near, far, got_near, got_down, cpl, inv, nxt_even, near_even)
    got_up2 = lax.ppermute(far_odd, "cells", up_pairs)
    got_near2 = lax.ppermute(near2, "cells", intra_pairs)
    adj, other, grads = pl.pallas_call(
        make_end(ranks - 1, nblk),
        out_shape=(
            field, shaped(nblk // 2, params), jax.ShapeDtypeStruct((2 * params, count), BF16)
        ),
        in_specs=[SM] + [VM] * 15,
        out_specs=(VM, VM, VM),
        compiler_params=room(16),
    )(
        pos, src, nxt2, got_near, got_up, got_down, near2, far_even, far_odd, got_near2, got_up2, got_down2,
        cpl, inv, onehot, turned,
    )
    chips = ranks // 2
    got_half = lax.ppermute(other, "cells", intra_pairs)
    mine, adjoint = pl.pallas_call(
        own_kernel,
        out_shape=(shaped(nblk // 2, params), field),
        in_specs=[VM, VM, VM],
        out_specs=(VM, pl.BlockSpec(memory_space=pltpu.HBM)),
        scratch_shapes=[pltpu.SemaphoreType.DMA((1,))],
        compiler_params=room(6),
    )(onehot, grads, adj)
    half = mine + got_half
    same_core = [[core + 2 * chip for chip in range(chips)] for core in range(2)]
    parts = lax.all_to_all(
        half.reshape(chips, BLK_DEV, params), "cells", 0, 0, tiled=True, axis_index_groups=same_core
    )
    owned = jnp.sum(parts, axis=0)
    gradient = owned + lax.ppermute(owned, "ens", [(0, 1), (1, 0)])
    return (adjoint, gradient)


def solution(mesh):
    placed = (
        P("ens", None, "cells", None, None),
        P("ens", None, None, None, "cells", None, None),
        P("ens", None, None, "cells", None, None),
        P("ens", None, "cells", None, None, None),
        P(),
        P("ens", None, None),
        P("cells", None, None),
    )
    return jax.shard_map(
        timestep,
        mesh=mesh,
        in_specs=placed,
        out_specs=(P("ens", None, "cells", None, None), P("cells", None)),
        check_vma=False,
    )
```
